128 devices in a mesh: tm: 128 (over x, z, y, core).
Axes of the slice: x: 4, y: 4, z: 4, core: 2. Of those that a mesh axis runs over, the one named last changes fastest.
Arguments:
- field: bfloat16 [43008, 8192], P('tm'), may hold values from -52 to 52
- index: float32 [43008, 10], P('tm'), may hold values from -13 to 13
- lag_list: int32 [61], replicated, may hold values from -30 to 30, as said below
- index_offset: int32 [10], replicated, may hold values from 0 to 14, as said below
- sea_mask: int32 [8192], P('tm'), may hold values 0 or 1
Outputs:
- corr_maps: float32 [8192, 10, 61], P('tm')
The draws below stay inside these ranges and needn't reach their ends.
Inputs may be any that keep to these rules, and one draw needn't show every extreme that they name: `lag_list`: each whole number of -30 to 30 appears once. `index_offset`: some index has the extra lead 14.
All inputs are finite; a program needn't handle non-finite values. No bound on the sum of `sea_mask` on one device may be relied on, other than what follows from the above.
Results may differ from the reference program's by a relative error of at most 0.00051.
Values may be sent and summed in bfloat16 or wider, within the bound.
A program may use at most 256 MiB of HBM per device.

```python
import jax
import jax.numpy as jnp
from jax import lax

T_DEV = 336
INDEX_COUNT = 10
MAXLAG = 30
MAXOFF = 14
LAGS = 61
TDAYS = 43008
CELLS = 8192
N_TM = 128


def index_base(key):
    keys = jax.random.split(jax.random.fold_in(key, 11), 2)
    times = jnp.arange(TDAYS, dtype=jnp.float32)[:, None]
    envelope = 1.0 + 2.0 * times / (TDAYS - 1.0)
    noise = jax.random.truncated_normal(keys[0], -4.0, 4.0, (TDAYS, INDEX_COUNT), jnp.float32)
    offset_means = jax.random.uniform(keys[1], (INDEX_COUNT,), jnp.float32, -0.5, 0.5)
    return envelope * noise + offset_means[None, :]


def draw_index(key, part):
    return index_base(key)


def draw_field(key, part):
    series = index_base(key)
    keys = jax.random.split(jax.random.fold_in(key, 23), 6)
    linked = jax.random.randint(keys[0], (CELLS,), 0, INDEX_COUNT)
    delays = jax.random.randint(keys[1], (CELLS,), -MAXLAG, MAXLAG + MAXOFF + 1)
    weights = jax.random.uniform(keys[2], (CELLS,), jnp.float32, 0.3, 1.0) * jnp.where(jax.random.randint(keys[3], (CELLS,), 0, 2) == 0, -1.0, 1.0)
    scales = jnp.exp(jax.random.uniform(keys[4], (CELLS,), jnp.float32, jnp.log(0.3), jnp.log(3.0)))
    times = jnp.arange(TDAYS, dtype=jnp.int32)[:, None]
    source = jnp.clip(times - delays[None, :], 0, TDAYS - 1)
    signal = series[source, linked[None, :]]
    noise = jax.random.truncated_normal(keys[5], -4.0, 4.0, (TDAYS, CELLS), jnp.float32)
    cell_means = 0.5 * weights
    return (scales[None, :] * (weights[None, :] * signal + noise + cell_means[None, :])).astype(jnp.bfloat16)


def draw_lag_list(key, part):
    order = jax.random.permutation(jax.random.fold_in(key, 31), LAGS)
    return (order - MAXLAG).astype(jnp.int32)


def draw_index_offset(key, part):
    keys = jax.random.split(jax.random.fold_in(key, 37), 2)
    series_values = jax.random.randint(keys[0], (INDEX_COUNT,), 0, MAXOFF + 1)
    chosen = jax.random.randint(keys[1], (), 0, INDEX_COUNT)
    return series_values.at[chosen].set(MAXOFF).astype(jnp.int32)


def place_ends(drawn, stream_key, smallest, high):
    dims = drawn.shape
    index_at = [jax.random.randint(jax.random.fold_in(stream_key, axis), (), 0, dims[axis]) for axis in range(len(dims))]
    drawn = drawn.at[tuple(index_at)].set(smallest)
    longest = dims.index(max(dims))
    index_at[longest] = (index_at[longest] + 1) % dims[longest]
    return drawn.at[tuple(index_at)].set(high)


def setup_inputs(seed: int = 0) -> dict:
    streams_of = jax.random.split(jax.random.key(seed), 6)
    field = draw_field(jax.random.fold_in(streams_of[5], 71), 0)
    index = draw_index(jax.random.fold_in(streams_of[5], 71), 0)
    lag_list = draw_lag_list(jax.random.fold_in(streams_of[5], 71), 0)
    index_offset = draw_index_offset(jax.random.fold_in(streams_of[5], 71), 0)
    sea_mask = place_ends((jax.random.randint(streams_of[4], (CELLS,), 0, 10) < 7).astype(jnp.int32), jax.random.fold_in(streams_of[4], 1), 0, 1)
    return dict(field=field, index=index, lag_list=lag_list, index_offset=index_offset, sea_mask=sea_mask)


def build_window_sums(padded, begin, length, reach, lag_low):
    count = reach + lag_low + 1
    piece = lax.dynamic_slice_in_dim(padded, begin, length + reach + lag_low, 0)
    windows = jnp.stack([piece[reach + lag_low - j:reach + lag_low - j + length] for j in range(count)], 1)
    return windows.reshape(length, count * padded.shape[1])

def lag_selector(shifts, reach, lag_low):
    count = reach + lag_low + 1
    places = jnp.arange(count, dtype=jnp.int32)
    return (places[None, :, None] == (shifts + lag_low)[:, None, :]).astype(jnp.float32)

def pick_lags(accum, selector):
    kcount, count, lcount = selector.shape
    spread = accum.reshape(accum.shape[0], count, kcount)
    chosen = jnp.einsum('cjk,kjl->ckl', spread, selector, precision=lax.Precision.HIGHEST)
    return chosen.reshape(accum.shape[0], kcount * lcount)

def reference(field, index, lag_list, index_offset, sea_mask):
    reach = MAXLAG + MAXOFF
    count = reach + MAXLAG + 1
    total_days = TDAYS * 1.0
    mean_i = lax.optimization_barrier(jnp.sum(index, 0)) / total_days
    var_i = lax.optimization_barrier(jnp.sum(index * index, 0)) / total_days - mean_i * mean_i
    centered = (index - mean_i).astype(jnp.bfloat16)
    shifts = (lag_list[None, :] + index_offset[:, None]).astype(jnp.int32)
    padded = jnp.pad(centered, ((reach, reach), (0, 0)))
    running_total = jnp.concatenate([jnp.zeros((1, INDEX_COUNT), jnp.float32), jnp.cumsum(padded.astype(jnp.float32), 0)], 0)
    upper_bound = (TDAYS - shifts + reach).astype(jnp.int32)
    lower_bound = (reach - shifts).astype(jnp.int32)
    series_number = jnp.arange(INDEX_COUNT, dtype=jnp.int32)[:, None]
    prefix_totals = running_total[upper_bound, series_number] - running_total[lower_bound, series_number]
    selector = lag_selector(shifts, reach, MAXLAG)
    block_rows = 8 * T_DEV
    turns = N_TM // 8

    def one_block(carry, turn):
        accum, first_sum, second_sum = carry
        begin = (turn * block_rows).astype(jnp.int32)
        rows = lax.dynamic_slice_in_dim(field, begin, block_rows, 0)
        windows = build_window_sums(padded, begin, block_rows, reach, MAXLAG)
        accum = accum + lax.dot_general(rows, windows, (((0,), (0,)), ((), ())), preferred_element_type=jnp.float32)
        wide = rows.astype(jnp.float32)
        return ((accum, first_sum + lax.optimization_barrier(jnp.sum(wide, 0)), second_sum + lax.optimization_barrier(jnp.sum(wide * wide, 0))), None)
    start_carry = (jnp.zeros((CELLS, count * INDEX_COUNT), jnp.float32), jnp.zeros((CELLS,), jnp.float32), jnp.zeros((CELLS,), jnp.float32))
    (accum, first_sum, second_sum), unused = lax.scan(one_block, start_carry, jnp.arange(turns, dtype=jnp.int32))
    products = pick_lags(accum, selector)
    mean_x = first_sum / total_days
    var_x = second_sum / total_days - mean_x * mean_x
    numer = products.reshape(CELLS, INDEX_COUNT, LAGS) - mean_x[:, None, None] * prefix_totals[None]
    scale = total_days * jnp.sqrt(var_x + 1e-06)[:, None, None] * jnp.sqrt(var_i + 1e-06)[None, :, None]
    return numer / scale * sea_mask.astype(jnp.float32)[:, None, None]
```

```python
import jax
import jax.numpy as jnp
from jax import lax
from jax.experimental import pallas as pl
from jax.experimental.pallas import tpu as pltpu
from jax.sharding import Mesh
from jax.sharding import PartitionSpec as P

MAXLAG = 30
MAXOFF = 14
LAGS = 61
KC = 10
T_DEV = 336
N_CHIP = 64
CELLS = 8192
TDAYS = 43008
TM = ("x", "z", "y", "core")
MESH = pl.DeviceIdType.MESH

K = 2 * T_DEV
KP = 768
R = 208
PR = 204
G = R // 16
LC = 896
QMAX = 32000.0
I32 = jnp.int32
F32 = jnp.float32
BF = jnp.bfloat16


def pieces():
    out = []
    for k in range(KC):
        r = k * LAGS
        end = r + LAGS
        while r < end:
            p = r // PR
            stop = min(end, (p + 1) * PR)
            out.append((k, r - k * LAGS, stop - r, p, r - p * PR))
            r = stop
    return out


def onehot3(t):
    return (2 - t) * (1 - t) // 2, t * (2 - t), t * (t - 1) // 2


def rows(g):
    return pl.ds(16 * g, 16)


def encode(chunk, put, width):
    m = jnp.abs(chunk(0))
    for g in range(1, G):
        m = jnp.maximum(m, jnp.abs(chunk(g)))
    m = jnp.max(m, axis=0, keepdims=True)
    e = jnp.ceil(jnp.log2(jnp.maximum(m, 1e-30)))
    scale = QMAX * jnp.exp2(-e)
    last = lax.broadcasted_iota(I32, (16, width), 0) == 15
    for g in range(G):
        q = jnp.round(chunk(g) * scale)
        if g == G - 1:
            q = jnp.where(last, jnp.broadcast_to(e, (16, width)), q)
        q = q.astype(I32).astype(jnp.int16)
        for i in range(width // 128):
            put(g, i, q[:, 128 * i : 128 * (i + 1)])


def decode(get):
    tail = get(G - 1).astype(I32).astype(F32)
    scale = jnp.exp2(tail[15:16, :]) * (1.0 / QMAX)
    last = lax.broadcasted_iota(I32, (16, 128), 0) == 15
    out = [get(g).astype(I32).astype(F32) * scale for g in range(G - 1)]
    out.append(jnp.where(last, 0.0, tail * scale))
    return out


def main_kernel(
    field, idxt, offv, fin, sums_o, tot_o, stat_o,
    F, W, WF, acc, S1,
    s_far, r_far, s_n, r_n, s2f, r2f, s2n, r2n, s3, r3,
    iw, g1, g2, g3, fsum, sx_s, sx_r, tb1, sy_r, tb2, sz_r, tb3,
    sem_loc, sem_fs, sem_fr, sem_is, sem_ir, sem_gs, sem_g1, sem_g2, sem_g3,
    sem_far, sem_n, sem_2f, sem_2n, sem_3,
    sem_sfar, sem_sn, sem_s2f, sem_s2n, sem_s3, sem_ss, sem_sr, sem_os, sem_or,
):
    X, Z, Y, C = (lax.axis_index(a) for a in TM)
    Q = (X * 4 + Z) * 4 + Y

    def peer(dx=0, dz=0, dy=0, dc=0):
        return {
            "x": (X + dx) % 4,
            "z": (Z + dz) % 4,
            "y": (Y + dy) % 4,
            "core": (C + dc) % 2,
        }

    def chip_peer(q, core):
        return {"x": q // 16, "z": (q // 4) % 4, "y": q % 4, "core": core}

    def along(t, delta):
        f0, f1, f2 = onehot3(t)
        return peer(dx=f0 * delta, dy=f1 * delta, dz=f2 * delta)

    partner = peer(dc=1)
    xpeers = [(dx, dc) for dx in range(4) for dc in range(2) if dx or dc]
    q_next, q_prev = (Q + 1) % N_CHIP, (Q + N_CHIP - 1) % N_CHIP

    barrier = pltpu.get_barrier_semaphore()

    def greet(device):
        pl.semaphore_signal(barrier, inc=1, device_id=device, device_id_type=MESH)

    for dx, dc in xpeers:
        greet(peer(dx=dx, dc=dc))
    for d in range(1, 4):
        greet(peer(dy=d))
        greet(peer(dz=d))
    for q in (q_next, q_prev):
        for core in range(2):
            greet(chip_peer(q, core))

    def tile_of(slot, core):
        jx, jz, h = slot // 8, (slot // 2) % 4, slot % 2
        jy = 2 * h + (core + jx + jz) % 2
        return (jx * 4 + jz) * 4 + jy

    def columns(slot, core):
        return pl.ds(pl.multiple_of(tile_of(slot, core) * 128, 128), 128)

    own_days = pl.ds(pl.multiple_of(C * T_DEV, 16), T_DEV)

    @pl.loop(0, 32)
    def _(s):
        pltpu.make_async_copy(
            field.at[:, columns(s, C)], F.at[s, own_days, :], sem_loc
        ).start()
        F[s, K:KP, :] = jnp.zeros((KP - K, 128), BF)

    mine = idxt[...]
    lane = lax.broadcasted_iota(I32, (16, 128), 1)
    first = jnp.sum(mine, axis=1, keepdims=True)
    second = jnp.sum(mine * mine, axis=1, keepdims=True)
    block = jnp.where(lane == 0, first, jnp.where(lane == 1, second, 0.0))
    me8 = X * 2 + C
    g1[me8] = block

    pl.semaphore_wait(barrier, 17)

    def remote(src, dst, ssem, rsem, device):
        return pltpu.make_async_remote_copy(
            src_ref=src, dst_ref=dst, send_sem=ssem, recv_sem=rsem,
            device_id=device, device_id_type=MESH,
        )

    g1c = [
        remote(g1.at[me8], g1.at[me8], sem_gs.at[i], sem_g1.at[i], peer(dx=dx, dc=dc))
        for i, (dx, dc) in enumerate(xpeers)
    ]
    for c in g1c:
        c.start()
    beside = (Q + N_CHIP + 2 * C - 1) % N_CHIP
    iwc = [remote(idxt, iw.at[2], sem_is.at[2], sem_ir.at[2], partner)]
    for core in range(2):
        iwc.append(
            remote(
                idxt, iw.at[1 - C], sem_is.at[core], sem_ir.at[1 - C], chip_peer(beside, core)
            )
        )
    for c in iwc:
        c.start()

    @pl.loop(0, 32)
    def _(s):
        remote(
            field.at[:, columns(s, 1 - C)], F.at[s, own_days, :], sem_fs, sem_fr, partner
        ).start()

    for c in g1c:
        c.wait_recv()
    g = g1[0]
    for i in range(1, 8):
        g = g + g1[i]
    g2[Y] = g
    g2c = [
        remote(g2.at[Y], g2.at[Y], sem_gs.at[6 + d], sem_g2.at[d - 1], peer(dy=d))
        for d in range(1, 4)
    ]
    for c in g2c:
        c.start()
    for c in g2c:
        c.wait_recv()
    g = (g2[0] + g2[1]) + (g2[2] + g2[3])
    g3[Z] = g
    g3c = [
        remote(g3.at[Z], g3.at[Z], sem_gs.at[9 + d], sem_g3.at[d - 1], peer(dz=d))
        for d in range(1, 4)
    ]
    for c in g3c:
        c.start()
    for i in range(3):
        pltpu.make_async_copy(iw.at[i], iw.at[i], sem_ir.at[i]).wait()
    for c in g3c:
        c.wait_recv()
    g = (g3[0] + g3[1]) + (g3[2] + g3[3])
    mean = g[:, 0:1] / float(TDAYS)
    var = g[:, 1:2] / float(TDAYS) - mean * mean
    stat_o[...] = jnp.where(lane == 0, mean, var)

    pos = lax.broadcasted_iota(I32, (16, LC), 1)

    def placed(piece, at):
        wide = jnp.concatenate([piece, jnp.zeros((16, LC - 384), F32)], axis=1)
        return pltpu.roll(wide, at % LC, axis=1)

    other = iw[2]
    fc = C.astype(F32)
    w0 = mine * (1.0 - fc) + other * fc
    w1 = mine * fc + other * (1.0 - fc)
    series = jnp.where(
        pos < 64,
        placed(iw[0], 64 - T_DEV),
        jnp.where(
            pos < 64 + T_DEV,
            placed(w0, 64),
            jnp.where(pos < 64 + K, placed(w1, 64 + T_DEV), placed(iw[1], 64 + K)),
        ),
    )
    centered = (series - mean).astype(BF).astype(F32)
    day = Q * K - 64 + pos
    centered = jnp.where((day >= 0) & (day < TDAYS), centered, 0.0)
    off = offv[:, 0:1]
    shifted = centered
    for o in range(1, MAXOFF + 1):
        shifted = jnp.where(off == o, pltpu.roll(centered, o, axis=1), shifted)
    tail = lax.broadcasted_iota(I32, (LAGS, KP), 1) < K
    for p in range(3):
        lo = PR if p < 2 else KC * LAGS - 2 * PR
        WF[R * p + lo - lo % 8 : R * (p + 1), :] = jnp.zeros((R - lo + lo % 8, KP), F32)
    todo = pieces()
    for k in range(KC):
        x = jnp.broadcast_to(shifted[k : k + 1, :], (64, LC))
        x = pltpu.roll(x, LC - 64 - MAXLAG, axis=1, stride=1, stride_axis=0)
        x = jnp.where(tail, x[:LAGS, :KP], 0.0)
        for kk, a, n, p, b in todo:
            if kk == k:
                WF[R * p + b : R * p + b + n, :] = x[a : a + n, :]
    for p in range(3):
        W[p] = WF[R * p : R * (p + 1), :].astype(BF)

    pltpu.make_async_copy(F.at[:, own_days, :], F.at[:, own_days, :], sem_loc).wait()
    pltpu.make_async_copy(F.at[:, own_days, :], F.at[:, own_days, :], sem_fr).wait()

    def part_coords(p):
        e0, e1, e2 = onehot3(p)
        return (
            e0 * X + e1 * Y + e2 * Z,
            e0 * Y + e1 * Z + e2 * X,
            e0 * Z + e1 * X + e2 * Y,
        )

    def slot_of(p, ja, jb, hd):
        e0, e1, e2 = onehot3(p)
        jd = 2 * hd + (C + ja + jb) % 2
        jx = e0 * ja + e1 * jd + e2 * jb
        jy = e0 * jb + e1 * ja + e2 * jd
        jz = e0 * jd + e1 * jb + e2 * ja
        return (jx * 4 + jz) * 2 + jy // 2

    def products(p, ja, hd):
        wide = jnp.concatenate([F[slot_of(p, ja, jb, hd)] for jb in range(4)], axis=1)
        return jnp.dot(W[p], wide, preferred_element_type=F32)

    def send4(buf, at, u, sgn, dst, dst_at, ssem, rsem):
        p = u // 2
        for jb in range(4):
            remote(
                buf.at[at + (jb,)], dst.at[dst_at + (jb,)], ssem, rsem.at[dst_at + (jb,)],
                along(p, sgn),
            ).start()

    def encode4(buf, at):
        def put(g, i, tile):
            buf[at + (i, rows(g), slice(None))] = tile

        encode(lambda g: acc[rows(g), :], put, 512)

    @pl.loop(0, 6)
    def _(u):
        p, dr = u // 2, u % 2
        a, b, d = part_coords(p)
        acc[...] = products(p, (a + 2) % 4, dr)
        encode4(s_far, (u,))
        send4(s_far, (u,), u, 1 - 2 * dr, r_far, (u,), sem_sfar, sem_far)

    @pl.loop(0, 6)
    def _(u):
        p, dr = u // 2, u % 2
        sgn = 1 - 2 * dr
        a, b, d = part_coords(p)
        acc[...] = products(p, (a + sgn + 4) % 4, 1 - dr)
        encode4(s_n, (u, 1 - dr))
        send4(s_n, (u, 1 - dr), u, sgn, r_n, (u, 1 - dr), sem_sn, sem_n)

    @pl.loop(0, 6)
    def _(u):
        p, dr = u // 2, u % 2
        sgn = 1 - 2 * dr
        a, b, d = part_coords(p)
        acc[...] = products(p, (a + sgn + 4) % 4, dr)
        for jb in range(4):
            pltpu.make_async_copy(r_far.at[u, jb], r_far.at[u, jb], sem_far.at[u, jb]).wait()
            got = decode(lambda g: r_far[u, jb, rows(g), :])
            for g in range(G):
                acc[rows(g), 128 * jb : 128 * (jb + 1)] += got[g]
        encode4(s_n, (u, dr))
        send4(s_n, (u, dr), u, sgn, r_n, (u, dr), sem_sn, sem_n)

    @pl.loop(0, 32)
    def _(s):
        x = F[s].astype(F32)
        fsum[s, 0:1, :] = jnp.sum(x, axis=0, keepdims=True)
        fsum[s, 1:2, :] = jnp.sum(x * x, axis=0, keepdims=True)

    tb1[...] = jnp.zeros((24, 128), F32)
    ones = jnp.ones((8, KP), BF)
    for p in range(3):
        t = lax.dot_general(ones, W[p], (((1,), (1,)), ((), ())), preferred_element_type=F32)
        tb1[16 + 2 * p : 17 + 2 * p, :] = t[0:1, 0:128]
        tb1[17 + 2 * p : 18 + 2 * p, 0:80] = t[0:1, 128:208]

    def cell_sums(dst, ja):
        for jb in range(4):
            for hd in range(2):
                s = slot_of(0, ja, jb, hd)
                i = 2 * jb + hd
                dst[i : i + 1, :] = fsum[s, 0:1, :]
                dst[8 + i : 9 + i, :] = fsum[s, 1:2, :]

    cell_sums(tb1, X)
    sxc = []
    for d in range(1, 4):
        to = sx_s.at[d - 1]
        to[16:24, :] = tb1[16:24, :]
        cell_sums(to, (X + d) % 4)
        c = remote(to, sx_r.at[d - 1], sem_ss.at[d - 1], sem_sr.at[d - 1], peer(dx=d))
        c.start()
        sxc.append(c)

    @pl.loop(0, 6)
    def _(w):
        p, hd = w // 2, w % 2
        a, b, d = part_coords(p)
        got = products(p, a, hd)
        for jb in range(4):
            S1[w, jb] = got[:, 128 * jb : 128 * (jb + 1)]

    for c in sxc:
        c.wait_recv()
    tb1[...] = (tb1[...] + sx_r[0]) + (sx_r[1] + sx_r[2])
    syc = [
        remote(tb1, sy_r.at[d - 1], sem_ss.at[2 + d], sem_sr.at[2 + d], peer(dy=d))
        for d in range(1, 4)
    ]
    for c in syc:
        c.start()

    def add_tile(w, jb, buf, at, sems):
        pltpu.make_async_copy(buf.at[at], buf.at[at], sems.at[at]).wait()
        got = decode(lambda g: buf[at + (rows(g), slice(None))])
        for g in range(G):
            S1[w, jb, rows(g), :] += got[g]

    def arrived1(w, jb):
        p, hd = w // 2, w % 2
        add_tile(w, jb, r_n, (2 * p + 1 - hd, hd, jb), sem_n)
        add_tile(w, jb, r_n, (2 * p + hd, hd, jb), sem_n)

    def encode1(w, jb, buf, at):
        def put(g, i, tile):
            buf[at + (rows(g), slice(None))] = tile

        encode(lambda g: S1[w, jb, rows(g), :], put, 128)

    @pl.loop(0, 6)
    def _(u):
        p, dr = u // 2, u % 2
        a, b, d = part_coords(p)
        w, jb = 2 * p + dr, (b + 2) % 4
        arrived1(w, jb)
        encode1(w, jb, s2f, (u,))
        remote(
            s2f.at[u], r2f.at[u], sem_s2f, sem_2f.at[u], along((p + 1) % 3, 1 - 2 * dr)
        ).start()

    @pl.loop(0, 6)
    def _(u):
        p, dr = u // 2, u % 2
        sgn = 1 - 2 * dr
        a, b, d = part_coords(p)
        w, jb = 2 * p + 1 - dr, (b + sgn + 4) % 4
        arrived1(w, jb)
        encode1(w, jb, s2n, (u, 1 - dr))
        remote(
            s2n.at[u, 1 - dr], r2n.at[u, 1 - dr], sem_s2n, sem_2n.at[u, 1 - dr],
            along((p + 1) % 3, sgn),
        ).start()

    for c in syc:
        c.wait_recv()
    tb2[...] = (tb1[...] + sy_r[0]) + (sy_r[1] + sy_r[2])
    szc = [
        remote(tb2, sz_r.at[d - 1], sem_ss.at[5 + d], sem_sr.at[5 + d], peer(dz=d))
        for d in range(1, 4)
    ]
    for c in szc:
        c.start()

    @pl.loop(0, 6)
    def _(u):
        p, dr = u // 2, u % 2
        sgn = 1 - 2 * dr
        a, b, d = part_coords(p)
        w, jb = 2 * p + dr, (b + sgn + 4) % 4
        arrived1(w, jb)
        add_tile(w, jb, r2f, (u,), sem_2f)
        encode1(w, jb, s2n, (u, dr))
        remote(
            s2n.at[u, dr], r2n.at[u, dr], sem_s2n, sem_2n.at[u, dr], along((p + 1) % 3, sgn)
        ).start()

    @pl.loop(0, 6)
    def _(w):
        p = w // 2
        a, b, d = part_coords(p)
        arrived1(w, b)

    for c in szc:
        c.wait_recv()
    total = (tb2[...] + sz_r[0]) + (sz_r[1] + sz_r[2])
    tot_o[...] = total[16:24, :]

    final = (C + X + Y + Z) % 2 == 0

    @pl.loop(0, 3)
    def _(p):
        a, b, d = part_coords(p)
        for hd in range(2):
            w = 2 * p + hd
            add_tile(w, b, r2n, (2 * p + 1 - hd, hd), sem_2n)
            add_tile(w, b, r2n, (2 * p + hd, hd), sem_2n)

        @pl.when(final)
        def _():
            encode1(2 * p + 1 - d // 2, b, s3, (p, 2))
            remote(
                s3.at[p, 2], r3.at[p, 2], sem_s3, sem_3.at[p, 2], along((p + 2) % 3, 2)
            ).start()

        @pl.when(jnp.logical_not(final))
        def _():
            for i, delta in enumerate((1, 3)):
                encode1(2 * p + ((d + delta) % 4) // 2, b, s3, (p, i))
                remote(
                    s3.at[p, i], r3.at[p, i], sem_s3, sem_3.at[p, i],
                    along((p + 2) % 3, delta),
                ).start()

    @pl.when(final)
    def _():
        i = 2 * Y + Z // 2
        tb3[...] = total
        sums_o[...] = jnp.zeros((8, 128), F32)
        sums_o[0:1, :] = tb3[pl.ds(i, 1), :]
        sums_o[1:2, :] = tb3[pl.ds(i + 8, 1), :]
        remote(sums_o, sums_o, sem_os.at[3], sem_or.at[3], partner).start()

        @pl.loop(0, 3)
        def _(p):
            a, b, d = part_coords(p)
            w = 2 * p + d // 2
            for i in range(3):
                add_tile(w, b, r3, (p, i), sem_3)
            fin[p] = S1[w, b]
            remote(fin.at[p], fin.at[p], sem_os.at[p], sem_or.at[p], partner).start()

        @pl.loop(0, 3)
        def _(p):
            pltpu.make_async_copy(fin.at[p], fin.at[p], sem_os.at[p]).wait()

        pltpu.make_async_copy(sums_o, sums_o, sem_os.at[3]).wait()
        pltpu.make_async_copy(s3.at[:, 2], s3.at[:, 2], sem_s3).wait()

    @pl.when(jnp.logical_not(final))
    def _():
        @pl.loop(0, 3)
        def _(p):
            pltpu.make_async_copy(fin.at[p], fin.at[p], sem_or.at[p]).wait()

        pltpu.make_async_copy(sums_o, sums_o, sem_or.at[3]).wait()
        pltpu.make_async_copy(s3.at[:, 0:2], s3.at[:, 0:2], sem_s3).wait()

    for c in g1c + g2c + g3c + iwc + sxc + syc + szc:
        c.wait_send()
    pltpu.make_async_copy(F.at[:, own_days, :], F.at[:, own_days, :], sem_fs).wait()
    for buf, sem in ((s_far, sem_sfar), (s_n, sem_sn), (s2f, sem_s2f), (s2n, sem_s2n)):
        pltpu.make_async_copy(buf, buf, sem).wait()


def last_kernel(fin, sums, tot, stat, lag_list, mask, out, WS):
    core = lax.axis_index("core")
    n = float(TDAYS)
    mean_x = sums[0:1, :] / n
    var_x = sums[1:2, :] / n - mean_x * mean_x
    inv = 1.0 / (n * jnp.sqrt(var_x + 1e-6))
    row = lax.broadcasted_iota(I32, (R, 256), 0)
    col = lax.broadcasted_iota(I32, (R, 256), 1)
    for p in range(3):
        t = jnp.concatenate([tot[2 * p : 2 * p + 1, :], tot[2 * p + 1 : 2 * p + 2, :]], axis=1)
        t = jnp.sum(jnp.where(row == col, t, 0.0), axis=1, keepdims=True)
        WS[R * p : R * (p + 1), :] = (fin[p] - mean_x * t) * inv
    inv_i = 1.0 / jnp.sqrt(stat[:, 1:2] + 1e-6)
    place = lax.broadcasted_iota(I32, (LAGS, 128), 0) - MAXLAG
    pick = (place == lag_list[...]).astype(F32)
    todo = pieces()
    half = mask[...]
    for k in range(KC):
        x = jnp.concatenate(
            [WS[R * p + b : R * p + b + m, :] for kk, a, m, p, b in todo if kk == k], axis=0
        )
        y = lax.dot_general(
            x, pick, (((0,), (0,)), ((), ())),
            precision=lax.Precision.HIGHEST, preferred_element_type=F32,
        )
        y = jnp.where(core == 0, y[:64], y[64:])
        y = y * inv_i[k : k + 1, :] * half
        out[:, k, :] = y[:, :LAGS]


def shards(field, index, lag_list, index_offset, sea_mask):
    idxt = jnp.pad(index.T, ((0, 16 - KC), (0, 384 - T_DEV)))
    offv = jnp.broadcast_to(jnp.pad(index_offset, (0, 16 - KC))[:, None], (16, 128))
    vmem = pl.BlockSpec(memory_space=pltpu.VMEM)
    i16 = jnp.int16
    dma = pltpu.SemaphoreType.DMA
    fin, sums, tot, stat = pl.pallas_call(
        main_kernel,
        out_shape=(
            jax.ShapeDtypeStruct((3, R, 128), F32),
            jax.ShapeDtypeStruct((8, 128), F32),
            jax.ShapeDtypeStruct((8, 128), F32),
            jax.ShapeDtypeStruct((16, 128), F32),
        ),
        in_specs=[pl.BlockSpec(memory_space=pl.ANY), vmem, vmem],
        out_specs=(vmem, vmem, vmem, vmem),
        scratch_shapes=[
            pltpu.VMEM((32, KP, 128), BF),
            pltpu.VMEM((3, R, KP), BF),
            pltpu.VMEM((3 * R, KP), F32),
            pltpu.VMEM((R, 512), F32),
            pltpu.VMEM((6, 4, R, 128), F32),
            pltpu.VMEM((6, 4, R, 128), i16),
            pltpu.VMEM((6, 4, R, 128), i16),
            pltpu.VMEM((6, 2, 4, R, 128), i16),
            pltpu.VMEM((6, 2, 4, R, 128), i16),
            pltpu.VMEM((6, R, 128), i16),
            pltpu.VMEM((6, R, 128), i16),
            pltpu.VMEM((6, 2, R, 128), i16),
            pltpu.VMEM((6, 2, R, 128), i16),
            pltpu.VMEM((3, 3, R, 128), i16),
            pltpu.VMEM((3, 3, R, 128), i16),
            pltpu.VMEM((3, 16, 384), F32),
            pltpu.VMEM((8, 16, 128), F32),
            pltpu.VMEM((4, 16, 128), F32),
            pltpu.VMEM((4, 16, 128), F32),
            pltpu.VMEM((32, 8, 128), F32),
            pltpu.VMEM((3, 24, 128), F32),
            pltpu.VMEM((3, 24, 128), F32),
            pltpu.VMEM((24, 128), F32),
            pltpu.VMEM((3, 24, 128), F32),
            pltpu.VMEM((24, 128), F32),
            pltpu.VMEM((3, 24, 128), F32),
            pltpu.VMEM((24, 128), F32),
            dma,
            dma,
            dma,
            dma((3,)),
            dma((3,)),
            dma((13,)),
            dma((7,)),
            dma((3,)),
            dma((3,)),
            dma((6, 4)),
            dma((6, 2, 4)),
            dma((6,)),
            dma((6, 2)),
            dma((3, 3)),
            dma,
            dma,
            dma,
            dma,
            dma,
            dma((9,)),
            dma((9,)),
            dma((4,)),
            dma((4,)),
        ],
        compiler_params=pltpu.CompilerParams(
            collective_id=0, has_side_effects=True, vmem_limit_bytes=60000 * 1024
        ),
    )(field, idxt, offv)
    lags = jnp.pad(lag_list, (0, 128 - LAGS), constant_values=1000)[None, :]
    mask = sea_mask.astype(F32)[:, None]
    return pl.pallas_call(
        last_kernel,
        out_shape=jax.ShapeDtypeStruct((CELLS // 128, KC, LAGS), F32),
        in_specs=[vmem] * 6,
        out_specs=vmem,
        scratch_shapes=[pltpu.VMEM((3 * R, 128), F32)],
    )(fin, sums, tot, stat, lags, mask)


def solution(mesh):
    finer = Mesh(mesh.devices.reshape(4, 4, 4, 2), TM)
    return jax.shard_map(
        shards,
        mesh=finer,
        in_specs=(P(TM, None), P(TM, None), P(), P(), P(TM)),
        out_specs=P(TM, None, None),
        check_vma=False,
    )
```

```python
import jax
import jax.numpy as jnp
from jax import lax
from jax.experimental import pallas as pl
from jax.experimental.pallas import tpu as pltpu
from jax.sharding import Mesh
from jax.sharding import PartitionSpec as P

MAXLAG = 30
MAXOFF = 14
LAGS = 61
KC = 10
T_DEV = 336
N_CHIP = 64
CELLS = 8192
TDAYS = 43008
TM = ("x", "z", "y", "core")
MESH = pl.DeviceIdType.MESH

K = 2 * T_DEV
KP = 768
R = 208
PR = 204
G = R // 16
LC = 896
QMAX = 32000.0
I32 = jnp.int32
F32 = jnp.float32
BF = jnp.bfloat16


def pieces():
    out = []
    for k in range(KC):
        r = k * LAGS
        end = r + LAGS
        while r < end:
            p = r // PR
            stop = min(end, (p + 1) * PR)
            out.append((k, r - k * LAGS, stop - r, p, r - p * PR))
            r = stop
    return out


def onehot3(t):
    return (2 - t) * (1 - t) // 2, t * (2 - t), t * (t - 1) // 2


def rows(g):
    return pl.ds(16 * g, 16)


def encode(chunk, put, width):
    m = jnp.abs(chunk(0))
    for g in range(1, G):
        m = jnp.maximum(m, jnp.abs(chunk(g)))
    m = jnp.max(m, axis=0, keepdims=True)
    e = jnp.ceil(jnp.log2(jnp.maximum(m, 1e-30)))
    scale = QMAX * jnp.exp2(-e)
    last = lax.broadcasted_iota(I32, (16, width), 0) == 15
    for g in range(G):
        q = jnp.round(chunk(g) * scale)
        if g == G - 1:
            q = jnp.where(last, jnp.broadcast_to(e, (16, width)), q)
        q = q.astype(I32).astype(jnp.int16)
        for i in range(width // 128):
            put(g, i, q[:, 128 * i : 128 * (i + 1)])


def decode(get):
    tail = get(G - 1).astype(I32).astype(F32)
    scale = jnp.exp2(tail[15:16, :]) * (1.0 / QMAX)
    last = lax.broadcasted_iota(I32, (16, 128), 0) == 15
    out = [get(g).astype(I32).astype(F32) * scale for g in range(G - 1)]
    out.append(jnp.where(last, 0.0, tail * scale))
    return out


def main_kernel(
    field, idx, offs, fin, sums_o, tot_o, stat_o,
    F, W, WF, acc, NP, S1,
    s_far, r_far, s_n, r_n, s2f, r2f, s2n, r2n, s3, r3,
    iw, ipad, bo, g1, g2, fsum, sx_s, sx_r, tb1, sy_r, tb2, sz_r, tb3,
    sem_loc, sem_fs, sem_fr, sem_is, sem_ir, sem_gs, sem_g1, sem_g2,
    sem_far, sem_n, sem_2f, sem_2n, sem_3,
    sem_sfar, sem_sn, sem_s2f, sem_s2n, sem_s3, sem_ss, sem_sr, sem_os, sem_or, sem_bs, sem_br,
):
    X, Z, Y, C = (lax.axis_index(a) for a in TM)
    Q = (X * 4 + Z) * 4 + Y

    def peer(dx=0, dz=0, dy=0, dc=0):
        return {
            "x": (X + dx) % 4,
            "z": (Z + dz) % 4,
            "y": (Y + dy) % 4,
            "core": (C + dc) % 2,
        }

    def chip_peer(q, core):
        return {"x": q // 16, "z": (q // 4) % 4, "y": q % 4, "core": core}

    def along(t, delta, dc=0):
        f0, f1, f2 = onehot3(t)
        return peer(dx=f0 * delta, dy=f1 * delta, dz=f2 * delta, dc=dc)

    partner = peer(dc=1)
    xpeers = [(dx, dc) for dx in range(4) for dc in range(2) if dx or dc]
    yzpeers = [(dy, dz) for dy in range(4) for dz in range(4) if dy or dz]
    q_next, q_prev = (Q + 1) % N_CHIP, (Q + N_CHIP - 1) % N_CHIP

    barrier = pltpu.get_barrier_semaphore()

    def greet(device):
        pl.semaphore_signal(barrier, inc=1, device_id=device, device_id_type=MESH)

    for dx, dc in xpeers:
        greet(peer(dx=dx, dc=dc))
    for dy, dz in yzpeers:
        greet(peer(dy=dy, dz=dz))
    for d in range(1, 4):
        greet(peer(dy=d, dc=1))
        greet(peer(dz=d, dc=1))
    for q in (q_next, q_prev):
        for core in range(2):
            greet(chip_peer(q, core))

    def tile_of(slot, core):
        jx, jz, h = slot // 8, (slot // 2) % 4, slot % 2
        jy = 2 * h + (core + jx + jz) % 2
        return (jx * 4 + jz) * 4 + jy

    def columns(slot, core):
        return pl.ds(pl.multiple_of(tile_of(slot, core) * 128, 128), 128)

    own_days = pl.ds(pl.multiple_of(C * T_DEV, 16), T_DEV)

    eye = lax.broadcasted_iota(I32, (16, 128), 0) == lax.broadcasted_iota(I32, (16, 128), 1)

    def as_row(col):
        return jnp.sum(jnp.where(eye[:KC], col, 0.0), axis=0, keepdims=True)

    def as_column(row):
        return jnp.sum(jnp.where(eye, row, 0.0), axis=1, keepdims=True)

    mine = idx[...]
    me8, me16 = X * 2 + C, Y * 4 + Z
    g1[me8, 0:1, :] = as_row(jnp.sum(mine, axis=1, keepdims=True))
    g1[me8, 1:2, :] = as_row(jnp.sum(mine * mine, axis=1, keepdims=True))

    pl.semaphore_wait(barrier, 32)

    def remote(src, dst, ssem, rsem, device):
        return pltpu.make_async_remote_copy(
            src_ref=src, dst_ref=dst, send_sem=ssem, recv_sem=rsem,
            device_id=device, device_id_type=MESH,
        )

    g1c = [
        remote(g1.at[me8], g1.at[me8], sem_gs.at[i], sem_g1.at[i], peer(dx=dx, dc=dc))
        for i, (dx, dc) in enumerate(xpeers)
    ]
    for c in g1c:
        c.start()
    beside = (Q + N_CHIP + 2 * C - 1) % N_CHIP
    iwc = [remote(idx, iw.at[2], sem_is.at[2], sem_ir.at[2], partner)]
    for core in range(2):
        iwc.append(
            remote(
                idx, iw.at[1 - C], sem_is.at[core], sem_ir.at[1 - C], chip_peer(beside, core)
            )
        )
    for c in iwc:
        c.start()

    def share(begin, end):
        @pl.loop(begin, end)
        def _(s):
            remote(
                field.at[:, columns(s, 1 - C)], F.at[s, own_days, :], sem_fs, sem_fr, partner
            ).start()

    @pl.loop(0, 32)
    def _(s):
        pltpu.make_async_copy(
            field.at[:, columns(s, C)], F.at[s, own_days, :], sem_loc
        ).start()

    share(0, 10)

    @pl.loop(0, 32)
    def _(s):
        F[s, K:KP, :] = jnp.zeros((KP - K, 128), BF)

    for i in range(4):
        ipad[i] = jnp.zeros((16, 384), F32)
    ipad[3, 0:KC, 0:T_DEV] = mine

    for c in g1c:
        c.wait_recv()
    g = ((g1[0] + g1[1]) + (g1[2] + g1[3])) + ((g1[4] + g1[5]) + (g1[6] + g1[7]))
    g2[me16] = g
    g2c = [
        remote(
            g2.at[me16], g2.at[me16], sem_gs.at[7 + i], sem_g2.at[i], peer(dy=dy, dz=dz)
        )
        for i, (dy, dz) in enumerate(yzpeers)
    ]
    for c in g2c:
        c.start()
    share(10, 32)

    def cell_sums(start, fresh):
        @pl.loop(0, 32)
        def _(s):
            one = two = jnp.zeros((16, 128), F32)
            for g in range(T_DEV // 16):
                v = F[s, pl.ds(pl.multiple_of(start + 16 * g, 16), 16), :].astype(F32)
                one, two = one + v, two + v * v
            one = jnp.sum(one, axis=0, keepdims=True)
            two = jnp.sum(two, axis=0, keepdims=True)
            if not fresh:
                one, two = one + fsum[s, 0:1, :], two + fsum[s, 1:2, :]
            fsum[s, 0:1, :] = one
            fsum[s, 1:2, :] = two

    pltpu.make_async_copy(F.at[:, own_days, :], F.at[:, own_days, :], sem_loc).wait()
    cell_sums(C * T_DEV, True)
    for i in range(3):
        pltpu.make_async_copy(iw.at[i], iw.at[i], sem_ir.at[i]).wait()
        ipad[i, 0:KC, 0:T_DEV] = iw[i]
    for c in g2c:
        c.wait_recv()
    g = g2[0]
    for i in range(1, 16):
        g = g + g2[i]
    mean_row = g[0:1, :] / float(TDAYS)
    stat_o[...] = jnp.zeros((8, 128), F32)
    stat_o[0:1, :] = mean_row
    stat_o[1:2, :] = g[1:2, :] / float(TDAYS) - mean_row * mean_row
    mean = as_column(mean_row)

    pos = lax.broadcasted_iota(I32, (16, LC), 1)

    def placed(piece, at):
        wide = jnp.concatenate([piece, jnp.zeros((16, LC - 384), F32)], axis=1)
        return pltpu.roll(wide, at % LC, axis=1)

    mine, other = ipad[3], ipad[2]
    fc = C.astype(F32)
    w0 = mine * (1.0 - fc) + other * fc
    w1 = mine * fc + other * (1.0 - fc)
    series = jnp.where(
        pos < 64,
        placed(ipad[0], 64 - T_DEV),
        jnp.where(
            pos < 64 + T_DEV,
            placed(w0, 64),
            jnp.where(pos < 64 + K, placed(w1, 64 + T_DEV), placed(ipad[1], 64 + K)),
        ),
    )
    centered = (series - mean).astype(BF).astype(F32)
    day = Q * K - 64 + pos
    centered = jnp.where((day >= 0) & (day < TDAYS), centered, 0.0)
    kth = lax.broadcasted_iota(I32, (16, LC), 0)
    off = jnp.zeros((16, LC), I32)
    for k in range(KC):
        off = jnp.where(kth == k, offs[k], off)
    shifted = centered
    for o in range(1, MAXOFF + 1):
        shifted = jnp.where(off == o, pltpu.roll(centered, o, axis=1), shifted)
    tail = lax.broadcasted_iota(I32, (LAGS, KP), 1) < K
    for p in range(3):
        lo = PR if p < 2 else KC * LAGS - 2 * PR
        WF[R * p + lo - lo % 8 : R * (p + 1), :] = jnp.zeros((R - lo + lo % 8, KP), F32)
    todo = pieces()
    for k in range(KC):
        x = jnp.broadcast_to(shifted[k : k + 1, :], (64, LC))
        x = pltpu.roll(x, LC - 64 - MAXLAG, axis=1, stride=1, stride_axis=0)
        x = jnp.where(tail, x[:LAGS, :KP], 0.0)
        for kk, a, n, p, b in todo:
            if kk == k:
                WF[R * p + b : R * p + b + n, :] = x[a : a + n, :]
    for p in range(3):
        W[p] = WF[R * p : R * (p + 1), :].astype(BF)

    pltpu.make_async_copy(F.at[:, own_days, :], F.at[:, own_days, :], sem_fr).wait()

    def part_coords(p):
        e0, e1, e2 = onehot3(p)
        return (
            e0 * X + e1 * Y + e2 * Z,
            e0 * Y + e1 * Z + e2 * X,
            e0 * Z + e1 * X + e2 * Y,
        )

    def slot_of(p, ja, jb, hd):
        e0, e1, e2 = onehot3(p)
        jd = 2 * hd + (C + ja + jb) % 2
        jx = e0 * ja + e1 * jd + e2 * jb
        jy = e0 * jb + e1 * ja + e2 * jd
        jz = e0 * jd + e1 * jb + e2 * ja
        return (jx * 4 + jz) * 2 + jy // 2

    sigma = 1 - 2 * C

    def order(b):
        return [(b + 2) % 4, (b + sigma + 4) % 4, (b - sigma + 4) % 4, b]

    def products(p, ja, b, h):
        wide = [F[slot_of(p, ja, jb, hd)] for hd in (h, 1 - h) for jb in order(b)]
        return jnp.dot(W[p], jnp.concatenate(wide, axis=1), preferred_element_type=F32)

    def settle(buf, at, sem):
        pltpu.make_async_copy(buf.at[at], buf.at[at], sem).wait()

    def send_pair(u, buf, at, half, dst, ssem, rsem):
        at = at + (pl.ds(2 * half, 2),)
        remote(buf.at[at], dst.at[at], ssem, rsem, along(u // 2, 1 - 2 * (u % 2))).start()

    @pl.loop(0, 3)
    def _(v):
        p = (v + C) % 3
        a, b, d = part_coords(p)
        acc[...] = products(p, (a + 2) % 4, b, 0)

        def put(g, i, tile):
            s_far[2 * p + i // 4, i % 4, rows(g), :] = tile

        encode(lambda g: acc[rows(g), :], put, 1024)
        for half in range(2):
            for hd in range(2):
                u = 2 * p + hd
                send_pair(u, s_far, (u,), half, r_far, sem_sfar, sem_far.at[u, half])

    cell_sums((1 - C) * T_DEV, False)
    tb1[...] = jnp.zeros((24, 128), F32)
    ones = jnp.ones((8, KP), BF)
    for p in range(3):
        t = lax.dot_general(ones, W[p], (((1,), (1,)), ((), ())), preferred_element_type=F32)
        tb1[16 + 2 * p : 17 + 2 * p, :] = t[0:1, 0:128]
        tb1[17 + 2 * p : 18 + 2 * p, 0:80] = t[0:1, 128:208]

    def gather_sums(dst, ja):
        for jb in range(4):
            for hd in range(2):
                s = slot_of(0, ja, jb, hd)
                i = 2 * jb + hd
                dst[i : i + 1, :] = fsum[s, 0:1, :]
                dst[8 + i : 9 + i, :] = fsum[s, 1:2, :]

    gather_sums(tb1, X)
    sxc = []
    for d in range(1, 4):
        to = sx_s.at[d - 1]
        to[16:24, :] = tb1[16:24, :]
        gather_sums(to, (X + d) % 4)
        c = remote(to, sx_r.at[d - 1], sem_ss.at[d - 1], sem_sr.at[d - 1], peer(dx=d))
        c.start()
        sxc.append(c)

    @pl.loop(0, 6)
    def _(v):
        u = (v + 2 * C) % 6
        p, dr = u // 2, u % 2
        a, b, d = part_coords(p)
        got = products(p, (a + 1 - 2 * dr + 4) % 4, b, 1 - dr)
        acc[:, 0:512] = got[:, 0:512]
        for i in range(4):
            NP[u, i] = got[:, 512 + 128 * i : 640 + 128 * i]

        def put(g, i, tile):
            s_n[u, 1 - dr, i, rows(g), :] = tile

        encode(lambda g: acc[rows(g), 0:512], put, 512)
        send_pair(u, s_n, (u, 1 - dr), 0, r_n, sem_sn, sem_n.at[u, 1 - dr, 0])

    def near_half(half):
        @pl.loop(0, 6)
        def _(v):
            u = (v + 2 * C) % 6
            p, dr = u // 2, u % 2
            if half:
                send_pair(u, s_n, (u, 1 - dr), 1, r_n, sem_sn, sem_n.at[u, 1 - dr, 1])
            settle(r_far, (u, pl.ds(2 * half, 2)), sem_far.at[u, half])
            for i in (2 * half, 2 * half + 1):
                got = decode(lambda g: r_far[u, i, rows(g), :])
                for g in range(G):
                    acc[rows(g), 128 * (i % 2) : 128 * (i % 2) + 128] = (
                        NP[u, i, rows(g), :] + got[g]
                    )

            def put(g, i, tile):
                s_n[u, dr, 2 * half + i, rows(g), :] = tile

            encode(lambda g: acc[rows(g), 0:256], put, 256)
            send_pair(u, s_n, (u, dr), half, r_n, sem_sn, sem_n.at[u, dr, half])

    near_half(0)

    @pl.loop(0, 3)
    def _(p):
        a, b, d = part_coords(p)
        got = products(p, a, b, 0)
        for hd in range(2):
            for i in range(4):
                at = 512 * hd + 128 * i
                S1[2 * p + hd, i] = got[:, at : at + 128]

    near_half(1)

    for c in sxc:
        c.wait_recv()
    tb1[...] = (tb1[...] + sx_r[0]) + (sx_r[1] + sx_r[2])
    syc = [
        remote(tb1, sy_r.at[d - 1], sem_ss.at[2 + d], sem_sr.at[2 + d], peer(dy=d))
        for d in range(1, 4)
    ]
    for c in syc:
        c.start()

    def add_tile(w, i, *coded):
        got = [decode(lambda g, c=c: c(g)) for c in coded]
        for g in range(G):
            one = S1[w, i, rows(g), :]
            for c in got:
                one = one + c[g]
            S1[w, i, rows(g), :] = one

    def arrived(w, half):
        p, hd = w // 2, w % 2
        for dr in (1 - hd, hd):
            u = 2 * p + dr
            settle(r_n, (u, hd, pl.ds(2 * half, 2)), sem_n.at[u, hd, half])
        for i in (2 * half, 2 * half + 1):
            add_tile(
                w, i,
                lambda g: r_n[2 * p, hd, i, rows(g), :],
                lambda g: r_n[2 * p + 1, hd, i, rows(g), :],
            )

    def encode1(w, i, buf, at):
        def put(g, t, tile):
            buf[at + (rows(g), slice(None))] = tile

        encode(lambda g: S1[w, i, rows(g), :], put, 128)

    @pl.loop(0, 6)
    def _(v):
        u = (v + 3 * C) % 6
        arrived(u, 0)
        encode1(u, 0, s2f, (u,))
        remote(
            s2f.at[u], r2f.at[u], sem_s2f, sem_2f.at[u],
            along((u // 2 + 1) % 3, 1 - 2 * (u % 2)),
        ).start()

    def near2(p, i, dr, hd):
        u = 2 * p + dr
        encode1(2 * p + hd, i, s2n, (u, hd))
        remote(
            s2n.at[u, hd], r2n.at[u, hd], sem_s2n, sem_2n.at[u, hd],
            along((p + 1) % 3, 1 - 2 * dr),
        ).start()

    def near2_sum(p, i, dr):
        u = 2 * p + dr
        settle(r2f, (u,), sem_2f.at[u])
        add_tile(u, i, lambda g: r2f[u, rows(g), :])
        near2(p, i, dr, dr)

    @pl.loop(0, 3)
    def _(p):
        near2(p, 1, C, 1 - C)

    for c in syc:
        c.wait_recv()
    tb2[...] = (tb1[...] + sy_r[0]) + (sy_r[1] + sy_r[2])
    szc = [
        remote(tb2, sz_r.at[d - 1], sem_ss.at[5 + d], sem_sr.at[5 + d], peer(dz=d))
        for d in range(1, 4)
    ]
    for c in szc:
        c.start()

    @pl.loop(0, 3)
    def _(p):
        near2_sum(p, 1, C)

    @pl.loop(0, 6)
    def _(w):
        arrived(w, 1)

    @pl.loop(0, 3)
    def _(p):
        near2(p, 2, 1 - C, C)

    @pl.loop(0, 3)
    def _(p):
        near2_sum(p, 2, 1 - C)

    final = (C + X + Y + Z) % 2 == 0

    @pl.loop(0, 3)
    def _(p):
        a, b, d = part_coords(p)
        for hd in range(2):
            w = 2 * p + hd
            settle(r2n, (2 * p + 1 - hd, hd), sem_2n.at[2 * p + 1 - hd, hd])
            settle(r2n, (2 * p + hd, hd), sem_2n.at[2 * p + hd, hd])
            add_tile(
                w, 3,
                lambda g: r2n[2 * p, hd, rows(g), :],
                lambda g: r2n[2 * p + 1, hd, rows(g), :],
            )

        @pl.when(final)
        def _():
            w = 2 * p + d // 2
            remote(S1.at[w, 3], bo.at[p], sem_bs, sem_br.at[p], partner).start()
            encode1(2 * p + 1 - d // 2, 3, s3, (p, 2))
            for dc in range(2):
                remote(
                    s3.at[p, 2], r3.at[p, 2], sem_s3.at[dc], sem_3.at[p, 2],
                    along((p + 2) % 3, 2, dc),
                ).start()

        @pl.when(jnp.logical_not(final))
        def _():
            for i, delta in enumerate((1, 3)):
                encode1(2 * p + ((d + delta) % 4) // 2, 3, s3, (p, i))
                for dc in range(2):
                    remote(
                        s3.at[p, i], r3.at[p, i], sem_s3.at[dc], sem_3.at[p, i],
                        along((p + 2) % 3, delta, dc),
                    ).start()

    for c in szc:
        c.wait_recv()
    total = (tb2[...] + sz_r[0]) + (sz_r[1] + sz_r[2])
    tot_o[...] = total[16:24, :]

    @pl.when(final)
    def _():
        i = 2 * Y + Z // 2
        tb3[...] = total
        sums_o[...] = jnp.zeros((8, 128), F32)
        sums_o[0:1, :] = tb3[pl.ds(i, 1), :]
        sums_o[1:2, :] = tb3[pl.ds(i + 8, 1), :]
        remote(sums_o, sums_o, sem_os, sem_or, partner).start()

    def finish(p, base):
        got = []
        for i in range(3):
            pltpu.make_async_copy(r3.at[p, i], r3.at[p, i], sem_3.at[p, i]).wait()
            got.append(decode(lambda g: r3[p, i, rows(g), :]))
        for g in range(G):
            fin[p, rows(g), :] = (base(g) + got[0][g]) + (got[1][g] + got[2][g])

    @pl.when(final)
    def _():
        @pl.loop(0, 3)
        def _(p):
            a, b, d = part_coords(p)
            finish(p, lambda g: S1[2 * p + d // 2, 3, rows(g), :])

        pltpu.make_async_copy(bo, bo, sem_bs).wait()
        pltpu.make_async_copy(sums_o, sums_o, sem_os).wait()
        for dc in range(2):
            pltpu.make_async_copy(s3.at[:, 2], s3.at[:, 2], sem_s3.at[dc]).wait()

    @pl.when(jnp.logical_not(final))
    def _():
        @pl.loop(0, 3)
        def _(p):
            pltpu.make_async_copy(bo.at[p], bo.at[p], sem_br.at[p]).wait()
            finish(p, lambda g: bo[p, rows(g), :])

        pltpu.make_async_copy(sums_o, sums_o, sem_or).wait()
        for dc in range(2):
            pltpu.make_async_copy(s3.at[:, 0:2], s3.at[:, 0:2], sem_s3.at[dc]).wait()

    for c in g1c + g2c + iwc + sxc + syc + szc:
        c.wait_send()
    pltpu.make_async_copy(F.at[:, own_days, :], F.at[:, own_days, :], sem_fs).wait()
    for buf, sem in ((s_far, sem_sfar), (s_n, sem_sn), (s2f, sem_s2f), (s2n, sem_s2n)):
        pltpu.make_async_copy(buf, buf, sem).wait()


def last_kernel(fin, sums, tot, stat, lag_list, mask, out, WS):
    core = lax.axis_index("core")
    n = float(TDAYS)
    mean_x = sums[0:1, :] / n
    var_x = sums[1:2, :] / n - mean_x * mean_x
    inv = 1.0 / (n * jnp.sqrt(var_x + 1e-6))
    row = lax.broadcasted_iota(I32, (R, 256), 0)
    col = lax.broadcasted_iota(I32, (R, 256), 1)
    WS[KC * LAGS - 2 : KC * LAGS + 6, :] = jnp.zeros((8, 128), F32)
    for p in range(3):
        t = jnp.concatenate([tot[2 * p : 2 * p + 1, :], tot[2 * p + 1 : 2 * p + 2, :]], axis=1)
        t = jnp.sum(jnp.where(row == col, t, 0.0), axis=1, keepdims=True)
        m = min(PR, KC * LAGS - PR * p)
        WS[PR * p : PR * p + m, :] = ((fin[p] - mean_x * t) * inv)[:m]
    inv_i = 1.0 / jnp.sqrt(stat[1:2, :] + 1e-6)
    lags = lag_list[...].reshape(1, LAGS)
    place = lax.broadcasted_iota(I32, (64, LAGS), 0) - MAXLAG
    pick = (place == lags).astype(F32).astype(BF)
    pick = jnp.concatenate([pick, pick, pick], axis=0)
    r64 = lax.broadcasted_iota(I32, (64, 64), 0)
    c64 = lax.broadcasted_iota(I32, (64, 64), 1)
    sea = mask[...].reshape(1, 64).astype(F32)
    sea = jnp.sum(jnp.where(r64 == c64, sea, 0.0), axis=1, keepdims=True)
    for k in range(KC):
        x = WS[LAGS * k : LAGS * k + 64, :]
        hi = x.astype(BF)
        x = x - hi.astype(F32)
        mid = x.astype(BF)
        lo = (x - mid.astype(F32)).astype(BF)
        y = lax.dot_general(
            jnp.concatenate([hi, mid, lo], axis=0), pick, (((0,), (0,)), ((), ())),
            preferred_element_type=F32,
        )
        y = jnp.where(core == 0, y[:64], y[64:])
        out[k] = y * inv_i[:, k : k + 1] * sea


def shards(field, index, lag_list, index_offset, sea_mask):
    vmem = pl.BlockSpec(memory_space=pltpu.VMEM)
    smem = pl.BlockSpec(memory_space=pltpu.SMEM)
    i16 = jnp.int16
    dma = pltpu.SemaphoreType.DMA
    fin, sums, tot, stat = pl.pallas_call(
        main_kernel,
        out_shape=(
            jax.ShapeDtypeStruct((3, R, 128), F32),
            jax.ShapeDtypeStruct((8, 128), F32),
            jax.ShapeDtypeStruct((8, 128), F32),
            jax.ShapeDtypeStruct((8, 128), F32),
        ),
        in_specs=[pl.BlockSpec(memory_space=pl.ANY), vmem, smem],
        out_specs=(vmem, vmem, vmem, vmem),
        scratch_shapes=[
            pltpu.VMEM((32, KP, 128), BF),
            pltpu.VMEM((3, R, KP), BF),
            pltpu.VMEM((3 * R, KP), F32),
            pltpu.VMEM((R, 1024), F32),
            pltpu.VMEM((6, 4, R, 128), F32),
            pltpu.VMEM((6, 4, R, 128), F32),
            pltpu.VMEM((6, 4, R, 128), i16),
            pltpu.VMEM((6, 4, R, 128), i16),
            pltpu.VMEM((6, 2, 4, R, 128), i16),
            pltpu.VMEM((6, 2, 4, R, 128), i16),
            pltpu.VMEM((6, R, 128), i16),
            pltpu.VMEM((6, R, 128), i16),
            pltpu.VMEM((6, 2, R, 128), i16),
            pltpu.VMEM((6, 2, R, 128), i16),
            pltpu.VMEM((3, 3, R, 128), i16),
            pltpu.VMEM((3, 3, R, 128), i16),
            pltpu.VMEM((3, KC, T_DEV), F32),
            pltpu.VMEM((4, 16, 384), F32),
            pltpu.VMEM((3, R, 128), F32),
            pltpu.VMEM((8, 2, 128), F32),
            pltpu.VMEM((16, 2, 128), F32),
            pltpu.VMEM((32, 8, 128), F32),
            pltpu.VMEM((3, 24, 128), F32),
            pltpu.VMEM((3, 24, 128), F32),
            pltpu.VMEM((24, 128), F32),
            pltpu.VMEM((3, 24, 128), F32),
            pltpu.VMEM((24, 128), F32),
            pltpu.VMEM((3, 24, 128), F32),
            pltpu.VMEM((24, 128), F32),
            dma,
            dma,
            dma,
            dma((3,)),
            dma((3,)),
            dma((22,)),
            dma((7,)),
            dma((15,)),
            dma((6, 2)),
            dma((6, 2, 2)),
            dma((6,)),
            dma((6, 2)),
            dma((3, 3)),
            dma,
            dma,
            dma,
            dma,
            dma((2,)),
            dma((9,)),
            dma((9,)),
            dma,
            dma,
            dma,
            dma((3,)),
        ],
        compiler_params=pltpu.CompilerParams(
            collective_id=0, has_side_effects=True, vmem_limit_bytes=60000 * 1024
        ),
    )(field, index.T, index_offset)
    maps = pl.pallas_call(
        last_kernel,
        out_shape=jax.ShapeDtypeStruct((KC, CELLS // 128, LAGS), F32),
        in_specs=[vmem] * 6,
        out_specs=vmem,
        scratch_shapes=[pltpu.VMEM((616, 128), F32)],
    )(fin, sums, tot, stat, lag_list, sea_mask)
    return jnp.transpose(maps, (1, 0, 2))


def solution(mesh):
    finer = Mesh(mesh.devices.reshape(4, 4, 4, 2), TM)
    return jax.shard_map(
        shards,
        mesh=finer,
        in_specs=(P(TM, None), P(TM, None), P(), P(), P(TM)),
        out_specs=P(TM, None, None),
        check_vma=False,
    )
```

```python
import jax
import jax.numpy as jnp
from jax import lax
from jax.experimental import pallas as pl
from jax.experimental.pallas import tpu as pltpu
from jax.sharding import Mesh
from jax.sharding import PartitionSpec as P

MAXLAG = 30
MAXOFF = 14
LAGS = 61
KC = 10
T_DEV = 336
N_CHIP = 64
CELLS = 8192
TDAYS = 43008
TM = ("x", "z", "y", "core")
MESH = pl.DeviceIdType.MESH

K = 2 * T_DEV
KP = 768
R = 208
PR = 204
G = R // 16
HG = 7
LC = 896
QMAX = 32000.0
FAR = 1e9
I32 = jnp.int32
F32 = jnp.float32
BF = jnp.bfloat16


def pieces():
    out = []
    for k in range(KC):
        r = k * LAGS
        end = r + LAGS
        while r < end:
            p = r // PR
            stop = min(end, (p + 1) * PR)
            out.append((k, r - k * LAGS, stop - r, p, r - p * PR))
            r = stop
    return out


def onehot3(t):
    return (2 - t) * (1 - t) // 2, t * (2 - t), t * (t - 1) // 2


def rows(g):
    return pl.ds(16 * g, 16)


def encode(chunk, put, width, raw=None):
    m = jnp.abs(chunk(0))
    for g in range(1, G):
        m = jnp.maximum(m, jnp.abs(chunk(g)))
    m = jnp.max(m, axis=0, keepdims=True)
    e = jnp.ceil(jnp.log2(jnp.maximum(m, 1e-30)))
    scale = QMAX * jnp.exp2(-e)
    last = lax.broadcasted_iota(I32, (16, width), 0) == 15
    for g in range(G):
        q = jnp.round(chunk(g) * scale)
        if g == G - 1:
            q = jnp.where(last, jnp.broadcast_to(e, (16, width)), q)
        if raw is not None:
            raw.append(q)
            continue
        q = q.astype(I32).astype(jnp.int16)
        for i in range(width // 128):
            put(g, i, q[:, 128 * i : 128 * (i + 1)])


def fold(chunks, h, lane):
    out = []
    for g in range(HG):
        lo = chunks[g]
        hi = chunks[g + HG] if g + HG < G else jnp.zeros((16, 128), F32)
        if h:
            out.append(jnp.where(lane < 64, pltpu.roll(lo, 64, axis=1), hi))
        else:
            out.append(jnp.where(lane < 64, lo, pltpu.roll(hi, 64, axis=1)))
    return out


def decode_folded(get):
    lane = lax.broadcasted_iota(I32, (16, 128), 1)
    row = lax.broadcasted_iota(I32, (16, 128), 0)
    out = [get(g).astype(I32).astype(F32) for g in range(HG)]
    e = out[G - 1 - HG][15:16, :]
    e = jnp.where(lane[0:1] < 64, pltpu.roll(jnp.broadcast_to(e, (8, 128)), 64, axis=1)[0:1], e)
    scale = jnp.exp2(e) * (1.0 / QMAX)
    out = [v * scale for v in out]
    out[G - 1 - HG] = jnp.where((row == 15) & (lane >= 64), 0.0, out[G - 1 - HG])
    return out


def decode(get):
    tail = get(G - 1).astype(I32).astype(F32)
    scale = jnp.exp2(tail[15:16, :]) * (1.0 / QMAX)
    last = lax.broadcasted_iota(I32, (16, 128), 0) == 15
    out = [get(g).astype(I32).astype(F32) * scale for g in range(G - 1)]
    out.append(jnp.where(last, 0.0, tail * scale))
    return out


def main_kernel(
    field, idx_in, offs_in, fin, sums_o, tot_o, stat_o,
    idx, offs, sem_in, F, W, WF, OH, acc, NP, S1,
    s_far, r_far, s_n, r_n, s2f, r2f, s2n, r2n, s3, r3,
    iw, ipad, bs, g1, g2, fsum, sx_s, sx_r, tb1, sy_r, tb2, sz_r, tb3,
    sem_loc, sem_fs, sem_fr, sem_is, sem_ir, sem_gs, sem_g1, sem_g2,
    sem_far, sem_n, sem_2f, sem_2n, sem_3,
    sem_sfar, sem_sn, sem_s2f, sem_s2n, sem_s3, sem_ss, sem_sr, sem_os, sem_or, sem_bs, sem_br,
):
    X, Z, Y, C = (lax.axis_index(a) for a in TM)
    Q = (X * 4 + Z) * 4 + Y

    def peer(dx=0, dz=0, dy=0, dc=0):
        return {
            "x": (X + dx) % 4,
            "z": (Z + dz) % 4,
            "y": (Y + dy) % 4,
            "core": (C + dc) % 2,
        }

    def chip_peer(q, core):
        return {"x": q // 16, "z": (q // 4) % 4, "y": q % 4, "core": core}

    def along(t, delta, dc=0):
        f0, f1, f2 = onehot3(t)
        return peer(dx=f0 * delta, dy=f1 * delta, dz=f2 * delta, dc=dc)

    partner = peer(dc=1)
    xpeers = [(dx, dc) for dx in range(4) for dc in range(2) if dx or dc]
    yzpeers = [(dy, dz) for dy in range(4) for dz in range(4) if dy or dz]
    q_next, q_prev = (Q + 1) % N_CHIP, (Q + N_CHIP - 1) % N_CHIP

    copies = [
        pltpu.make_async_copy(idx_in, idx, sem_in.at[0]),
        pltpu.make_async_copy(offs_in, offs, sem_in.at[1]),
    ]
    for c in copies:
        c.start()

    barrier = pltpu.get_barrier_semaphore()

    def greet(device):
        pl.semaphore_signal(barrier, inc=1, device_id=device, device_id_type=MESH)

    for dx, dc in xpeers:
        greet(peer(dx=dx, dc=dc))
    for dy, dz in yzpeers:
        greet(peer(dy=dy, dz=dz))
    for d in range(1, 4):
        greet(peer(dy=d, dc=1))
        greet(peer(dz=d, dc=1))
    for q in (q_next, q_prev):
        for core in range(2):
            greet(chip_peer(q, core))

    def tile_of(slot, core):
        jx, jz, h = slot // 8, (slot // 2) % 4, slot % 2
        jy = 2 * h + (core + jx + jz) % 2
        return (jx * 4 + jz) * 4 + jy

    def columns(slot, core):
        return pl.ds(pl.multiple_of(tile_of(slot, core) * 128, 128), 128)

    own_days = pl.ds(pl.multiple_of(C * T_DEV, 16), T_DEV)

    eye = lax.broadcasted_iota(I32, (16, 128), 0) == lax.broadcasted_iota(I32, (16, 128), 1)

    def as_row(col):
        return jnp.sum(jnp.where(eye[:KC], col, 0.0), axis=0, keepdims=True)

    for c in copies:
        c.wait()
    mine = idx[...]
    me8, me16 = X * 2 + C, Y * 4 + Z
    g1[me8, 0:1, :] = as_row(jnp.sum(mine, axis=1, keepdims=True))
    g1[me8, 1:2, :] = as_row(jnp.sum(mine * mine, axis=1, keepdims=True))

    pl.semaphore_wait(barrier, 32)

    def remote(src, dst, ssem, rsem, device):
        return pltpu.make_async_remote_copy(
            src_ref=src, dst_ref=dst, send_sem=ssem, recv_sem=rsem,
            device_id=device, device_id_type=MESH,
        )

    g1c = [
        remote(g1.at[me8], g1.at[me8], sem_gs.at[i], sem_g1.at[i], peer(dx=dx, dc=dc))
        for i, (dx, dc) in enumerate(xpeers)
    ]
    for c in g1c:
        c.start()
    beside = (Q + N_CHIP + 2 * C - 1) % N_CHIP
    iwc = [remote(idx, iw.at[2], sem_is.at[2], sem_ir.at[2], partner)]
    for core in range(2):
        iwc.append(
            remote(
                idx, iw.at[1 - C], sem_is.at[core], sem_ir.at[1 - C], chip_peer(beside, core)
            )
        )
    for c in iwc:
        c.start()

    def share(begin, end):
        @pl.loop(begin, end)
        def _(s):
            remote(
                field.at[:, columns(s, 1 - C)], F.at[s, own_days, :], sem_fs, sem_fr, partner
            ).start()

    @pl.loop(0, 32)
    def _(s):
        pltpu.make_async_copy(
            field.at[:, columns(s, C)], F.at[s, own_days, :], sem_loc
        ).start()

    share(0, 10)

    @pl.loop(0, 32)
    def _(s):
        F[s, K:KP, :] = jnp.zeros((KP - K, 128), BF)

    for i in range(4):
        ipad[i] = jnp.zeros((16, 384), F32)
    ipad[3, 0:KC, 0:T_DEV] = mine

    for c in g1c:
        c.wait_recv()
    g = ((g1[0] + g1[1]) + (g1[2] + g1[3])) + ((g1[4] + g1[5]) + (g1[6] + g1[7]))
    g2[me16] = g
    g2c = [
        remote(
            g2.at[me16], g2.at[me16], sem_gs.at[7 + i], sem_g2.at[i], peer(dy=dy, dz=dz)
        )
        for i, (dy, dz) in enumerate(yzpeers)
    ]
    for c in g2c:
        c.start()
    share(10, 32)

    def cell_sums(start, fresh):
        @pl.loop(0, 32)
        def _(s):
            one = two = jnp.zeros((16, 128), F32)
            for g in range(T_DEV // 16):
                v = F[s, pl.ds(pl.multiple_of(start + 16 * g, 16), 16), :].astype(F32)
                one, two = one + v, two + v * v
            one = jnp.sum(one, axis=0, keepdims=True)
            two = jnp.sum(two, axis=0, keepdims=True)
            if not fresh:
                one, two = one + fsum[s, 0:1, :], two + fsum[s, 1:2, :]
            fsum[s, 0:1, :] = one
            fsum[s, 1:2, :] = two

    pltpu.make_async_copy(F.at[:, own_days, :], F.at[:, own_days, :], sem_loc).wait()
    cell_sums(C * T_DEV, True)
    for i in range(3):
        pltpu.make_async_copy(iw.at[i], iw.at[i], sem_ir.at[i]).wait()
        ipad[i, 0:KC, 0:T_DEV] = iw[i]
    pos = lax.broadcasted_iota(I32, (16, LC), 1)

    def placed(piece, at):
        wide = jnp.concatenate([piece, jnp.zeros((16, LC - 384), F32)], axis=1)
        return pltpu.roll(wide, at % LC, axis=1)

    mine, other = ipad[3], ipad[2]
    fc = C.astype(F32)
    w0 = mine * (1.0 - fc) + other * fc
    w1 = mine * fc + other * (1.0 - fc)
    series = jnp.where(
        pos < 64,
        placed(ipad[0], 64 - T_DEV),
        jnp.where(
            pos < 64 + T_DEV,
            placed(w0, 64),
            jnp.where(pos < 64 + K, placed(w1, 64 + T_DEV), placed(ipad[1], 64 + K)),
        ),
    )
    day = Q * K - 64 + pos
    series = jnp.where((day >= 0) & (day < TDAYS), series, FAR)
    kth = lax.broadcasted_iota(I32, (16, LC), 0)
    off = jnp.zeros((16, LC), I32)
    for k in range(KC):
        off = jnp.where(kth == k, offs[k], off)
    shifted = series
    for o in range(1, MAXOFF + 1):
        shifted = jnp.where(off == o, pltpu.roll(series, o, axis=1), shifted)
    tail = lax.broadcasted_iota(I32, (LAGS, KP), 1) < K
    lane_r = lax.broadcasted_iota(I32, (R, 128), 1)
    for p in range(3):
        lo = PR if p < 2 else KC * LAGS - 2 * PR
        WF[p, lo - lo % 8 : R, :] = jnp.full((R - lo + lo % 8, KP), FAR, F32)
        r = lax.broadcasted_iota(I32, (R, 128), 0) + PR * p
        OH[p] = jnp.where((r >= lane_r * LAGS) & (r < lane_r * LAGS + LAGS), 1.0, 0.0)
    todo = pieces()
    for k in range(KC):
        x = jnp.broadcast_to(shifted[k : k + 1, :], (64, LC))
        x = pltpu.roll(x, LC - 64 - MAXLAG, axis=1, stride=1, stride_axis=0)
        x = jnp.where(tail, x[:LAGS, :KP], FAR)
        for kk, a, n, p, b in todo:
            if kk == k:
                WF[p, b : b + n, :] = x[a : a + n, :]

    for c in g2c:
        c.wait_recv()
    g = g2[0]
    for i in range(1, 16):
        g = g + g2[i]
    mean_row = g[0:1, :] / float(TDAYS)
    stat_o[...] = jnp.zeros((8, 128), F32)
    stat_o[0:1, :] = mean_row
    stat_o[1:2, :] = g[1:2, :] / float(TDAYS) - mean_row * mean_row

    def center(p):
        col = jnp.sum(OH[p] * mean_row, axis=1, keepdims=True)
        for g in range(G):
            x = WF[p, rows(g), :]
            x = jnp.where(x > 0.5 * FAR, 0.0, x - col[16 * g : 16 * g + 16])
            W[p, rows(g), :] = x.astype(BF)

    pltpu.make_async_copy(F.at[:, own_days, :], F.at[:, own_days, :], sem_fr).wait()

    def part_coords(p):
        e0, e1, e2 = onehot3(p)
        return (
            e0 * X + e1 * Y + e2 * Z,
            e0 * Y + e1 * Z + e2 * X,
            e0 * Z + e1 * X + e2 * Y,
        )

    def slot_of(p, ja, jb, hd):
        e0, e1, e2 = onehot3(p)
        jd = 2 * hd + (C + ja + jb) % 2
        jx = e0 * ja + e1 * jd + e2 * jb
        jy = e0 * jb + e1 * ja + e2 * jd
        jz = e0 * jd + e1 * jb + e2 * ja
        return (jx * 4 + jz) * 2 + jy // 2

    sigma = 1 - 2 * C

    def order(b):
        return [(b + 2) % 4, (b + sigma + 4) % 4, (b - sigma + 4) % 4, b]

    def products(p, ja, b, h):
        wide = [F[slot_of(p, ja, jb, hd)] for hd in (h, 1 - h) for jb in order(b)]
        return jnp.dot(W[p], jnp.concatenate(wide, axis=1), preferred_element_type=F32)

    def settle(buf, at, sem):
        pltpu.make_async_copy(buf.at[at], buf.at[at], sem).wait()

    def send_pair(u, buf, at, half, dst, ssem, rsem):
        at = at + (pl.ds(2 * half, 2),)
        remote(buf.at[at], dst.at[at], ssem, rsem, along(u // 2, 1 - 2 * (u % 2))).start()

    n_piece = (pl.ds(0, 2), 2, 3)

    def send_n(u, hd, m):
        at = (u, hd, n_piece[m])
        remote(
            s_n.at[at], r_n.at[at], sem_sn, sem_n.at[u, hd, m], along(u // 2, 1 - 2 * (u % 2))
        ).start()

    @pl.loop(0, 3)
    def _(v):
        p = (v + C) % 3
        a, b, d = part_coords(p)
        center(p)
        acc[...] = products(p, (a + 2) % 4, b, 0)

        def put(g, i, tile):
            s_far[2 * p + i // 4, i % 4, rows(g), :] = tile

        encode(lambda g: acc[rows(g), :], put, 1024)
        for half in range(2):
            for hd in range(2):
                u = 2 * p + hd
                send_pair(u, s_far, (u,), half, r_far, sem_sfar, sem_far.at[u, half])

    cell_sums((1 - C) * T_DEV, False)
    tb1[...] = jnp.zeros((24, 128), F32)
    ones = jnp.ones((8, KP), BF)
    for p in range(3):
        t = lax.dot_general(ones, W[p], (((1,), (1,)), ((), ())), preferred_element_type=F32)
        tb1[16 + 2 * p : 17 + 2 * p, :] = t[0:1, 0:128]
        tb1[17 + 2 * p : 18 + 2 * p, 0:80] = t[0:1, 128:208]

    def gather_sums(dst, ja):
        for jb in range(4):
            for hd in range(2):
                s = slot_of(0, ja, jb, hd)
                i = 2 * jb + hd
                dst[i : i + 1, :] = fsum[s, 0:1, :]
                dst[8 + i : 9 + i, :] = fsum[s, 1:2, :]

    gather_sums(tb1, X)
    sxc = []
    for d in range(1, 4):
        to = sx_s.at[d - 1]
        to[16:24, :] = tb1[16:24, :]
        gather_sums(to, (X + d) % 4)
        c = remote(to, sx_r.at[d - 1], sem_ss.at[d - 1], sem_sr.at[d - 1], peer(dx=d))
        c.start()
        sxc.append(c)

    @pl.loop(0, 6)
    def _(v):
        u = (v + 2 * C) % 6
        p, dr = u // 2, u % 2
        a, b, d = part_coords(p)
        got = products(p, (a + 1 - 2 * dr + 4) % 4, b, 1 - dr)
        acc[:, 0:512] = got[:, 0:512]
        for i in range(4):
            NP[u, i] = got[:, 512 + 128 * i : 640 + 128 * i]

        def put(g, i, tile):
            s_n[u, 1 - dr, i, rows(g), :] = tile

        encode(lambda g: acc[rows(g), 0:512], put, 512)
        send_n(u, 1 - dr, 0)

    def near_half(half):
        @pl.loop(0, 6)
        def _(v):
            u = (v + 2 * C) % 6
            p, dr = u // 2, u % 2
            if half:
                send_n(u, 1 - dr, 1)
            settle(r_far, (u, pl.ds(2 * half, 2)), sem_far.at[u, half])
            for i in (2 * half, 2 * half + 1):
                got = decode(lambda g: r_far[u, i, rows(g), :])
                for g in range(G):
                    acc[rows(g), 128 * (i % 2) : 128 * (i % 2) + 128] = (
                        NP[u, i, rows(g), :] + got[g]
                    )

            def put(g, i, tile):
                s_n[u, dr, 2 * half + i, rows(g), :] = tile

            encode(lambda g: acc[rows(g), 0:256], put, 256)
            send_n(u, dr, half)
            if half:
                send_n(u, 1 - dr, 2)

    near_half(0)

    @pl.loop(0, 3)
    def _(p):
        a, b, d = part_coords(p)
        got = products(p, a, b, 0)
        for hd in range(2):
            for i in range(4):
                at = 512 * hd + 128 * i
                S1[2 * p + hd, i] = got[:, at : at + 128]

    near_half(1)

    for c in sxc:
        c.wait_recv()
    tb1[...] = (tb1[...] + sx_r[0]) + (sx_r[1] + sx_r[2])
    syc = [
        remote(tb1, sy_r.at[d - 1], sem_ss.at[2 + d], sem_sr.at[2 + d], peer(dy=d))
        for d in range(1, 4)
    ]
    for c in syc:
        c.start()

    def add_tile(w, i, *coded):
        got = [decode(lambda g, c=c: c(g)) for c in coded]
        for g in range(G):
            one = S1[w, i, rows(g), :]
            for c in got:
                one = one + c[g]
            S1[w, i, rows(g), :] = one

    def arrived(w, m):
        p, hd = w // 2, w % 2
        for dr in (1 - hd, hd):
            u = 2 * p + dr
            settle(r_n, (u, hd, n_piece[m]), sem_n.at[u, hd, m])
        for i in ((0, 1), (2,), (3,))[m]:
            add_tile(
                w, i,
                lambda g: r_n[2 * p, hd, i, rows(g), :],
                lambda g: r_n[2 * p + 1, hd, i, rows(g), :],
            )

    def encode1(w, i, buf, at):
        def put(g, t, tile):
            buf[at + (rows(g), slice(None))] = tile

        encode(lambda g: S1[w, i, rows(g), :], put, 128)

    @pl.loop(0, 6)
    def _(v):
        u = (v + 3 * C) % 6
        arrived(u, 0)
        encode1(u, 0, s2f, (u,))
        remote(
            s2f.at[u], r2f.at[u], sem_s2f, sem_2f.at[u],
            along((u // 2 + 1) % 3, 1 - 2 * (u % 2)),
        ).start()

    def near2(p, i, dr, hd):
        u = 2 * p + dr
        encode1(2 * p + hd, i, s2n, (u, hd))
        remote(
            s2n.at[u, hd], r2n.at[u, hd], sem_s2n, sem_2n.at[u, hd],
            along((p + 1) % 3, 1 - 2 * dr),
        ).start()

    def near2_sum(p, i, dr):
        u = 2 * p + dr
        settle(r2f, (u,), sem_2f.at[u])
        add_tile(u, i, lambda g: r2f[u, rows(g), :])
        near2(p, i, dr, dr)

    @pl.loop(0, 3)
    def _(p):
        near2(p, 1, C, 1 - C)

    @pl.loop(0, 6)
    def _(v):
        u = (v + 2 * C) % 6
        send_n(u, u % 2, 2)

    for c in syc:
        c.wait_recv()
    tb2[...] = (tb1[...] + sy_r[0]) + (sy_r[1] + sy_r[2])
    szc = [
        remote(tb2, sz_r.at[d - 1], sem_ss.at[5 + d], sem_sr.at[5 + d], peer(dz=d))
        for d in range(1, 4)
    ]
    for c in szc:
        c.start()

    @pl.loop(0, 3)
    def _(p):
        near2_sum(p, 1, C)

    @pl.loop(0, 3)
    def _(p):
        arrived(2 * p + C, 1)
        near2(p, 2, 1 - C, C)

    @pl.loop(0, 3)
    def _(p):
        arrived(2 * p + 1 - C, 1)
        near2_sum(p, 2, 1 - C)

    @pl.loop(0, 6)
    def _(w):
        arrived(w, 2)

    final = (C + X + Y + Z) % 2 == 0
    lane16 = lax.broadcasted_iota(I32, (16, 128), 1)

    @pl.loop(0, 3)
    def _(p):
        a, b, d = part_coords(p)
        for hd in range(2):
            w = 2 * p + hd
            settle(r2n, (2 * p + 1 - hd, hd), sem_2n.at[2 * p + 1 - hd, hd])
            settle(r2n, (2 * p + hd, hd), sem_2n.at[2 * p + hd, hd])
            add_tile(
                w, 3,
                lambda g: r2n[2 * p, hd, rows(g), :],
                lambda g: r2n[2 * p + 1, hd, rows(g), :],
            )

        def last_send(w, i, delta):
            raw = []
            encode(lambda g: S1[w, 3, rows(g), :], None, 128, raw)
            for h in range(2):
                for g, q in enumerate(fold(raw, h, lane16)):
                    s3[p, i, h, rows(g), :] = q.astype(I32).astype(jnp.int16)
                remote(
                    s3.at[p, i, h], r3.at[p, i], sem_s3.at[h], sem_3.at[p, i],
                    along((p + 2) % 3, delta, (h + C) % 2),
                ).start()

        @pl.when(final)
        def _():
            last_send(2 * p + 1 - d // 2, 2, 2)
            chunks = [S1[2 * p + d // 2, 3, rows(g), :] for g in range(G)]
            two = [fold(chunks, h, lane16) for h in range(2)]
            for g in range(HG):
                fin[p, rows(g), :] = jnp.where(C == 0, two[0][g], two[1][g])
                bs[p, rows(g), :] = jnp.where(C == 0, two[1][g], two[0][g])
            remote(bs.at[p], fin.at[p], sem_bs, sem_br.at[p], partner).start()

        @pl.when(jnp.logical_not(final))
        def _():
            for i, delta in enumerate((1, 3)):
                last_send(2 * p + ((d + delta) % 4) // 2, i, delta)

    for c in szc:
        c.wait_recv()
    total = (tb2[...] + sz_r[0]) + (sz_r[1] + sz_r[2])
    tot_o[...] = total[16:24, :]

    @pl.when(final)
    def _():
        i = 2 * Y + Z // 2
        tb3[...] = total
        sums_o[...] = jnp.zeros((8, 128), F32)
        sums_o[0:1, :] = tb3[pl.ds(i, 1), :]
        sums_o[1:2, :] = tb3[pl.ds(i + 8, 1), :]
        remote(sums_o, sums_o, sem_os, sem_or, partner).start()

    @pl.loop(0, 3)
    def _(p):
        @pl.when(jnp.logical_not(final))
        def _():
            settle(fin, (p,), sem_br.at[p])

        got = []
        for i in range(3):
            settle(r3, (p, i), sem_3.at[p, i])
            got.append(decode_folded(lambda g: r3[p, i, rows(g), :]))
        for g in range(HG):
            fin[p, rows(g), :] = (fin[p, rows(g), :] + got[0][g]) + (got[1][g] + got[2][g])

    @pl.when(final)
    def _():
        pltpu.make_async_copy(bs, bs, sem_bs).wait()
        pltpu.make_async_copy(sums_o, sums_o, sem_os).wait()
        for h in range(2):
            pltpu.make_async_copy(s3.at[:, 2, h], s3.at[:, 2, h], sem_s3.at[h]).wait()

    @pl.when(jnp.logical_not(final))
    def _():
        pltpu.make_async_copy(sums_o, sums_o, sem_or).wait()
        for h in range(2):
            pltpu.make_async_copy(s3.at[:, 0:2, h], s3.at[:, 0:2, h], sem_s3.at[h]).wait()

    for c in g1c + g2c + iwc + sxc + syc + szc:
        c.wait_send()
    pltpu.make_async_copy(F.at[:, own_days, :], F.at[:, own_days, :], sem_fs).wait()
    for buf, sem in ((s_far, sem_sfar), (s_n, sem_sn), (s2f, sem_s2f), (s2n, sem_s2n)):
        pltpu.make_async_copy(buf, buf, sem).wait()


def last_kernel(fin, sums, tot, stat, lag_list, mask, out, WS):
    core = lax.axis_index("core")
    n = float(TDAYS)
    half = 16 * HG
    both = sums[0:8, :]
    turned = pltpu.roll(both, 64, axis=1)
    low = lax.broadcasted_iota(I32, (8, 128), 1) < 64
    both = jnp.where(low == (core == 0), both, turned)
    mean_x = both[0:1, :] / n
    var_x = both[1:2, :] / n - mean_x * mean_x
    inv = 1.0 / (n * jnp.sqrt(var_x + 1e-6))
    row = lax.broadcasted_iota(I32, (half, 256), 0)
    col = lax.broadcasted_iota(I32, (half, 256), 1)
    left = lax.broadcasted_iota(I32, (half, 128), 1) < 64
    WS[KC * LAGS - 2 : KC * LAGS + 6, :] = jnp.zeros((8, 128), F32)
    for p in range(3):
        t = jnp.concatenate([tot[2 * p : 2 * p + 1, :], tot[2 * p + 1 : 2 * p + 2, :]], axis=1)
        t0 = jnp.sum(jnp.where(row == col, t, 0.0), axis=1, keepdims=True)
        t1 = jnp.sum(jnp.where(row + half == col, t, 0.0), axis=1, keepdims=True)
        x = (fin[p] - mean_x * jnp.where(left, t0, t1)) * inv
        m = min(PR, KC * LAGS - PR * p)
        WS[PR * p : PR * p + half, 0:64] = x[:, 0:64]
        WS[PR * p + half : PR * p + m, 0:64] = x[: m - half, 64:128]
    inv_i = 1.0 / jnp.sqrt(stat[1:2, :] + 1e-6)
    lags = lag_list[...].reshape(1, LAGS)
    place = lax.broadcasted_iota(I32, (64, LAGS), 0) - MAXLAG
    pick = (place == lags).astype(F32).astype(BF)
    pick = jnp.concatenate([pick, pick, pick], axis=0)
    r64 = lax.broadcasted_iota(I32, (64, 64), 0)
    c64 = lax.broadcasted_iota(I32, (64, 64), 1)
    sea = mask[...].reshape(1, 64).astype(F32)
    sea = jnp.sum(jnp.where(r64 == c64, sea, 0.0), axis=1, keepdims=True)
    for k in range(KC):
        x = WS[LAGS * k : LAGS * k + 64, 0:64]
        hi = x.astype(BF)
        x = x - hi.astype(F32)
        mid = x.astype(BF)
        lo = (x - mid.astype(F32)).astype(BF)
        y = lax.dot_general(
            jnp.concatenate([hi, mid, lo], axis=0), pick, (((0,), (0,)), ((), ())),
            preferred_element_type=F32,
        )
        out[k] = y * inv_i[:, k : k + 1] * sea


def shards(field, index, lag_list, index_offset, sea_mask):
    vmem = pl.BlockSpec(memory_space=pltpu.VMEM)
    i16 = jnp.int16
    dma = pltpu.SemaphoreType.DMA
    fin, sums, tot, stat = pl.pallas_call(
        main_kernel,
        out_shape=(
            jax.ShapeDtypeStruct((3, 16 * HG, 128), F32),
            jax.ShapeDtypeStruct((8, 128), F32),
            jax.ShapeDtypeStruct((8, 128), F32),
            jax.ShapeDtypeStruct((8, 128), F32),
        ),
        in_specs=[pl.BlockSpec(memory_space=pltpu.HBM)] * 3,
        out_specs=(vmem, vmem, vmem, vmem),
        scratch_shapes=[
            pltpu.VMEM((KC, T_DEV), F32),
            pltpu.SMEM((KC,), I32),
            dma((2,)),
            pltpu.VMEM((32, KP, 128), BF),
            pltpu.VMEM((3, R, KP), BF),
            pltpu.VMEM((3, R, KP), F32),
            pltpu.VMEM((3, R, 128), F32),
            pltpu.VMEM((R, 1024), F32),
            pltpu.VMEM((6, 4, R, 128), F32),
            pltpu.VMEM((6, 4, R, 128), F32),
            pltpu.VMEM((6, 4, R, 128), i16),
            pltpu.VMEM((6, 4, R, 128), i16),
            pltpu.VMEM((6, 2, 4, R, 128), i16),
            pltpu.VMEM((6, 2, 4, R, 128), i16),
            pltpu.VMEM((6, R, 128), i16),
            pltpu.VMEM((6, R, 128), i16),
            pltpu.VMEM((6, 2, R, 128), i16),
            pltpu.VMEM((6, 2, R, 128), i16),
            pltpu.VMEM((3, 3, 2, 16 * HG, 128), i16),
            pltpu.VMEM((3, 3, 16 * HG, 128), i16),
            pltpu.VMEM((3, KC, T_DEV), F32),
            pltpu.VMEM((4, 16, 384), F32),
            pltpu.VMEM((3, 16 * HG, 128), F32),
            pltpu.VMEM((8, 2, 128), F32),
            pltpu.VMEM((16, 2, 128), F32),
            pltpu.VMEM((32, 8, 128), F32),
            pltpu.VMEM((3, 24, 128), F32),
            pltpu.VMEM((3, 24, 128), F32),
            pltpu.VMEM((24, 128), F32),
            pltpu.VMEM((3, 24, 128), F32),
            pltpu.VMEM((24, 128), F32),
            pltpu.VMEM((3, 24, 128), F32),
            pltpu.VMEM((24, 128), F32),
            dma,
            dma,
            dma,
            dma((3,)),
            dma((3,)),
            dma((22,)),
            dma((7,)),
            dma((15,)),
            dma((6, 2)),
            dma((6, 2, 3)),
            dma((6,)),
            dma((6, 2)),
            dma((3, 3)),
            dma,
            dma,
            dma,
            dma,
            dma((2,)),
            dma((9,)),
            dma((9,)),
            dma,
            dma,
            dma,
            dma((3,)),
        ],
        compiler_params=pltpu.CompilerParams(
            collective_id=0, has_side_effects=True, vmem_limit_bytes=36 * 1024 * 1024
        ),
    )(*(pltpu.with_memory_space_constraint(v, pltpu.HBM) for v in (field, index.T, index_offset)))
    maps = pl.pallas_call(
        last_kernel,
        out_shape=jax.ShapeDtypeStruct((KC, CELLS // 128, LAGS), F32),
        in_specs=[vmem] * 6,
        out_specs=vmem,
        scratch_shapes=[pltpu.VMEM((616, 128), F32)],
        compiler_params=pltpu.CompilerParams(vmem_limit_bytes=8 * 1024 * 1024),
    )(fin, sums, tot, stat, lag_list, sea_mask)
    return jnp.transpose(maps, (1, 0, 2))


def solution(mesh):
    finer = Mesh(mesh.devices.reshape(4, 4, 4, 2), TM)
    return jax.shard_map(
        shards,
        mesh=finer,
        in_specs=(P(TM, None), P(TM, None), P(), P(), P(TM)),
        out_specs=P(TM, None, None),
        check_vma=False,
    )
```

```python
import jax
import jax.numpy as jnp
from jax import lax
from jax.experimental import pallas as pl
from jax.experimental.pallas import tpu as pltpu
from jax.sharding import Mesh
from jax.sharding import PartitionSpec as P

MAXLAG = 30
MAXOFF = 14
LAGS = 61
KC = 10
T_DEV = 336
N_CHIP = 64
CELLS = 8192
TDAYS = 43008
TM = ("x", "z", "y", "core")
MESH = pl.DeviceIdType.MESH

K = 2 * T_DEV
KP = 768
R = 208
PR = 204
G = R // 16
HG = 7
LC = 896
QMAX = 32000.0
FAR = 1e9
I32 = jnp.int32
F32 = jnp.float32
BF = jnp.bfloat16


def pieces():
    out = []
    for k in range(KC):
        r = k * LAGS
        end = r + LAGS
        while r < end:
            p = r // PR
            stop = min(end, (p + 1) * PR)
            out.append((k, r - k * LAGS, stop - r, p, r - p * PR))
            r = stop
    return out


def onehot3(t):
    return (2 - t) * (1 - t) // 2, t * (2 - t), t * (t - 1) // 2


def rows(g):
    return pl.ds(16 * g, 16)


def encode(chunk, put, width, raw=None):
    m = jnp.abs(chunk(0))
    for g in range(1, G):
        m = jnp.maximum(m, jnp.abs(chunk(g)))
    m = jnp.max(m, axis=0, keepdims=True)
    e = jnp.ceil(jnp.log2(jnp.maximum(m, 1e-30)))
    scale = QMAX * jnp.exp2(-e)
    last = lax.broadcasted_iota(I32, (16, width), 0) == 15
    for g in range(G):
        q = jnp.round(chunk(g) * scale)
        if g == G - 1:
            q = jnp.where(last, jnp.broadcast_to(e, (16, width)), q)
        if raw is not None:
            raw.append(q)
            continue
        q = q.astype(I32).astype(jnp.int16)
        for i in range(width // 128):
            put(g, i, q[:, 128 * i : 128 * (i + 1)])


def fold(chunks, h, lane):
    out = []
    for g in range(HG):
        lo = chunks[g]
        hi = chunks[g + HG] if g + HG < G else jnp.zeros((16, 128), F32)
        if h:
            out.append(jnp.where(lane < 64, pltpu.roll(lo, 64, axis=1), hi))
        else:
            out.append(jnp.where(lane < 64, lo, pltpu.roll(hi, 64, axis=1)))
    return out


def decode_folded(get):
    lane = lax.broadcasted_iota(I32, (16, 128), 1)
    row = lax.broadcasted_iota(I32, (16, 128), 0)
    out = [get(g).astype(I32).astype(F32) for g in range(HG)]
    e = out[G - 1 - HG][15:16, :]
    e = jnp.where(lane[0:1] < 64, pltpu.roll(jnp.broadcast_to(e, (8, 128)), 64, axis=1)[0:1], e)
    scale = jnp.exp2(e) * (1.0 / QMAX)
    out = [v * scale for v in out]
    out[G - 1 - HG] = jnp.where((row == 15) & (lane >= 64), 0.0, out[G - 1 - HG])
    return out


def decode(get):
    tail = get(G - 1).astype(I32).astype(F32)
    scale = jnp.exp2(tail[15:16, :]) * (1.0 / QMAX)
    last = lax.broadcasted_iota(I32, (16, 128), 0) == 15
    out = [get(g).astype(I32).astype(F32) * scale for g in range(G - 1)]
    out.append(jnp.where(last, 0.0, tail * scale))
    return out


def main_kernel(
    field, idx_in, offs_in, fin, sums_o, tot_o, stat_o,
    idx, offs, sem_in, F, W, WF, OH, acc, NP, S1,
    s_far, r_far, s_n, r_n, s2f, r2f, s2n, r2n, s3, r3,
    iw, ipad, bs, g1, g2, fsum, sx_s, sx_r, tb1, sy_s, sy_r, tb3,
    sem_loc, sem_fs, sem_fr, sem_is, sem_ir, sem_gs, sem_g1, sem_g2,
    sem_far, sem_n, sem_2f, sem_2n, sem_3,
    sem_sfar, sem_sn, sem_s2f, sem_s2n, sem_s3, sem_ss, sem_sr, sem_os, sem_or, sem_bs, sem_br,
):
    X, Z, Y, C = (lax.axis_index(a) for a in TM)
    Q = (X * 4 + Z) * 4 + Y

    def peer(dx=0, dz=0, dy=0, dc=0):
        return {
            "x": (X + dx) % 4,
            "z": (Z + dz) % 4,
            "y": (Y + dy) % 4,
            "core": (C + dc) % 2,
        }

    def chip_peer(q, core):
        return {"x": q // 16, "z": (q // 4) % 4, "y": q % 4, "core": core}

    def along(t, delta, dc=0):
        f0, f1, f2 = onehot3(t)
        return peer(dx=f0 * delta, dy=f1 * delta, dz=f2 * delta, dc=dc)

    partner = peer(dc=1)
    xpeers = [(dx, dc) for dx in range(4) for dc in range(2) if dx or dc]
    yzpeers = [(dy, dz) for dy in range(4) for dz in range(4) if dy or dz]
    q_next, q_prev = (Q + 1) % N_CHIP, (Q + N_CHIP - 1) % N_CHIP

    copies = [
        pltpu.make_async_copy(idx_in, idx, sem_in.at[0]),
        pltpu.make_async_copy(offs_in, offs, sem_in.at[1]),
    ]
    for c in copies:
        c.start()

    barrier = pltpu.get_barrier_semaphore()

    def greet(device):
        pl.semaphore_signal(barrier, inc=1, device_id=device, device_id_type=MESH)

    for dx, dc in xpeers:
        greet(peer(dx=dx, dc=dc))
    for dy, dz in yzpeers:
        greet(peer(dy=dy, dz=dz))
    for d in range(1, 4):
        greet(peer(dy=d, dc=1))
        greet(peer(dz=d, dc=1))
    for q in (q_next, q_prev):
        for core in range(2):
            greet(chip_peer(q, core))

    def tile_of(slot, core):
        jx, jz, h = slot // 8, (slot // 2) % 4, slot % 2
        jy = 2 * h + (core + jx + jz) % 2
        return (jx * 4 + jz) * 4 + jy

    def columns(slot, core):
        return pl.ds(pl.multiple_of(tile_of(slot, core) * 128, 128), 128)

    own_days = pl.ds(pl.multiple_of(C * T_DEV, 16), T_DEV)

    eye = lax.broadcasted_iota(I32, (16, 128), 0) == lax.broadcasted_iota(I32, (16, 128), 1)

    def as_row(col):
        return jnp.sum(jnp.where(eye[:KC], col, 0.0), axis=0, keepdims=True)

    for c in copies:
        c.wait()
    mine = idx[...]
    me8, me16 = X * 2 + C, Y * 4 + Z
    g1[me8, 0:1, :] = as_row(jnp.sum(mine, axis=1, keepdims=True))
    g1[me8, 1:2, :] = as_row(jnp.sum(mine * mine, axis=1, keepdims=True))

    pl.semaphore_wait(barrier, 32)

    def remote(src, dst, ssem, rsem, device):
        return pltpu.make_async_remote_copy(
            src_ref=src, dst_ref=dst, send_sem=ssem, recv_sem=rsem,
            device_id=device, device_id_type=MESH,
        )

    def settle(buf, at, sem):
        pltpu.make_async_copy(buf.at[at], buf.at[at], sem).wait()

    g1c = [
        remote(g1.at[me8], g1.at[me8], sem_gs.at[0], sem_g1, peer(dx=dx, dc=dc))
        for dx, dc in xpeers
    ]
    for c in g1c:
        c.start()
    beside = (Q + N_CHIP + 2 * C - 1) % N_CHIP
    iwc = [remote(idx, iw.at[2], sem_is, sem_ir, partner)]
    for core in range(2):
        iwc.append(
            remote(
                idx, iw.at[1 - C], sem_is, sem_ir, chip_peer(beside, core)
            )
        )
    for c in iwc:
        c.start()

    def share(begin, end):
        @pl.loop(begin, end)
        def _(s):
            remote(
                field.at[:, columns(s, 1 - C)], F.at[s, own_days, :], sem_fs, sem_fr, partner
            ).start()

    @pl.loop(0, 32)
    def _(s):
        pltpu.make_async_copy(
            field.at[:, columns(s, C)], F.at[s, own_days, :], sem_loc
        ).start()

    share(0, 10)

    @pl.loop(0, 32)
    def _(s):
        F[s, K:KP, :] = jnp.zeros((KP - K, 128), BF)

    for i in range(4):
        ipad[i] = jnp.zeros((16, 384), F32)
    ipad[3, 0:KC, 0:T_DEV] = mine

    settle(g1, (pl.ds(0, 7),), sem_g1)
    g = ((g1[0] + g1[1]) + (g1[2] + g1[3])) + ((g1[4] + g1[5]) + (g1[6] + g1[7]))
    g2[me16] = g
    g2c = [
        remote(
            g2.at[me16], g2.at[me16], sem_gs.at[1], sem_g2, peer(dy=dy, dz=dz)
        )
        for dy, dz in yzpeers
    ]
    for c in g2c:
        c.start()
    share(10, 32)

    def cell_sums():
        @pl.loop(0, 32)
        def _(s):
            one = two = jnp.zeros((16, 128), F32)
            for g in range(K // 16):
                v = F[s, rows(g), :].astype(F32)
                one, two = one + v, two + v * v
            fsum[s, 0:1, :] = jnp.sum(one, axis=0, keepdims=True)
            fsum[s, 1:2, :] = jnp.sum(two, axis=0, keepdims=True)

    pltpu.make_async_copy(F.at[:, own_days, :], F.at[:, own_days, :], sem_loc).wait()
    pltpu.make_async_copy(iw, iw, sem_ir).wait()
    for i in range(3):
        ipad[i, 0:KC, 0:T_DEV] = iw[i]
    pos = lax.broadcasted_iota(I32, (16, LC), 1)

    def placed(piece, at):
        wide = jnp.concatenate([piece, jnp.zeros((16, LC - 384), F32)], axis=1)
        return pltpu.roll(wide, at % LC, axis=1)

    mine, other = ipad[3], ipad[2]
    fc = C.astype(F32)
    w0 = mine * (1.0 - fc) + other * fc
    w1 = mine * fc + other * (1.0 - fc)
    series = jnp.where(
        pos < 64,
        placed(ipad[0], 64 - T_DEV),
        jnp.where(
            pos < 64 + T_DEV,
            placed(w0, 64),
            jnp.where(pos < 64 + K, placed(w1, 64 + T_DEV), placed(ipad[1], 64 + K)),
        ),
    )
    day = Q * K - 64 + pos
    series = jnp.where((day >= 0) & (day < TDAYS), series, FAR)
    kth = lax.broadcasted_iota(I32, (16, LC), 0)
    off = jnp.zeros((16, LC), I32)
    for k in range(KC):
        off = jnp.where(kth == k, offs[k], off)
    shifted = series
    for o in range(1, MAXOFF + 1):
        shifted = jnp.where(off == o, pltpu.roll(series, o, axis=1), shifted)
    tail = lax.broadcasted_iota(I32, (LAGS, KP), 1) < K
    lane_r = lax.broadcasted_iota(I32, (R, 128), 1)
    for p in range(3):
        lo = PR if p < 2 else KC * LAGS - 2 * PR
        WF[p, lo - lo % 8 : R, :] = jnp.full((R - lo + lo % 8, KP), FAR, F32)
        r = lax.broadcasted_iota(I32, (R, 128), 0) + PR * p
        OH[p] = jnp.where((r >= lane_r * LAGS) & (r < lane_r * LAGS + LAGS), 1.0, 0.0)
    todo = pieces()
    for k in range(KC):
        x = jnp.broadcast_to(shifted[k : k + 1, :], (64, LC))
        x = pltpu.roll(x, LC - 64 - MAXLAG, axis=1, stride=1, stride_axis=0)
        x = jnp.where(tail, x[:LAGS, :KP], FAR)
        for kk, a, n, p, b in todo:
            if kk == k:
                WF[p, b : b + n, :] = x[a : a + n, :]

    settle(g2, (pl.ds(0, 15),), sem_g2)
    g = g2[0]
    for i in range(1, 16):
        g = g + g2[i]
    mean_row = g[0:1, :] / float(TDAYS)
    stat_o[...] = jnp.zeros((8, 128), F32)
    stat_o[0:1, :] = mean_row
    stat_o[1:2, :] = g[1:2, :] / float(TDAYS) - mean_row * mean_row

    def center(p):
        col = jnp.sum(OH[p] * mean_row, axis=1, keepdims=True)
        for g in range(G):
            x = WF[p, rows(g), :]
            x = jnp.where(x > 0.5 * FAR, 0.0, x - col[16 * g : 16 * g + 16])
            W[p, rows(g), :] = x.astype(BF)

    pltpu.make_async_copy(F.at[:, own_days, :], F.at[:, own_days, :], sem_fr).wait()

    def part_coords(p):
        e0, e1, e2 = onehot3(p)
        return (
            e0 * X + e1 * Y + e2 * Z,
            e0 * Y + e1 * Z + e2 * X,
            e0 * Z + e1 * X + e2 * Y,
        )

    def slot_of(p, ja, jb, hd):
        e0, e1, e2 = onehot3(p)
        jd = 2 * hd + (C + ja + jb) % 2
        jx = e0 * ja + e1 * jd + e2 * jb
        jy = e0 * jb + e1 * ja + e2 * jd
        jz = e0 * jd + e1 * jb + e2 * ja
        return (jx * 4 + jz) * 2 + jy // 2

    sigma = 1 - 2 * C

    def order(b):
        return [(b + 2) % 4, (b + sigma + 4) % 4, (b - sigma + 4) % 4, b]

    def products(p, ja, b, h):
        wide = [F[slot_of(p, ja, jb, hd)] for hd in (h, 1 - h) for jb in order(b)]
        return jnp.dot(W[p], jnp.concatenate(wide, axis=1), preferred_element_type=F32)

    def send_n(u, hd, m):
        at = (u, hd, m)
        remote(
            s_n.at[at], r_n.at[at], sem_sn, sem_n.at[u // 2, hd, m], along(u // 2, 1 - 2 * (u % 2))
        ).start()

    def send_far(u, m):
        at = (u, m)
        remote(
            s_far.at[at], r_far.at[at], sem_sfar, sem_far.at[u, m],
            along(u // 2, 1 - 2 * (u % 2)),
        ).start()

    def turn(v):
        return v + C * (5 - 2 * v)

    @pl.loop(0, 3)
    def _(v):
        p = (v + C) % 3
        a, b, d = part_coords(p)
        center(p)
        acc[...] = products(p, (a + 2) % 4, b, 0)

        def put(g, i, tile):
            s_far[2 * p + i // 4, i % 4, rows(g), :] = tile

        encode(lambda g: acc[rows(g), :], put, 1024)
        for hd in range(2):
            for i in range(3):
                send_far(2 * p + hd, i)

    @pl.loop(0, 6)
    def _(v):
        u = turn(v)
        p, dr = u // 2, u % 2
        a, b, d = part_coords(p)
        got = products(p, (a + 1 - 2 * dr + 4) % 4, b, 1 - dr)
        acc[:, 0:512] = got[:, 0:512]
        for i in range(4):
            NP[u, i] = got[:, 512 + 128 * i : 640 + 128 * i]

        def put(g, i, tile):
            s_n[u, 1 - dr, i, rows(g), :] = tile

        encode(lambda g: acc[rows(g), 0:512], put, 512)
        send_n(u, 1 - dr, 0)
        send_n(u, 1 - dr, 1)

    def near_sum(i):
        @pl.loop(0, 6)
        def _(v):
            u = turn(v)
            dr = u % 2
            settle(r_far, (u, i), sem_far.at[u, i])
            got = decode(lambda g: r_far[u, i, rows(g), :])
            for g in range(G):
                acc[rows(g), 0:128] = NP[u, i, rows(g), :] + got[g]

            def put(g, t, tile):
                s_n[u, dr, i, rows(g), :] = tile

            encode(lambda g: acc[rows(g), 0:128], put, 128)
            send_n(u, dr, i)
            if i == 0:
                send_far(u, 3)
            if 0 < i < 3:
                send_n(u, 1 - dr, i + 1)

    near_sum(0)
    near_sum(1)

    @pl.loop(0, 3)
    def _(p):
        a, b, d = part_coords(p)
        got = products(p, a, b, 0)
        for hd in range(2):
            for i in range(4):
                at = 512 * hd + 128 * i
                S1[2 * p + hd, i] = got[:, at : at + 128]

    def add_tile(w, i, *coded):
        got = [decode(lambda g, c=c: c(g)) for c in coded]
        for g in range(G):
            one = S1[w, i, rows(g), :]
            for c in got:
                one = one + c[g]
            S1[w, i, rows(g), :] = one

    def arrived(w, i):
        p, hd = w // 2, w % 2
        settle(r_n, (pl.ds(2 * p, 2), hd, i), sem_n.at[p, hd, i])
        add_tile(
            w, i,
            lambda g: r_n[2 * p, hd, i, rows(g), :],
            lambda g: r_n[2 * p + 1, hd, i, rows(g), :],
        )

    def encode1(w, i, buf, at):
        def put(g, t, tile):
            buf[at + (rows(g), slice(None))] = tile

        encode(lambda g: S1[w, i, rows(g), :], put, 128)

    cell_sums()
    tb1[...] = jnp.zeros((24, 128), F32)
    ones = jnp.ones((8, KP), BF)
    for p in range(3):
        t = lax.dot_general(ones, W[p], (((1,), (1,)), ((), ())), preferred_element_type=F32)
        tb1[16 + 2 * p : 17 + 2 * p, :] = t[0:1, 0:128]
        tb1[17 + 2 * p : 18 + 2 * p, 0:80] = t[0:1, 128:208]

    def gather_sums(dst, ja):
        for jb in range(4):
            for hd in range(2):
                s = slot_of(0, ja, jb, hd)
                i = 2 * jb + hd
                dst[i : i + 1, :] = fsum[s, 0:1, :]
                dst[8 + i : 9 + i, :] = fsum[s, 1:2, :]

    gather_sums(tb1, X)
    for d in range(1, 4):
        to = sx_s.at[d - 1]
        to[16:24, :] = tb1[16:24, :]
        gather_sums(to, (X + d) % 4)
        c = remote(to, sx_r.at[d - 1], sem_ss.at[0], sem_sr.at[0], peer(dx=d))
        c.start()

    @pl.loop(0, 6)
    def _(v):
        u = (v + 3 * C) % 6
        arrived(u, 0)
        encode1(u, 0, s2f, (u,))
        remote(
            s2f.at[u], r2f.at[u], sem_s2f, sem_2f.at[u],
            along((u // 2 + 1) % 3, 1 - 2 * (u % 2)),
        ).start()

    def near2(p, i, dr, hd):
        u = 2 * p + dr
        encode1(2 * p + hd, i, s2n, (u, hd))
        remote(
            s2n.at[u, hd], r2n.at[u, hd], sem_s2n, sem_2n.at[p, hd],
            along((p + 1) % 3, 1 - 2 * dr),
        ).start()

    def near2_sum(p, i, dr):
        u = 2 * p + dr
        settle(r2f, (u,), sem_2f.at[u])
        add_tile(u, i, lambda g: r2f[u, rows(g), :])
        near2(p, i, dr, dr)

    near_sum(2)
    near_sum(3)

    @pl.loop(0, 3)
    def _(p):
        arrived(2 * p + 1 - C, 1)
        near2(p, 1, C, 1 - C)

    @pl.loop(0, 3)
    def _(p):
        arrived(2 * p + C, 1)
        near2_sum(p, 1, C)

    pltpu.make_async_copy(sx_r, sx_r, sem_sr.at[0]).wait()
    tb1[...] = (tb1[...] + sx_r[0]) + (sx_r[1] + sx_r[2])

    def side_rows(dst, y, z):
        i = 2 * y + z // 2
        dst[0:1, :] = tb1[pl.ds(i, 1), :]
        dst[1:2, :] = tb1[pl.ds(8 + i, 1), :]
        dst[2:8, :] = tb1[16:22, :]

    for n, (dy, dz) in enumerate(yzpeers):
        side_rows(sy_s.at[n], (Y + dy) % 4, (Z + dz) % 4)
        c = remote(
            sy_s.at[n], sy_r.at[n], sem_ss.at[1], sem_sr.at[1], peer(dy=dy, dz=dz)
        )
        c.start()

    @pl.loop(0, 3)
    def _(p):
        arrived(2 * p + C, 2)
        near2(p, 2, 1 - C, C)

    @pl.loop(0, 3)
    def _(p):
        arrived(2 * p + 1 - C, 2)
        near2_sum(p, 2, 1 - C)

    @pl.loop(0, 6)
    def _(w):
        arrived(w, 3)

    final = (C + X + Y + Z) % 2 == 0
    lane16 = lax.broadcasted_iota(I32, (16, 128), 1)

    @pl.loop(0, 3)
    def _(p):
        a, b, d = part_coords(p)
        for hd in range(2):
            w = 2 * p + hd
            settle(r2n, (pl.ds(2 * p, 2), hd), sem_2n.at[p, hd])
            add_tile(
                w, 3,
                lambda g: r2n[2 * p, hd, rows(g), :],
                lambda g: r2n[2 * p + 1, hd, rows(g), :],
            )

        def last_send(w, i, delta):
            raw = []
            encode(lambda g: S1[w, 3, rows(g), :], None, 128, raw)
            for h in range(2):
                for g, q in enumerate(fold(raw, h, lane16)):
                    s3[p, i, h, rows(g), :] = q.astype(I32).astype(jnp.int16)
                remote(
                    s3.at[p, i, h], r3.at[p, i], sem_s3.at[h], sem_3.at[p],
                    along((p + 2) % 3, delta, (h + C) % 2),
                ).start()

        @pl.when(final)
        def _():
            last_send(2 * p + 1 - d // 2, 2, 2)
            chunks = [S1[2 * p + d // 2, 3, rows(g), :] for g in range(G)]
            two = [fold(chunks, h, lane16) for h in range(2)]
            for g in range(HG):
                fin[p, rows(g), :] = jnp.where(C == 0, two[0][g], two[1][g])
                bs[p, rows(g), :] = jnp.where(C == 0, two[1][g], two[0][g])
            remote(bs.at[p], fin.at[p], sem_bs, sem_br.at[p], partner).start()

        @pl.when(jnp.logical_not(final))
        def _():
            for i, delta in enumerate((1, 3)):
                last_send(2 * p + ((d + delta) % 4) // 2, i, delta)

    side_rows(tb3, Y, Z)
    total = tb3[...]
    pltpu.make_async_copy(sy_r, sy_r, sem_sr.at[1]).wait()
    for n in range(15):
        total = total + sy_r[n]
    tot_o[...] = total

    @pl.when(final)
    def _():
        sums_o[...] = total
        remote(sums_o, sums_o, sem_os, sem_or, partner).start()

    @pl.loop(0, 3)
    def _(p):
        @pl.when(jnp.logical_not(final))
        def _():
            settle(fin, (p,), sem_br.at[p])

        settle(r3, (p,), sem_3.at[p])
        got = []
        for i in range(3):
            got.append(decode_folded(lambda g: r3[p, i, rows(g), :]))
        for g in range(HG):
            fin[p, rows(g), :] = (fin[p, rows(g), :] + got[0][g]) + (got[1][g] + got[2][g])

    @pl.when(final)
    def _():
        pltpu.make_async_copy(bs, bs, sem_bs).wait()
        pltpu.make_async_copy(sums_o, sums_o, sem_os).wait()
        for h in range(2):
            pltpu.make_async_copy(s3.at[:, 2, h], s3.at[:, 2, h], sem_s3.at[h]).wait()

    @pl.when(jnp.logical_not(final))
    def _():
        pltpu.make_async_copy(sums_o, sums_o, sem_or).wait()
        for h in range(2):
            pltpu.make_async_copy(s3.at[:, 0:2, h], s3.at[:, 0:2, h], sem_s3.at[h]).wait()

    settle(g1, (pl.ds(0, 7),), sem_gs.at[0])
    settle(g2, (pl.ds(0, 15),), sem_gs.at[1])
    pltpu.make_async_copy(iw, iw, sem_is).wait()
    pltpu.make_async_copy(sx_s, sx_s, sem_ss.at[0]).wait()
    pltpu.make_async_copy(sy_s, sy_s, sem_ss.at[1]).wait()
    pltpu.make_async_copy(F.at[:, own_days, :], F.at[:, own_days, :], sem_fs).wait()
    for buf, sem in ((s_far, sem_sfar), (s_n, sem_sn), (s2f, sem_s2f), (s2n, sem_s2n)):
        pltpu.make_async_copy(buf, buf, sem).wait()


def last_kernel(fin, sums, tot, stat, lag_list, mask, out_hbm, WS, out, sem):
    core = lax.axis_index("core")
    n = float(TDAYS)
    half = 16 * HG
    both = sums[0:8, :]
    turned = pltpu.roll(both, 64, axis=1)
    low = lax.broadcasted_iota(I32, (8, 128), 1) < 64
    both = jnp.where(low == (core == 0), both, turned)
    mean_x = both[0:1, :] / n
    var_x = both[1:2, :] / n - mean_x * mean_x
    inv = 1.0 / (n * jnp.sqrt(var_x + 1e-6))
    row = lax.broadcasted_iota(I32, (half, 256), 0)
    col = lax.broadcasted_iota(I32, (half, 256), 1)
    left = lax.broadcasted_iota(I32, (half, 128), 1) < 64
    WS[KC * LAGS - 2 : KC * LAGS + 6, :] = jnp.zeros((8, 128), F32)
    for p in range(3):
        t = jnp.concatenate([tot[2 * p + 2 : 2 * p + 3, :], tot[2 * p + 3 : 2 * p + 4, :]], axis=1)
        t0 = jnp.sum(jnp.where(row == col, t, 0.0), axis=1, keepdims=True)
        t1 = jnp.sum(jnp.where(row + half == col, t, 0.0), axis=1, keepdims=True)
        x = (fin[p] - mean_x * jnp.where(left, t0, t1)) * inv
        m = min(PR, KC * LAGS - PR * p)
        WS[PR * p : PR * p + half, 0:64] = x[:, 0:64]
        WS[PR * p + half : PR * p + m, 0:64] = x[: m - half, 64:128]
    inv_i = 1.0 / jnp.sqrt(stat[1:2, :] + 1e-6)
    lags = lag_list[...].reshape(1, LAGS)
    place = lax.broadcasted_iota(I32, (64, LAGS), 0) - MAXLAG
    pick = (place == lags).astype(F32).astype(BF)
    pick = jnp.concatenate([pick, pick, pick], axis=0)
    r64 = lax.broadcasted_iota(I32, (64, 64), 0)
    c64 = lax.broadcasted_iota(I32, (64, 64), 1)
    sea = mask[...].reshape(1, 64).astype(F32)
    sea = jnp.sum(jnp.where(r64 == c64, sea, 0.0), axis=1, keepdims=True)
    for k in range(KC):
        x = WS[LAGS * k : LAGS * k + 64, 0:64]
        hi = x.astype(BF)
        x = x - hi.astype(F32)
        mid = x.astype(BF)
        lo = (x - mid.astype(F32)).astype(BF)
        y = lax.dot_general(
            jnp.concatenate([hi, mid, lo], axis=0), pick, (((0,), (0,)), ((), ())),
            preferred_element_type=F32,
        )
        out[k] = y * inv_i[:, k : k + 1] * sea
        pltpu.make_async_copy(out.at[k], out_hbm.at[k], sem.at[k]).start()
    for k in range(KC):
        pltpu.make_async_copy(out.at[k], out_hbm.at[k], sem.at[k]).wait()


def shards(field, index, lag_list, index_offset, sea_mask):
    vmem = pl.BlockSpec(memory_space=pltpu.VMEM)
    i16 = jnp.int16
    dma = pltpu.SemaphoreType.DMA
    fin, sums, tot, stat = pl.pallas_call(
        main_kernel,
        out_shape=(
            jax.ShapeDtypeStruct((3, 16 * HG, 128), F32),
            jax.ShapeDtypeStruct((8, 128), F32),
            jax.ShapeDtypeStruct((8, 128), F32),
            jax.ShapeDtypeStruct((8, 128), F32),
        ),
        in_specs=[pl.BlockSpec(memory_space=pltpu.HBM)] * 3,
        out_specs=(vmem, vmem, vmem, vmem),
        scratch_shapes=[
            pltpu.VMEM((KC, T_DEV), F32),
            pltpu.SMEM((KC,), I32),
            dma((2,)),
            pltpu.VMEM((32, KP, 128), BF),
            pltpu.VMEM((3, R, KP), BF),
            pltpu.VMEM((3, R, KP), F32),
            pltpu.VMEM((3, R, 128), F32),
            pltpu.VMEM((R, 1024), F32),
            pltpu.VMEM((6, 4, R, 128), F32),
            pltpu.VMEM((6, 4, R, 128), F32),
            pltpu.VMEM((6, 4, R, 128), i16),
            pltpu.VMEM((6, 4, R, 128), i16),
            pltpu.VMEM((6, 2, 4, R, 128), i16),
            pltpu.VMEM((6, 2, 4, R, 128), i16),
            pltpu.VMEM((6, R, 128), i16),
            pltpu.VMEM((6, R, 128), i16),
            pltpu.VMEM((6, 2, R, 128), i16),
            pltpu.VMEM((6, 2, R, 128), i16),
            pltpu.VMEM((3, 3, 2, 16 * HG, 128), i16),
            pltpu.VMEM((3, 3, 16 * HG, 128), i16),
            pltpu.VMEM((3, KC, T_DEV), F32),
            pltpu.VMEM((4, 16, 384), F32),
            pltpu.VMEM((3, 16 * HG, 128), F32),
            pltpu.VMEM((8, 2, 128), F32),
            pltpu.VMEM((16, 2, 128), F32),
            pltpu.VMEM((32, 8, 128), F32),
            pltpu.VMEM((3, 24, 128), F32),
            pltpu.VMEM((3, 24, 128), F32),
            pltpu.VMEM((24, 128), F32),
            pltpu.VMEM((15, 8, 128), F32),
            pltpu.VMEM((15, 8, 128), F32),
            pltpu.VMEM((8, 128), F32),
            dma,
            dma,
            dma,
            dma,
            dma,
            dma((2,)),
            dma,
            dma,
            dma((6, 4)),
            dma((3, 2, 4)),
            dma((6,)),
            dma((3, 2)),
            dma((3,)),
            dma,
            dma,
            dma,
            dma,
            dma((2,)),
            dma((2,)),
            dma((2,)),
            dma,
            dma,
            dma,
            dma((3,)),
        ],
        compiler_params=pltpu.CompilerParams(
            collective_id=0, has_side_effects=True, vmem_limit_bytes=36 * 1024 * 1024
        ),
    )(*(pltpu.with_memory_space_constraint(v, pltpu.HBM) for v in (field, index.T, index_offset)))
    maps = pl.pallas_call(
        last_kernel,
        out_shape=jax.ShapeDtypeStruct((KC, CELLS // 128, LAGS), F32),
        in_specs=[vmem] * 6,
        out_specs=pl.BlockSpec(memory_space=pltpu.HBM),
        scratch_shapes=[
            pltpu.VMEM((616, 128), F32),
            pltpu.VMEM((KC, CELLS // 128, LAGS), F32),
            dma((KC,)),
        ],
        compiler_params=pltpu.CompilerParams(vmem_limit_bytes=8 * 1024 * 1024),
    )(fin, sums, tot, stat, lag_list, sea_mask)
    return jnp.transpose(maps, (1, 0, 2))


def solution(mesh):
    finer = Mesh(mesh.devices.reshape(4, 4, 4, 2), TM)
    return jax.shard_map(
        shards,
        mesh=finer,
        in_specs=(P(TM, None), P(TM, None), P(), P(), P(TM)),
        out_specs=P(TM, None, None),
        check_vma=False,
    )
```

```python
import jax
import jax.numpy as jnp
from jax import lax
from jax.experimental import pallas as pl
from jax.experimental.pallas import tpu as pltpu
from jax.sharding import Mesh
from jax.sharding import PartitionSpec as P

MAXLAG = 30
MAXOFF = 14
LAGS = 61
KC = 10
T_DEV = 336
N_CHIP = 64
CELLS = 8192
TDAYS = 43008
TM = ("x", "z", "y", "core")
MESH = pl.DeviceIdType.MESH

K = 2 * T_DEV
KP = 768
R = 208
PR = 204
G = R // 16
HG = 7
LC = 896
QMAX = 32000.0
FAR = 1e9
I32 = jnp.int32
F32 = jnp.float32
BF = jnp.bfloat16


def pieces():
    out = []
    for k in range(KC):
        r = k * LAGS
        end = r + LAGS
        while r < end:
            p = r // PR
            stop = min(end, (p + 1) * PR)
            out.append((k, r - k * LAGS, stop - r, p, r - p * PR))
            r = stop
    return out


def onehot3(t):
    return (2 - t) * (1 - t) // 2, t * (2 - t), t * (t - 1) // 2


def rows(g):
    return pl.ds(16 * g, 16)


def encode(chunk, put, width, raw=None):
    m = jnp.abs(chunk(0))
    for g in range(1, G):
        m = jnp.maximum(m, jnp.abs(chunk(g)))
    m = jnp.max(m, axis=0, keepdims=True)
    e = jnp.ceil(jnp.log2(jnp.maximum(m, 1e-30)))
    scale = QMAX * jnp.exp2(-e)
    last = lax.broadcasted_iota(I32, (16, width), 0) == 15
    for g in range(G):
        q = jnp.round(chunk(g) * scale)
        if g == G - 1:
            q = jnp.where(last, jnp.broadcast_to(e, (16, width)), q)
        if raw is not None:
            raw.append(q)
            continue
        q = q.astype(I32).astype(jnp.int16)
        for i in range(width // 128):
            put(g, i, q[:, 128 * i : 128 * (i + 1)])


def fold(chunks, h, lane):
    out = []
    for g in range(HG):
        lo = chunks[g]
        hi = chunks[g + HG] if g + HG < G else jnp.zeros((16, 128), F32)
        if h:
            out.append(jnp.where(lane < 64, pltpu.roll(lo, 64, axis=1), hi))
        else:
            out.append(jnp.where(lane < 64, lo, pltpu.roll(hi, 64, axis=1)))
    return out


def decode_folded(get):
    lane = lax.broadcasted_iota(I32, (16, 128), 1)
    row = lax.broadcasted_iota(I32, (16, 128), 0)
    out = [get(g).astype(I32).astype(F32) for g in range(HG)]
    e = out[G - 1 - HG][15:16, :]
    e = jnp.where(lane[0:1] < 64, pltpu.roll(jnp.broadcast_to(e, (8, 128)), 64, axis=1)[0:1], e)
    scale = jnp.exp2(e) * (1.0 / QMAX)
    out = [v * scale for v in out]
    out[G - 1 - HG] = jnp.where((row == 15) & (lane >= 64), 0.0, out[G - 1 - HG])
    return out


def decode(get):
    tail = get(G - 1).astype(I32).astype(F32)
    scale = jnp.exp2(tail[15:16, :]) * (1.0 / QMAX)
    last = lax.broadcasted_iota(I32, (16, 128), 0) == 15
    out = [get(g).astype(I32).astype(F32) * scale for g in range(G - 1)]
    out.append(jnp.where(last, 0.0, tail * scale))
    return out


def main_kernel(
    field, idx_in, offs_in, fin, sums_o, tot_o, stat_o,
    idx, offs, sem_in, F, W, WF, OH, acc, NP, S1,
    s_far, r_far, s_n, r_n, s2f, r2f, s2n, r2n, s3, r3,
    iw, ipad, bs, g1, g2, fsum, sx_s, sx_r, tb1, sy_s, sy_r, tb3,
    sem_loc, sem_fs, sem_fr, sem_is, sem_ir, sem_gs, sem_g1, sem_g2,
    sem_far, sem_n, sem_2f, sem_2n, sem_3,
    sem_sfar, sem_sn, sem_s2f, sem_s2n, sem_s3, sem_ss, sem_sr, sem_os, sem_or, sem_bs, sem_br,
):
    X, Z, Y, C = (lax.axis_index(a) for a in TM)
    Q = (X * 4 + Z) * 4 + Y

    def peer(dx=0, dz=0, dy=0, dc=0):
        return {
            "x": (X + dx) % 4,
            "z": (Z + dz) % 4,
            "y": (Y + dy) % 4,
            "core": (C + dc) % 2,
        }

    def chip_peer(q, core):
        return {"x": q // 16, "z": (q // 4) % 4, "y": q % 4, "core": core}

    def along(t, delta, dc=0):
        f0, f1, f2 = onehot3(t)
        return peer(dx=f0 * delta, dy=f1 * delta, dz=f2 * delta, dc=dc)

    partner = peer(dc=1)
    xpeers = [(dx, dc) for dx in range(4) for dc in range(2) if dx or dc]
    yzpeers = [(dy, dz) for dy in range(4) for dz in range(4) if dy or dz]
    q_next, q_prev = (Q + 1) % N_CHIP, (Q + N_CHIP - 1) % N_CHIP

    copies = [
        pltpu.make_async_copy(idx_in, idx, sem_in.at[0]),
        pltpu.make_async_copy(offs_in, offs, sem_in.at[1]),
    ]
    for c in copies:
        c.start()

    barrier = pltpu.get_barrier_semaphore()

    def greet(device):
        pl.semaphore_signal(barrier, inc=1, device_id=device, device_id_type=MESH)

    for dx, dc in xpeers:
        greet(peer(dx=dx, dc=dc))
    for dy, dz in yzpeers:
        greet(peer(dy=dy, dz=dz))
    for d in range(1, 4):
        greet(peer(dy=d, dc=1))
        greet(peer(dz=d, dc=1))
    for q in (q_next, q_prev):
        for core in range(2):
            greet(chip_peer(q, core))

    def tile_of(slot, core):
        jx, jz, h = slot // 8, (slot // 2) % 4, slot % 2
        jy = 2 * h + (core + jx + jz) % 2
        return (jx * 4 + jz) * 4 + jy

    def columns(slot, core):
        return pl.ds(pl.multiple_of(tile_of(slot, core) * 128, 128), 128)

    own_days = pl.ds(pl.multiple_of(C * T_DEV, 16), T_DEV)

    eye = lax.broadcasted_iota(I32, (16, 128), 0) == lax.broadcasted_iota(I32, (16, 128), 1)

    def as_row(col):
        return jnp.sum(jnp.where(eye[:KC], col, 0.0), axis=0, keepdims=True)

    for c in copies:
        c.wait()
    mine = idx[...]
    me8, me16 = X * 2 + C, Y * 4 + Z
    g1[me8, 0:1, :] = as_row(jnp.sum(mine, axis=1, keepdims=True))
    g1[me8, 1:2, :] = as_row(jnp.sum(mine * mine, axis=1, keepdims=True))

    pl.semaphore_wait(barrier, 32)

    def remote(src, dst, ssem, rsem, device):
        return pltpu.make_async_remote_copy(
            src_ref=src, dst_ref=dst, send_sem=ssem, recv_sem=rsem,
            device_id=device, device_id_type=MESH,
        )

    def settle(buf, at, sem):
        pltpu.make_async_copy(buf.at[at], buf.at[at], sem).wait()

    g1c = [
        remote(g1.at[me8], g1.at[me8], sem_gs.at[0], sem_g1, peer(dx=dx, dc=dc))
        for dx, dc in xpeers
    ]
    for c in g1c:
        c.start()
    beside = (Q + N_CHIP + 2 * C - 1) % N_CHIP
    iwc = [remote(idx, iw.at[2], sem_is, sem_ir, partner)]
    for core in range(2):
        iwc.append(
            remote(
                idx, iw.at[1 - C], sem_is, sem_ir, chip_peer(beside, core)
            )
        )
    for c in iwc:
        c.start()

    def share(begin, end):
        @pl.loop(begin, end)
        def _(s):
            remote(
                field.at[:, columns(s, 1 - C)], F.at[s, own_days, :], sem_fs, sem_fr, partner
            ).start()

    @pl.loop(0, 32)
    def _(s):
        pltpu.make_async_copy(
            field.at[:, columns(s, C)], F.at[s, own_days, :], sem_loc
        ).start()

    share(0, 20)

    @pl.loop(0, 32)
    def _(s):
        F[s, K:KP, :] = jnp.zeros((KP - K, 128), BF)

    for i in range(4):
        ipad[i] = jnp.zeros((16, 384), F32)
    ipad[3, 0:KC, 0:T_DEV] = mine

    settle(g1, (pl.ds(0, 7),), sem_g1)
    g = ((g1[0] + g1[1]) + (g1[2] + g1[3])) + ((g1[4] + g1[5]) + (g1[6] + g1[7]))
    g2[me16] = g
    g2c = [
        remote(
            g2.at[me16], g2.at[me16], sem_gs.at[1], sem_g2, peer(dy=dy, dz=dz)
        )
        for dy, dz in yzpeers
    ]
    for c in g2c:
        c.start()
    share(20, 32)

    def cell_sums():
        @pl.loop(0, 32)
        def _(s):
            one = two = jnp.zeros((16, 128), F32)
            for g in range(K // 16):
                v = F[s, rows(g), :].astype(F32)
                one, two = one + v, two + v * v
            fsum[s, 0:1, :] = jnp.sum(one, axis=0, keepdims=True)
            fsum[s, 1:2, :] = jnp.sum(two, axis=0, keepdims=True)

    pltpu.make_async_copy(F.at[:, own_days, :], F.at[:, own_days, :], sem_loc).wait()
    pltpu.make_async_copy(iw, iw, sem_ir).wait()
    for i in range(3):
        ipad[i, 0:KC, 0:T_DEV] = iw[i]
    pos = lax.broadcasted_iota(I32, (16, LC), 1)

    def placed(piece, at):
        wide = jnp.concatenate([piece, jnp.zeros((16, LC - 384), F32)], axis=1)
        return pltpu.roll(wide, at % LC, axis=1)

    mine, other = ipad[3], ipad[2]
    fc = C.astype(F32)
    w0 = mine * (1.0 - fc) + other * fc
    w1 = mine * fc + other * (1.0 - fc)
    series = jnp.where(
        pos < 64,
        placed(ipad[0], 64 - T_DEV),
        jnp.where(
            pos < 64 + T_DEV,
            placed(w0, 64),
            jnp.where(pos < 64 + K, placed(w1, 64 + T_DEV), placed(ipad[1], 64 + K)),
        ),
    )
    day = Q * K - 64 + pos
    series = jnp.where((day >= 0) & (day < TDAYS), series, FAR)
    kth = lax.broadcasted_iota(I32, (16, LC), 0)
    off = jnp.zeros((16, LC), I32)
    for k in range(KC):
        off = jnp.where(kth == k, offs[k], off)
    shifted = series
    for o in range(1, MAXOFF + 1):
        shifted = jnp.where(off == o, pltpu.roll(series, o, axis=1), shifted)
    tail = lax.broadcasted_iota(I32, (LAGS, KP), 1) < K
    lane_r = lax.broadcasted_iota(I32, (R, 128), 1)
    for p in range(3):
        lo = PR if p < 2 else KC * LAGS - 2 * PR
        WF[p, lo - lo % 8 : R, :] = jnp.full((R - lo + lo % 8, KP), FAR, F32)
        r = lax.broadcasted_iota(I32, (R, 128), 0) + PR * p
        OH[p] = jnp.where((r >= lane_r * LAGS) & (r < lane_r * LAGS + LAGS), 1.0, 0.0)
    todo = pieces()
    for k in range(KC):
        x = jnp.broadcast_to(shifted[k : k + 1, :], (64, LC))
        x = pltpu.roll(x, LC - 64 - MAXLAG, axis=1, stride=1, stride_axis=0)
        x = jnp.where(tail, x[:LAGS, :KP], FAR)
        for kk, a, n, p, b in todo:
            if kk == k:
                WF[p, b : b + n, :] = x[a : a + n, :]

    settle(g2, (pl.ds(0, 15),), sem_g2)
    g = g2[0]
    for i in range(1, 16):
        g = g + g2[i]
    mean_row = g[0:1, :] / float(TDAYS)
    stat_o[...] = jnp.zeros((8, 128), F32)
    stat_o[0:1, :] = mean_row
    stat_o[1:2, :] = g[1:2, :] / float(TDAYS) - mean_row * mean_row

    def center(p):
        col = jnp.sum(OH[p] * mean_row, axis=1, keepdims=True)
        for g in range(G):
            x = WF[p, rows(g), :]
            x = jnp.where(x > 0.5 * FAR, 0.0, x - col[16 * g : 16 * g + 16])
            W[p, rows(g), :] = x.astype(BF)

    pltpu.make_async_copy(F.at[:, own_days, :], F.at[:, own_days, :], sem_fr).wait()

    def part_coords(p):
        e0, e1, e2 = onehot3(p)
        return (
            e0 * X + e1 * Y + e2 * Z,
            e0 * Y + e1 * Z + e2 * X,
            e0 * Z + e1 * X + e2 * Y,
        )

    def slot_of(p, ja, jb, hd):
        e0, e1, e2 = onehot3(p)
        jd = 2 * hd + (C + ja + jb) % 2
        jx = e0 * ja + e1 * jd + e2 * jb
        jy = e0 * jb + e1 * ja + e2 * jd
        jz = e0 * jd + e1 * jb + e2 * ja
        return (jx * 4 + jz) * 2 + jy // 2

    sigma = 1 - 2 * C

    def order(b):
        return [(b + 2) % 4, (b + sigma + 4) % 4, (b - sigma + 4) % 4, b]

    def products(p, ja, b, h):
        wide = [F[slot_of(p, ja, jb, hd)] for hd in (h, 1 - h) for jb in order(b)]
        return jnp.dot(W[p], jnp.concatenate(wide, axis=1), preferred_element_type=F32)

    def send_n(u, hd, m):
        at = (u, hd, m)
        remote(
            s_n.at[at], r_n.at[at], sem_sn, sem_n.at[u // 2, m], along(u // 2, 1 - 2 * (u % 2))
        ).start()

    def send_far(u, m):
        at = (u, m)
        remote(
            s_far.at[at], r_far.at[at], sem_sfar, sem_far.at[u, m],
            along(u // 2, 1 - 2 * (u % 2)),
        ).start()

    def turn(v):
        return v + C * (5 - 2 * v)

    @pl.loop(0, 3)
    def _(v):
        p = (v + C) % 3
        a, b, d = part_coords(p)
        center(p)
        acc[...] = products(p, (a + 2) % 4, b, 0)

        def put(g, i, tile):
            s_far[2 * p + i // 4, i % 4, rows(g), :] = tile

        encode(lambda g: acc[rows(g), :], put, 1024)
        for hd in range(2):
            for i in range(3):
                send_far(2 * p + hd, i)

    @pl.loop(0, 6)
    def _(v):
        u = turn(v)
        p, dr = u // 2, u % 2
        a, b, d = part_coords(p)
        got = products(p, (a + 1 - 2 * dr + 4) % 4, b, 1 - dr)
        acc[:, 0:512] = got[:, 0:512]
        for i in range(4):
            NP[u, i] = got[:, 512 + 128 * i : 640 + 128 * i]

        def put(g, i, tile):
            s_n[u, 1 - dr, i, rows(g), :] = tile

        encode(lambda g: acc[rows(g), 0:512], put, 512)
        send_n(u, 1 - dr, 0)
        send_n(u, 1 - dr, 1)

    def near_sum(i):
        @pl.loop(0, 6)
        def _(v):
            u = turn(v)
            dr = u % 2
            settle(r_far, (u, i), sem_far.at[u, i])
            got = decode(lambda g: r_far[u, i, rows(g), :])
            for g in range(G):
                acc[rows(g), 0:128] = NP[u, i, rows(g), :] + got[g]

            def put(g, t, tile):
                s_n[u, dr, i, rows(g), :] = tile

            encode(lambda g: acc[rows(g), 0:128], put, 128)
            send_n(u, dr, i)
            if i == 0:
                send_far(u, 3)
            if 0 < i < 3:
                send_n(u, 1 - dr, i + 1)

    near_sum(0)
    near_sum(1)

    @pl.loop(0, 3)
    def _(p):
        a, b, d = part_coords(p)
        got = products(p, a, b, 0)
        for hd in range(2):
            for i in range(4):
                at = 512 * hd + 128 * i
                S1[2 * p + hd, i] = got[:, at : at + 128]

    def add_tile(w, i, *coded):
        got = [decode(lambda g, c=c: c(g)) for c in coded]
        for g in range(G):
            one = S1[w, i, rows(g), :]
            for c in got:
                one = one + c[g]
            S1[w, i, rows(g), :] = one

    def arrived(p, i):
        settle(r_n, (pl.ds(2 * p, 2), slice(None), i), sem_n.at[p, i])
        for hd in range(2):
            add_tile(
                2 * p + hd, i,
                lambda g: r_n[2 * p, hd, i, rows(g), :],
                lambda g: r_n[2 * p + 1, hd, i, rows(g), :],
            )

    def encode1(w, i, buf, at):
        def put(g, t, tile):
            buf[at + (rows(g), slice(None))] = tile

        encode(lambda g: S1[w, i, rows(g), :], put, 128)

    cell_sums()
    tb1[...] = jnp.zeros((24, 128), F32)
    ones = jnp.ones((8, KP), BF)
    for p in range(3):
        t = lax.dot_general(ones, W[p], (((1,), (1,)), ((), ())), preferred_element_type=F32)
        tb1[16 + 2 * p : 17 + 2 * p, :] = t[0:1, 0:128]
        tb1[17 + 2 * p : 18 + 2 * p, 0:80] = t[0:1, 128:208]

    def gather_sums(dst, ja):
        for jb in range(4):
            for hd in range(2):
                s = slot_of(0, ja, jb, hd)
                i = 2 * jb + hd
                dst[i : i + 1, :] = fsum[s, 0:1, :]
                dst[8 + i : 9 + i, :] = fsum[s, 1:2, :]

    gather_sums(tb1, X)
    for d in range(1, 4):
        to = sx_s.at[d - 1]
        to[16:24, :] = tb1[16:24, :]
        gather_sums(to, (X + d) % 4)
        c = remote(to, sx_r.at[d - 1], sem_ss.at[0], sem_sr.at[0], peer(dx=d))
        c.start()

    @pl.loop(0, 3)
    def _(p):
        arrived(p, 0)
        for hd in range(2):
            u = 2 * p + hd
            encode1(u, 0, s2f, (u,))
            remote(
                s2f.at[u], r2f.at[u], sem_s2f, sem_2f.at[u], along((p + 1) % 3, 1 - 2 * hd)
            ).start()

    def near2(p, i, dr, hd):
        u = 2 * p + dr
        encode1(2 * p + hd, i, s2n, (u, hd))
        remote(
            s2n.at[u, hd], r2n.at[u, hd], sem_s2n, sem_2n.at[p],
            along((p + 1) % 3, 1 - 2 * dr),
        ).start()

    def near2_sum(p, i, dr):
        u = 2 * p + dr
        settle(r2f, (u,), sem_2f.at[u])
        add_tile(u, i, lambda g: r2f[u, rows(g), :])
        near2(p, i, dr, dr)

    near_sum(2)
    near_sum(3)

    @pl.loop(0, 3)
    def _(p):
        arrived(p, 1)
        near2(p, 1, C, 1 - C)

    @pl.loop(0, 3)
    def _(p):
        near2_sum(p, 1, C)

    pltpu.make_async_copy(sx_r, sx_r, sem_sr.at[0]).wait()
    tb1[...] = (tb1[...] + sx_r[0]) + (sx_r[1] + sx_r[2])

    def side_rows(dst, y, z):
        i = 2 * y + z // 2
        dst[0:1, :] = tb1[pl.ds(i, 1), :]
        dst[1:2, :] = tb1[pl.ds(8 + i, 1), :]
        dst[2:8, :] = tb1[16:22, :]

    for n, (dy, dz) in enumerate(yzpeers):
        side_rows(sy_s.at[n], (Y + dy) % 4, (Z + dz) % 4)
        c = remote(
            sy_s.at[n], sy_r.at[n], sem_ss.at[1], sem_sr.at[1], peer(dy=dy, dz=dz)
        )
        c.start()

    @pl.loop(0, 3)
    def _(p):
        arrived(p, 2)
        near2(p, 2, 1 - C, C)

    @pl.loop(0, 3)
    def _(p):
        near2_sum(p, 2, 1 - C)

    @pl.loop(0, 3)
    def _(p):
        arrived(p, 3)

    final = (C + X + Y + Z) % 2 == 0
    lane16 = lax.broadcasted_iota(I32, (16, 128), 1)

    @pl.loop(0, 3)
    def _(p):
        a, b, d = part_coords(p)
        settle(r2n, (pl.ds(2 * p, 2),), sem_2n.at[p])
        for hd in range(2):
            w = 2 * p + hd
            add_tile(
                w, 3,
                lambda g: r2n[2 * p, hd, rows(g), :],
                lambda g: r2n[2 * p + 1, hd, rows(g), :],
            )

        def last_send(w, i, delta):
            raw = []
            encode(lambda g: S1[w, 3, rows(g), :], None, 128, raw)
            for h in range(2):
                for g, q in enumerate(fold(raw, h, lane16)):
                    s3[p, i, h, rows(g), :] = q.astype(I32).astype(jnp.int16)
                remote(
                    s3.at[p, i, h], r3.at[p, i], sem_s3.at[h], sem_3.at[p],
                    along((p + 2) % 3, delta, (h + C) % 2),
                ).start()

        @pl.when(final)
        def _():
            last_send(2 * p + 1 - d // 2, 2, 2)
            chunks = [S1[2 * p + d // 2, 3, rows(g), :] for g in range(G)]
            two = [fold(chunks, h, lane16) for h in range(2)]
            for g in range(HG):
                fin[p, rows(g), :] = jnp.where(C == 0, two[0][g], two[1][g])
                bs[p, rows(g), :] = jnp.where(C == 0, two[1][g], two[0][g])
            remote(bs.at[p], fin.at[p], sem_bs, sem_br.at[p], partner).start()

        @pl.when(jnp.logical_not(final))
        def _():
            for i, delta in enumerate((1, 3)):
                last_send(2 * p + ((d + delta) % 4) // 2, i, delta)

    side_rows(tb3, Y, Z)
    total = tb3[...]
    pltpu.make_async_copy(sy_r, sy_r, sem_sr.at[1]).wait()
    for n in range(15):
        total = total + sy_r[n]
    tot_o[...] = total

    @pl.when(final)
    def _():
        sums_o[...] = total
        remote(sums_o, sums_o, sem_os, sem_or, partner).start()

    @pl.loop(0, 3)
    def _(p):
        @pl.when(jnp.logical_not(final))
        def _():
            settle(fin, (p,), sem_br.at[p])

        settle(r3, (p,), sem_3.at[p])
        got = []
        for i in range(3):
            got.append(decode_folded(lambda g: r3[p, i, rows(g), :]))
        for g in range(HG):
            fin[p, rows(g), :] = (fin[p, rows(g), :] + got[0][g]) + (got[1][g] + got[2][g])

    @pl.when(final)
    def _():
        pltpu.make_async_copy(bs, bs, sem_bs).wait()
        pltpu.make_async_copy(sums_o, sums_o, sem_os).wait()
        for h in range(2):
            pltpu.make_async_copy(s3.at[:, 2, h], s3.at[:, 2, h], sem_s3.at[h]).wait()

    @pl.when(jnp.logical_not(final))
    def _():
        pltpu.make_async_copy(sums_o, sums_o, sem_or).wait()
        for h in range(2):
            pltpu.make_async_copy(s3.at[:, 0:2, h], s3.at[:, 0:2, h], sem_s3.at[h]).wait()

    settle(g1, (pl.ds(0, 7),), sem_gs.at[0])
    settle(g2, (pl.ds(0, 15),), sem_gs.at[1])
    pltpu.make_async_copy(iw, iw, sem_is).wait()
    pltpu.make_async_copy(sx_s, sx_s, sem_ss.at[0]).wait()
    pltpu.make_async_copy(sy_s, sy_s, sem_ss.at[1]).wait()
    pltpu.make_async_copy(F.at[:, own_days, :], F.at[:, own_days, :], sem_fs).wait()
    for buf, sem in ((s_far, sem_sfar), (s_n, sem_sn), (s2f, sem_s2f), (s2n, sem_s2n)):
        pltpu.make_async_copy(buf, buf, sem).wait()


def last_kernel(fin, sums, tot, stat, lag_list, mask, out_hbm, WS, out, sem):
    core = lax.axis_index("core")
    n = float(TDAYS)
    half = 16 * HG
    both = sums[0:8, :]
    turned = pltpu.roll(both, 64, axis=1)
    low = lax.broadcasted_iota(I32, (8, 128), 1) < 64
    both = jnp.where(low == (core == 0), both, turned)
    mean_x = both[0:1, :] / n
    var_x = both[1:2, :] / n - mean_x * mean_x
    inv = 1.0 / (n * jnp.sqrt(var_x + 1e-6))
    row = lax.broadcasted_iota(I32, (half, 256), 0)
    col = lax.broadcasted_iota(I32, (half, 256), 1)
    left = lax.broadcasted_iota(I32, (half, 128), 1) < 64
    WS[KC * LAGS - LAGS - 5 : KC * LAGS + 6, :] = jnp.zeros((LAGS + 11, 128), F32)
    for p in range(3):
        t = jnp.concatenate([tot[2 * p + 2 : 2 * p + 3, :], tot[2 * p + 3 : 2 * p + 4, :]], axis=1)
        t0 = jnp.sum(jnp.where(row == col, t, 0.0), axis=1, keepdims=True)
        t1 = jnp.sum(jnp.where(row + half == col, t, 0.0), axis=1, keepdims=True)
        x = (fin[p] - mean_x * jnp.where(left, t0, t1)) * inv
        y = pltpu.roll(x, 64, axis=1)
        m = min(PR, KC * LAGS - PR * p) - half
        at = PR * p
        WS[at : at + half, 0:64] = x[:, 0:64]
        WS[at + half : at + half + m, 0:64] = y[:m, 0:64]
        cut = max(0, LAGS - at)
        WS[at - LAGS + cut : at - LAGS + half, 64:128] = y[cut:, 64:128]
        WS[at - LAGS + half : at - LAGS + half + m, 64:128] = x[:m, 64:128]
    inv_i = 1.0 / jnp.sqrt(stat[1:2, :] + 1e-6)
    lags = lag_list[...].reshape(1, LAGS)
    place = lax.broadcasted_iota(I32, (64, LAGS), 0) - MAXLAG
    pick = (place == lags).astype(F32).astype(BF)
    pick = jnp.concatenate([pick, pick, pick], axis=0)
    r64 = lax.broadcasted_iota(I32, (64, 64), 0)
    c64 = lax.broadcasted_iota(I32, (64, 64), 1)
    sea = mask[...].reshape(1, 64).astype(F32)
    sea = jnp.sum(jnp.where(r64 == c64, sea, 0.0), axis=1, keepdims=True)
    terms = []
    for k in range(0, KC, 2):
        x = WS[LAGS * k : LAGS * k + 64, :]
        hi = x.astype(BF)
        x = x - hi.astype(F32)
        mid = x.astype(BF)
        lo = (x - mid.astype(F32)).astype(BF)
        terms.append(jnp.concatenate([hi, mid, lo], axis=0))
    y = lax.dot_general(
        jnp.concatenate(terms, axis=1), pick, (((0,), (0,)), ((), ())),
        preferred_element_type=F32,
    )
    for k in range(KC):
        out[k] = y[64 * k : 64 * k + 64] * inv_i[:, k : k + 1] * sea
        pltpu.make_async_copy(out.at[k], out_hbm.at[k], sem.at[k]).start()
    for k in range(KC):
        pltpu.make_async_copy(out.at[k], out_hbm.at[k], sem.at[k]).wait()


def shards(field, index, lag_list, index_offset, sea_mask):
    vmem = pl.BlockSpec(memory_space=pltpu.VMEM)
    i16 = jnp.int16
    dma = pltpu.SemaphoreType.DMA
    fin, sums, tot, stat = pl.pallas_call(
        main_kernel,
        out_shape=(
            jax.ShapeDtypeStruct((3, 16 * HG, 128), F32),
            jax.ShapeDtypeStruct((8, 128), F32),
            jax.ShapeDtypeStruct((8, 128), F32),
            jax.ShapeDtypeStruct((8, 128), F32),
        ),
        in_specs=[pl.BlockSpec(memory_space=pltpu.HBM)] * 3,
        out_specs=(vmem, vmem, vmem, vmem),
        scratch_shapes=[
            pltpu.VMEM((KC, T_DEV), F32),
            pltpu.SMEM((KC,), I32),
            dma((2,)),
            pltpu.VMEM((32, KP, 128), BF),
            pltpu.VMEM((3, R, KP), BF),
            pltpu.VMEM((3, R, KP), F32),
            pltpu.VMEM((3, R, 128), F32),
            pltpu.VMEM((R, 1024), F32),
            pltpu.VMEM((6, 4, R, 128), F32),
            pltpu.VMEM((6, 4, R, 128), F32),
            pltpu.VMEM((6, 4, R, 128), i16),
            pltpu.VMEM((6, 4, R, 128), i16),
            pltpu.VMEM((6, 2, 4, R, 128), i16),
            pltpu.VMEM((6, 2, 4, R, 128), i16),
            pltpu.VMEM((6, R, 128), i16),
            pltpu.VMEM((6, R, 128), i16),
            pltpu.VMEM((6, 2, R, 128), i16),
            pltpu.VMEM((6, 2, R, 128), i16),
            pltpu.VMEM((3, 3, 2, 16 * HG, 128), i16),
            pltpu.VMEM((3, 3, 16 * HG, 128), i16),
            pltpu.VMEM((3, KC, T_DEV), F32),
            pltpu.VMEM((4, 16, 384), F32),
            pltpu.VMEM((3, 16 * HG, 128), F32),
            pltpu.VMEM((8, 2, 128), F32),
            pltpu.VMEM((16, 2, 128), F32),
            pltpu.VMEM((32, 8, 128), F32),
            pltpu.VMEM((3, 24, 128), F32),
            pltpu.VMEM((3, 24, 128), F32),
            pltpu.VMEM((24, 128), F32),
            pltpu.VMEM((15, 8, 128), F32),
            pltpu.VMEM((15, 8, 128), F32),
            pltpu.VMEM((8, 128), F32),
            dma,
            dma,
            dma,
            dma,
            dma,
            dma((2,)),
            dma,
            dma,
            dma((6, 4)),
            dma((3, 4)),
            dma((6,)),
            dma((3,)),
            dma((3,)),
            dma,
            dma,
            dma,
            dma,
            dma((2,)),
            dma((2,)),
            dma((2,)),
            dma,
            dma,
            dma,
            dma((3,)),
        ],
        compiler_params=pltpu.CompilerParams(
            collective_id=0, has_side_effects=True, vmem_limit_bytes=36 * 1024 * 1024
        ),
    )(*(pltpu.with_memory_space_constraint(v, pltpu.HBM) for v in (field, index.T, index_offset)))
    maps = pl.pallas_call(
        last_kernel,
        out_shape=jax.ShapeDtypeStruct((KC, CELLS // 128, LAGS), F32),
        in_specs=[vmem] * 6,
        out_specs=pl.BlockSpec(memory_space=pltpu.HBM),
        scratch_shapes=[
            pltpu.VMEM((616, 128), F32),
            pltpu.VMEM((KC, CELLS // 128, LAGS), F32),
            dma((KC,)),
        ],
        compiler_params=pltpu.CompilerParams(vmem_limit_bytes=8 * 1024 * 1024),
    )(fin, sums, tot, stat, lag_list, sea_mask)
    return jnp.transpose(maps, (1, 0, 2))


def solution(mesh):
    finer = Mesh(mesh.devices.reshape(4, 4, 4, 2), TM)
    return jax.shard_map(
        shards,
        mesh=finer,
        in_specs=(P(TM, None), P(TM, None), P(), P(), P(TM)),
        out_specs=P(TM, None, None),
        check_vma=False,
    )
```

```python
import jax
import jax.numpy as jnp
from jax import lax
from jax.experimental import pallas as pl
from jax.experimental.pallas import tpu as pltpu
from jax.sharding import Mesh
from jax.sharding import PartitionSpec as P

MAXLAG = 30
MAXOFF = 14
LAGS = 61
KC = 10
T_DEV = 336
N_CHIP = 64
CELLS = 8192
TDAYS = 43008
TM = ("x", "z", "y", "core")
MESH = pl.DeviceIdType.MESH

K = 2 * T_DEV
KP = 768
R = 208
PR = 204
G = R // 16
HG = 7
LC = 896
QMAX = 32000.0
FAR = 1e9
I32 = jnp.int32
F32 = jnp.float32
BF = jnp.bfloat16


def pieces():
    out = []
    for k in range(KC):
        r = k * LAGS
        end = r + LAGS
        while r < end:
            p = r // PR
            stop = min(end, (p + 1) * PR)
            out.append((k, r - k * LAGS, stop - r, p, r - p * PR))
            r = stop
    return out


def onehot3(t):
    return (2 - t) * (1 - t) // 2, t * (2 - t), t * (t - 1) // 2


def rows(g):
    return pl.ds(16 * g, 16)


def encode(chunk, put, width, raw=None):
    m = jnp.abs(chunk(0))
    for g in range(1, G):
        m = jnp.maximum(m, jnp.abs(chunk(g)))
    m = jnp.max(m, axis=0, keepdims=True)
    e = jnp.ceil(jnp.log2(jnp.maximum(m, 1e-30)))
    scale = QMAX * jnp.exp2(-e)
    last = lax.broadcasted_iota(I32, (16, width), 0) == 15
    for g in range(G):
        q = jnp.round(chunk(g) * scale)
        if g == G - 1:
            q = jnp.where(last, jnp.broadcast_to(e, (16, width)), q)
        if raw is not None:
            raw.append(q)
            continue
        q = q.astype(I32).astype(jnp.int16)
        for i in range(width // 128):
            put(g, i, q[:, 128 * i : 128 * (i + 1)])


def fold(chunks, h, lane):
    out = []
    for g in range(HG):
        lo = chunks[g]
        hi = chunks[g + HG] if g + HG < G else jnp.zeros((16, 128), F32)
        if h:
            out.append(jnp.where(lane < 64, pltpu.roll(lo, 64, axis=1), hi))
        else:
            out.append(jnp.where(lane < 64, lo, pltpu.roll(hi, 64, axis=1)))
    return out


def decode_folded(get):
    lane = lax.broadcasted_iota(I32, (16, 128), 1)
    row = lax.broadcasted_iota(I32, (16, 128), 0)
    out = [get(g).astype(I32).astype(F32) for g in range(HG)]
    e = out[G - 1 - HG][15:16, :]
    e = jnp.where(lane[0:1] < 64, pltpu.roll(jnp.broadcast_to(e, (8, 128)), 64, axis=1)[0:1], e)
    scale = jnp.exp2(e) * (1.0 / QMAX)
    out = [v * scale for v in out]
    out[G - 1 - HG] = jnp.where((row == 15) & (lane >= 64), 0.0, out[G - 1 - HG])
    return out


def decode(get):
    tail = get(G - 1).astype(I32).astype(F32)
    scale = jnp.exp2(tail[15:16, :]) * (1.0 / QMAX)
    last = lax.broadcasted_iota(I32, (16, 128), 0) == 15
    out = [get(g).astype(I32).astype(F32) * scale for g in range(G - 1)]
    out.append(jnp.where(last, 0.0, tail * scale))
    return out


def main_kernel(
    field, idx_in, offs_in, fin, sums_o, stat_o,
    idx, offs, sem_in, F, W, WF, OH, acc, NP, S1,
    s_far, r_far, s_n, r_n, s2f, r2f, s2n, r2n, s3, r3,
    iw, ipad, bs, g1, g2, fsum, sx_s, sx_r, tb1, sy_s, sy_r, tb3,
    sem_loc, sem_fs, sem_fr, sem_is, sem_ir, sem_gs, sem_g1, sem_g2,
    sem_far, sem_n, sem_2f, sem_2n, sem_3,
    sem_sfar, sem_sn, sem_s2f, sem_s2n, sem_s3, sem_ss, sem_sr, sem_os, sem_or, sem_bs, sem_br,
):
    X, Z, Y, C = (lax.axis_index(a) for a in TM)
    Q = (X * 4 + Z) * 4 + Y

    def peer(dx=0, dz=0, dy=0, dc=0):
        return {
            "x": (X + dx) % 4,
            "z": (Z + dz) % 4,
            "y": (Y + dy) % 4,
            "core": (C + dc) % 2,
        }

    def chip_peer(q, core):
        return {"x": q // 16, "z": (q // 4) % 4, "y": q % 4, "core": core}

    def along(t, delta, dc=0):
        f0, f1, f2 = onehot3(t)
        return peer(dx=f0 * delta, dy=f1 * delta, dz=f2 * delta, dc=dc)

    partner = peer(dc=1)
    xpeers = [(dx, dc) for dx in (2, 1, 3, 0) for dc in (1, 0) if dx or dc]
    yzpeers = [(dy, dz) for dy in range(4) for dz in range(4) if dy or dz]
    yzpeers.sort(key=lambda v: -min(v[0], 4 - v[0]) - min(v[1], 4 - v[1]))
    q_next, q_prev = (Q + 1) % N_CHIP, (Q + N_CHIP - 1) % N_CHIP

    copies = [
        pltpu.make_async_copy(idx_in, idx, sem_in.at[0]),
        pltpu.make_async_copy(offs_in, offs, sem_in.at[1]),
    ]
    for c in copies:
        c.start()

    barrier = pltpu.get_barrier_semaphore()

    def greet(device):
        pl.semaphore_signal(barrier, inc=1, device_id=device, device_id_type=MESH)

    for dy, dz in yzpeers:
        greet(peer(dy=dy, dz=dz))
    for dx, dc in xpeers:
        greet(peer(dx=dx, dc=dc))
    for d in range(1, 4):
        greet(peer(dy=d, dc=1))
        greet(peer(dz=d, dc=1))
    for q in (q_next, q_prev):
        for core in range(2):
            greet(chip_peer(q, core))

    def tile_of(slot, core):
        jx, jz, h = slot // 8, (slot // 2) % 4, slot % 2
        jy = 2 * h + (core + jx + jz) % 2
        return (jx * 4 + jz) * 4 + jy

    def columns(slot, core):
        return pl.ds(pl.multiple_of(tile_of(slot, core) * 128, 128), 128)

    own_days = pl.ds(pl.multiple_of(C * T_DEV, 16), T_DEV)

    eye = lax.broadcasted_iota(I32, (16, 128), 0) == lax.broadcasted_iota(I32, (16, 128), 1)

    def as_row(col):
        return jnp.sum(jnp.where(eye[:KC], col, 0.0), axis=0, keepdims=True)

    for c in copies:
        c.wait()
    mine = idx[...]
    final = (C + X + Y + Z) % 2 == 0
    me8, me16 = X * 2 + C, Y * 4 + Z
    g1[me8, 0:1, :] = as_row(jnp.sum(mine, axis=1, keepdims=True))
    g1[me8, 1:2, :] = as_row(jnp.sum(mine * mine, axis=1, keepdims=True))

    pl.semaphore_wait(barrier, 32)

    def remote(src, dst, ssem, rsem, device):
        return pltpu.make_async_remote_copy(
            src_ref=src, dst_ref=dst, send_sem=ssem, recv_sem=rsem,
            device_id=device, device_id_type=MESH,
        )

    def settle(buf, at, sem):
        pltpu.make_async_copy(buf.at[at], buf.at[at], sem).wait()

    g1c = [
        remote(g1.at[me8], g1.at[me8], sem_gs.at[0], sem_g1, peer(dx=dx, dc=dc))
        for dx, dc in xpeers
    ]
    for c in g1c:
        c.start()
    beside = (Q + N_CHIP + 2 * C - 1) % N_CHIP
    iwc = [remote(idx, iw.at[2], sem_is, sem_ir, partner)]
    for core in range(2):
        iwc.append(
            remote(
                idx, iw.at[1 - C], sem_is, sem_ir, chip_peer(beside, core)
            )
        )
    for c in iwc:
        c.start()

    def share(begin, end):
        @pl.loop(begin, end)
        def _(s):
            remote(
                field.at[:, columns(s, 1 - C)], F.at[s, own_days, :], sem_fs, sem_fr, partner
            ).start()

    @pl.loop(0, 32)
    def _(s):
        pltpu.make_async_copy(
            field.at[:, columns(s, C)], F.at[s, own_days, :], sem_loc
        ).start()

    share(0, 20)

    @pl.loop(0, 32)
    def _(s):
        F[s, K:KP, :] = jnp.zeros((KP - K, 128), BF)

    for i in range(4):
        ipad[i] = jnp.zeros((16, 384), F32)
    ipad[3, 0:KC, 0:T_DEV] = mine

    settle(g1, (pl.ds(0, 7),), sem_g1)
    g = ((g1[0] + g1[1]) + (g1[2] + g1[3])) + ((g1[4] + g1[5]) + (g1[6] + g1[7]))
    g2[me16] = g
    g2c = [
        remote(
            g2.at[me16], g2.at[me16], sem_gs.at[1], sem_g2, peer(dy=dy, dz=dz)
        )
        for dy, dz in yzpeers
    ]
    for c in g2c:
        c.start()
    share(20, 32)

    def cell_sums():
        @pl.loop(0, 32)
        def _(s):
            one = two = jnp.zeros((16, 128), F32)
            for g in range(K // 16):
                v = F[s, rows(g), :].astype(F32)
                one, two = one + v, two + v * v
            fsum[s, 0:1, :] = jnp.sum(one, axis=0, keepdims=True)
            fsum[s, 1:2, :] = jnp.sum(two, axis=0, keepdims=True)

    pltpu.make_async_copy(F.at[:, own_days, :], F.at[:, own_days, :], sem_loc).wait()
    pltpu.make_async_copy(iw, iw, sem_ir).wait()
    for i in range(3):
        ipad[i, 0:KC, 0:T_DEV] = iw[i]
    pos = lax.broadcasted_iota(I32, (16, LC), 1)

    def placed(piece, at):
        wide = jnp.concatenate([piece, jnp.zeros((16, LC - 384), F32)], axis=1)
        return pltpu.roll(wide, at % LC, axis=1)

    mine, other = ipad[3], ipad[2]
    fc = C.astype(F32)
    w0 = mine * (1.0 - fc) + other * fc
    w1 = mine * fc + other * (1.0 - fc)
    series = jnp.where(
        pos < 64,
        placed(ipad[0], 64 - T_DEV),
        jnp.where(
            pos < 64 + T_DEV,
            placed(w0, 64),
            jnp.where(pos < 64 + K, placed(w1, 64 + T_DEV), placed(ipad[1], 64 + K)),
        ),
    )
    day = Q * K - 64 + pos
    series = jnp.where((day >= 0) & (day < TDAYS), series, FAR)
    kth = lax.broadcasted_iota(I32, (16, LC), 0)
    off = jnp.zeros((16, LC), I32)
    for k in range(KC):
        off = jnp.where(kth == k, offs[k], off)
    shifted = series
    for o in range(1, MAXOFF + 1):
        shifted = jnp.where(off == o, pltpu.roll(series, o, axis=1), shifted)
    tail = lax.broadcasted_iota(I32, (LAGS, KP), 1) < K
    lane_r = lax.broadcasted_iota(I32, (R, 128), 1)
    for p in range(3):
        lo = PR if p < 2 else KC * LAGS - 2 * PR
        WF[p, lo - lo % 8 : R, :] = jnp.full((R - lo + lo % 8, KP), FAR, F32)
        r = lax.broadcasted_iota(I32, (R, 128), 0) + PR * p
        OH[p] = jnp.where((r >= lane_r * LAGS) & (r < lane_r * LAGS + LAGS), 1.0, 0.0)
    todo = pieces()
    for k in range(KC):
        x = jnp.broadcast_to(shifted[k : k + 1, :], (64, LC))
        x = pltpu.roll(x, LC - 64 - MAXLAG, axis=1, stride=1, stride_axis=0)
        x = jnp.where(tail, x[:LAGS, :KP], FAR)
        for kk, a, n, p, b in todo:
            if kk == k:
                WF[p, b : b + n, :] = x[a : a + n, :]

    settle(g2, (pl.ds(0, 15),), sem_g2)
    g = g2[0]
    for i in range(1, 16):
        g = g + g2[i]
    mean_row = g[0:1, :] / float(TDAYS)
    stat_o[...] = jnp.zeros((8, 128), F32)
    stat_o[0:1, :] = mean_row
    stat_o[1:2, :] = g[1:2, :] / float(TDAYS) - mean_row * mean_row

    def center(p):
        col = jnp.sum(OH[p] * mean_row, axis=1, keepdims=True)
        for g in range(G):
            x = WF[p, rows(g), :]
            x = jnp.where(x > 0.5 * FAR, 0.0, x - col[16 * g : 16 * g + 16])
            W[p, rows(g), :] = x.astype(BF)

    pltpu.make_async_copy(F.at[:, own_days, :], F.at[:, own_days, :], sem_fr).wait()

    def part_coords(p):
        e0, e1, e2 = onehot3(p)
        return (
            e0 * X + e1 * Y + e2 * Z,
            e0 * Y + e1 * Z + e2 * X,
            e0 * Z + e1 * X + e2 * Y,
        )

    def slot_of(p, ja, jb, hd):
        e0, e1, e2 = onehot3(p)
        jd = 2 * hd + (C + ja + jb) % 2
        jx = e0 * ja + e1 * jd + e2 * jb
        jy = e0 * jb + e1 * ja + e2 * jd
        jz = e0 * jd + e1 * jb + e2 * ja
        return (jx * 4 + jz) * 2 + jy // 2

    sigma = 1 - 2 * C

    def order(b):
        return [(b + 2) % 4, (b + sigma + 4) % 4, (b - sigma + 4) % 4, b]

    def products(p, ja, b, h):
        wide = [F[slot_of(p, ja, jb, hd)] for hd in (h, 1 - h) for jb in order(b)]
        return jnp.dot(W[p], jnp.concatenate(wide, axis=1), preferred_element_type=F32)

    def send_n(u, hd, m):
        at = (u, hd, m)
        remote(
            s_n.at[at], r_n.at[at], sem_sn, sem_n.at[u // 2, m], along(u // 2, 1 - 2 * (u % 2))
        ).start()

    def send_far(u, m):
        at = (u, m)
        remote(
            s_far.at[at], r_far.at[at], sem_sfar, sem_far.at[u, m],
            along(u // 2, 1 - 2 * (u % 2)),
        ).start()

    def turn(v):
        return v + C * (5 - 2 * v)

    @pl.loop(0, 3)
    def _(v):
        p = (v + C) % 3
        a, b, d = part_coords(p)
        center(p)
        acc[...] = products(p, (a + 2) % 4, b, 0)

        def put(g, i, tile):
            s_far[2 * p + i // 4, i % 4, rows(g), :] = tile

        encode(lambda g: acc[rows(g), :], put, 1024)
        for hd in range(2):
            for i in range(3):
                send_far(2 * p + hd, i)

    @pl.loop(0, 6)
    def _(v):
        u = turn(v)
        p, dr = u // 2, u % 2
        a, b, d = part_coords(p)
        got = products(p, (a + 1 - 2 * dr + 4) % 4, b, 1 - dr)
        acc[:, 0:512] = got[:, 0:512]
        for i in range(4):
            NP[u, i] = got[:, 512 + 128 * i : 640 + 128 * i]

        def put(g, i, tile):
            s_n[u, 1 - dr, i, rows(g), :] = tile

        encode(lambda g: acc[rows(g), 0:512], put, 512)
        send_n(u, 1 - dr, 0)
        send_n(u, 1 - dr, 1)

    def near_sum(i):
        @pl.loop(0, 6)
        def _(v):
            u = turn(v)
            dr = u % 2
            settle(r_far, (u, i), sem_far.at[u, i])
            got = decode(lambda g: r_far[u, i, rows(g), :])
            for g in range(G):
                acc[rows(g), 0:128] = NP[u, i, rows(g), :] + got[g]

            def put(g, t, tile):
                s_n[u, dr, i, rows(g), :] = tile

            encode(lambda g: acc[rows(g), 0:128], put, 128)
            send_n(u, dr, i)
            if i == 0:
                send_far(u, 3)
            if i == 1:
                send_n(u, 1 - dr, 2)
            if i == 3:
                send_n(u, 1 - dr, 3)

    near_sum(0)
    near_sum(1)
    near_sum(2)

    @pl.loop(0, 3)
    def _(p):
        a, b, d = part_coords(p)
        got = products(p, a, b, 0)
        for hd in range(2):
            for i in range(4):
                at = 512 * hd + 128 * i
                S1[2 * p + hd, i] = got[:, at : at + 128]

    def add_tile(w, i, *coded):
        got = [decode(lambda g, c=c: c(g)) for c in coded]
        for g in range(G):
            one = S1[w, i, rows(g), :]
            for c in got:
                one = one + c[g]
            S1[w, i, rows(g), :] = one

    def arrived(p, i):
        settle(r_n, (pl.ds(2 * p, 2), slice(None), i), sem_n.at[p, i])
        for hd in range(2):
            add_tile(
                2 * p + hd, i,
                lambda g: r_n[2 * p, hd, i, rows(g), :],
                lambda g: r_n[2 * p + 1, hd, i, rows(g), :],
            )

    def encode1(w, i, buf, at):
        def put(g, t, tile):
            buf[at + (rows(g), slice(None))] = tile

        encode(lambda g: S1[w, i, rows(g), :], put, 128)

    cell_sums()
    tb1[...] = jnp.zeros((24, 128), F32)
    ones = jnp.ones((8, KP), BF)
    for p in range(3):
        t = lax.dot_general(ones, W[p], (((1,), (1,)), ((), ())), preferred_element_type=F32)
        tb1[16 + 2 * p : 17 + 2 * p, :] = t[0:1, 0:128]
        tb1[17 + 2 * p : 18 + 2 * p, 0:80] = t[0:1, 128:208]

    def gather_sums(dst, ja):
        for jb in range(4):
            for hd in range(2):
                s = slot_of(0, ja, jb, hd)
                i = 2 * jb + hd
                dst[i : i + 1, :] = fsum[s, 0:1, :]
                dst[8 + i : 9 + i, :] = fsum[s, 1:2, :]

    gather_sums(tb1, X)
    for d in range(1, 4):
        to = sx_s.at[d - 1]
        to[16:24, :] = tb1[16:24, :]
        gather_sums(to, (X + d) % 4)
        c = remote(to, sx_r.at[d - 1], sem_ss.at[0], sem_sr.at[0], peer(dx=d))
        c.start()


    @pl.loop(0, 3)
    def _(p):
        arrived(p, 0)
        for hd in range(2):
            u = 2 * p + hd
            encode1(u, 0, s2f, (u,))
            remote(
                s2f.at[u], r2f.at[u], sem_s2f, sem_2f.at[u], along((p + 1) % 3, 1 - 2 * hd)
            ).start()

    def near2(p, i, dr, hd):
        u = 2 * p + dr
        encode1(2 * p + hd, i, s2n, (u, hd))
        remote(
            s2n.at[u, hd], r2n.at[u, hd], sem_s2n, sem_2n.at[p],
            along((p + 1) % 3, 1 - 2 * dr),
        ).start()

    def near2_sum(p, i, dr):
        u = 2 * p + dr
        settle(r2f, (u,), sem_2f.at[u])
        add_tile(u, i, lambda g: r2f[u, rows(g), :])
        near2(p, i, dr, dr)

    near_sum(3)

    @pl.loop(0, 3)
    def _(p):
        arrived(p, 1)
        near2(p, 1, C, 1 - C)

    @pl.loop(0, 3)
    def _(p):
        near2_sum(p, 1, C)

    @pl.loop(0, 3)
    def _(p):
        arrived(p, 2)
        near2(p, 2, 1 - C, C)

    @pl.loop(0, 3)
    def _(p):
        near2_sum(p, 2, 1 - C)

    pltpu.make_async_copy(sx_r, sx_r, sem_sr.at[0]).wait()
    tb1[...] = (tb1[...] + sx_r[0]) + (sx_r[1] + sx_r[2])

    def side_rows(dst, y, z):
        i = 2 * y + z // 2
        dst[0:1, :] = tb1[pl.ds(i, 1), :]
        dst[1:2, :] = tb1[pl.ds(8 + i, 1), :]
        dst[2:8, :] = tb1[16:22, :]

    def side_send(odd):
        some = [(dy, dz) for dy, dz in yzpeers if (dy + dz) % 2 == odd]
        for n, (dy, dz) in enumerate(some):
            side_rows(sy_s.at[n], (Y + dy) % 4, (Z + dz) % 4)
            remote(
                sy_s.at[n], sy_r.at[7 * odd + n], sem_ss.at[1], sem_sr.at[1], peer(dy=dy, dz=dz)
            ).start()

    @pl.when(final)
    def _():
        side_send(0)

    @pl.when(jnp.logical_not(final))
    def _():
        side_send(1)

    @pl.loop(0, 3)
    def _(p):
        arrived(p, 3)

    lane16 = lax.broadcasted_iota(I32, (16, 128), 1)

    @pl.loop(0, 3)
    def _(p):
        a, b, d = part_coords(p)
        settle(r2n, (pl.ds(2 * p, 2),), sem_2n.at[p])
        for hd in range(2):
            w = 2 * p + hd
            add_tile(
                w, 3,
                lambda g: r2n[2 * p, hd, rows(g), :],
                lambda g: r2n[2 * p + 1, hd, rows(g), :],
            )

        def last_send(w, i, delta):
            raw = []
            encode(lambda g: S1[w, 3, rows(g), :], None, 128, raw)
            for h in range(2):
                for g, q in enumerate(fold(raw, h, lane16)):
                    s3[p, i, h, rows(g), :] = q.astype(I32).astype(jnp.int16)
                remote(
                    s3.at[p, i, h], r3.at[p, i], sem_s3.at[h], sem_3.at[p],
                    along((p + 2) % 3, delta, (h + C) % 2),
                ).start()

        @pl.when(final)
        def _():
            last_send(2 * p + 1 - d // 2, 2, 2)
            chunks = [S1[2 * p + d // 2, 3, rows(g), :] for g in range(G)]
            two = [fold(chunks, h, lane16) for h in range(2)]
            for g in range(HG):
                fin[p, rows(g), :] = jnp.where(C == 0, two[0][g], two[1][g])
                bs[p, rows(g), :] = jnp.where(C == 0, two[1][g], two[0][g])
            remote(bs.at[p], fin.at[p], sem_bs, sem_br.at[p], partner).start()

        @pl.when(jnp.logical_not(final))
        def _():
            for i, delta in enumerate((1, 3)):
                last_send(2 * p + ((d + delta) % 4) // 2, i, delta)

    @pl.when(final)
    def _():
        pltpu.make_async_copy(sy_r, sy_r, sem_sr.at[1]).wait()
        side_rows(tb3, Y, Z)
        total = tb3[...]
        for n in range(15):
            total = total + sy_r[n]
        sums_o[...] = total
        remote(sums_o, sums_o, sem_os, sem_or, partner).start()

    @pl.loop(0, 3)
    def _(p):
        @pl.when(jnp.logical_not(final))
        def _():
            settle(fin, (p,), sem_br.at[p])

        settle(r3, (p,), sem_3.at[p])
        got = []
        for i in range(3):
            got.append(decode_folded(lambda g: r3[p, i, rows(g), :]))
        for g in range(HG):
            fin[p, rows(g), :] = (fin[p, rows(g), :] + got[0][g]) + (got[1][g] + got[2][g])

    @pl.when(final)
    def _():
        pltpu.make_async_copy(bs, bs, sem_bs).wait()
        pltpu.make_async_copy(sums_o, sums_o, sem_os).wait()
        settle(sy_s, (pl.ds(0, 7),), sem_ss.at[1])
        for h in range(2):
            pltpu.make_async_copy(s3.at[:, 2, h], s3.at[:, 2, h], sem_s3.at[h]).wait()

    @pl.when(jnp.logical_not(final))
    def _():
        pltpu.make_async_copy(sums_o, sums_o, sem_or).wait()
        settle(sy_s, (pl.ds(0, 8),), sem_ss.at[1])
        for h in range(2):
            pltpu.make_async_copy(s3.at[:, 0:2, h], s3.at[:, 0:2, h], sem_s3.at[h]).wait()

    settle(g1, (pl.ds(0, 7),), sem_gs.at[0])
    settle(g2, (pl.ds(0, 15),), sem_gs.at[1])
    pltpu.make_async_copy(iw, iw, sem_is).wait()
    pltpu.make_async_copy(sx_s, sx_s, sem_ss.at[0]).wait()
    pltpu.make_async_copy(F.at[:, own_days, :], F.at[:, own_days, :], sem_fs).wait()
    for buf, sem in ((s_far, sem_sfar), (s_n, sem_sn), (s2f, sem_s2f), (s2n, sem_s2n)):
        pltpu.make_async_copy(buf, buf, sem).wait()


def last_kernel(fin, sums, stat, lag_list, mask, out_hbm, WS, out, sem):
    core = lax.axis_index("core")
    n = float(TDAYS)
    half = 16 * HG
    both = sums[0:8, :]
    turned = pltpu.roll(both, 64, axis=1)
    low = lax.broadcasted_iota(I32, (8, 128), 1) < 64
    both = jnp.where(low == (core == 0), both, turned)
    mean_x = both[0:1, :] / n
    var_x = both[1:2, :] / n - mean_x * mean_x
    inv = 1.0 / (n * jnp.sqrt(var_x + 1e-6))
    row = lax.broadcasted_iota(I32, (half, 256), 0)
    col = lax.broadcasted_iota(I32, (half, 256), 1)
    left = lax.broadcasted_iota(I32, (half, 128), 1) < 64
    WS[KC * LAGS - LAGS - 5 : KC * LAGS + 6, :] = jnp.zeros((LAGS + 11, 128), F32)
    for p in range(3):
        t = jnp.concatenate([sums[2 * p + 2 : 2 * p + 3, :], sums[2 * p + 3 : 2 * p + 4, :]], axis=1)
        t0 = jnp.sum(jnp.where(row == col, t, 0.0), axis=1, keepdims=True)
        t1 = jnp.sum(jnp.where(row + half == col, t, 0.0), axis=1, keepdims=True)
        x = (fin[p] - mean_x * jnp.where(left, t0, t1)) * inv
        y = pltpu.roll(x, 64, axis=1)
        m = min(PR, KC * LAGS - PR * p) - half
        at = PR * p
        WS[at : at + half, 0:64] = x[:, 0:64]
        WS[at + half : at + half + m, 0:64] = y[:m, 0:64]
        cut = max(0, LAGS - at)
        WS[at - LAGS + cut : at - LAGS + half, 64:128] = y[cut:, 64:128]
        WS[at - LAGS + half : at - LAGS + half + m, 64:128] = x[:m, 64:128]
    inv_i = 1.0 / jnp.sqrt(stat[1:2, :] + 1e-6)
    lags = lag_list[...].reshape(1, LAGS)
    place = lax.broadcasted_iota(I32, (64, LAGS), 0) - MAXLAG
    pick = (place == lags).astype(F32).astype(BF)
    pick = jnp.concatenate([pick, pick, pick], axis=0)
    r64 = lax.broadcasted_iota(I32, (64, 64), 0)
    c64 = lax.broadcasted_iota(I32, (64, 64), 1)
    sea = mask[...].reshape(1, 64).astype(F32)
    sea = jnp.sum(jnp.where(r64 == c64, sea, 0.0), axis=1, keepdims=True)
    terms = []
    for k in range(0, KC, 2):
        x = WS[LAGS * k : LAGS * k + 64, :]
        hi = x.astype(BF)
        x = x - hi.astype(F32)
        mid = x.astype(BF)
        lo = (x - mid.astype(F32)).astype(BF)
        terms.append(jnp.concatenate([hi, mid, lo], axis=0))
    y = lax.dot_general(
        jnp.concatenate(terms, axis=1), pick, (((0,), (0,)), ((), ())),
        preferred_element_type=F32,
    )
    for k in range(KC):
        out[k] = y[64 * k : 64 * k + 64] * inv_i[:, k : k + 1] * sea
        pltpu.make_async_copy(out.at[k], out_hbm.at[k], sem.at[k]).start()
    for k in range(KC):
        pltpu.make_async_copy(out.at[k], out_hbm.at[k], sem.at[k]).wait()


def shards(field, index, lag_list, index_offset, sea_mask):
    vmem = pl.BlockSpec(memory_space=pltpu.VMEM)
    i16 = jnp.int16
    dma = pltpu.SemaphoreType.DMA
    fin, sums, stat = pl.pallas_call(
        main_kernel,
        out_shape=(
            jax.ShapeDtypeStruct((3, 16 * HG, 128), F32),
            jax.ShapeDtypeStruct((8, 128), F32),
            jax.ShapeDtypeStruct((8, 128), F32),
        ),
        in_specs=[pl.BlockSpec(memory_space=pltpu.HBM)] * 3,
        out_specs=(vmem, vmem, vmem),
        scratch_shapes=[
            pltpu.VMEM((KC, T_DEV), F32),
            pltpu.SMEM((KC,), I32),
            dma((2,)),
            pltpu.VMEM((32, KP, 128), BF),
            pltpu.VMEM((3, R, KP), BF),
            pltpu.VMEM((3, R, KP), F32),
            pltpu.VMEM((3, R, 128), F32),
            pltpu.VMEM((R, 1024), F32),
            pltpu.VMEM((6, 4, R, 128), F32),
            pltpu.VMEM((6, 4, R, 128), F32),
            pltpu.VMEM((6, 4, R, 128), i16),
            pltpu.VMEM((6, 4, R, 128), i16),
            pltpu.VMEM((6, 2, 4, R, 128), i16),
            pltpu.VMEM((6, 2, 4, R, 128), i16),
            pltpu.VMEM((6, R, 128), i16),
            pltpu.VMEM((6, R, 128), i16),
            pltpu.VMEM((6, 2, R, 128), i16),
            pltpu.VMEM((6, 2, R, 128), i16),
            pltpu.VMEM((3, 3, 2, 16 * HG, 128), i16),
            pltpu.VMEM((3, 3, 16 * HG, 128), i16),
            pltpu.VMEM((3, KC, T_DEV), F32),
            pltpu.VMEM((4, 16, 384), F32),
            pltpu.VMEM((3, 16 * HG, 128), F32),
            pltpu.VMEM((8, 2, 128), F32),
            pltpu.VMEM((16, 2, 128), F32),
            pltpu.VMEM((32, 8, 128), F32),
            pltpu.VMEM((3, 24, 128), F32),
            pltpu.VMEM((3, 24, 128), F32),
            pltpu.VMEM((24, 128), F32),
            pltpu.VMEM((8, 8, 128), F32),
            pltpu.VMEM((15, 8, 128), F32),
            pltpu.VMEM((8, 128), F32),
            dma,
            dma,
            dma,
            dma,
            dma,
            dma((2,)),
            dma,
            dma,
            dma((6, 4)),
            dma((3, 4)),
            dma((6,)),
            dma((3,)),
            dma((3,)),
            dma,
            dma,
            dma,
            dma,
            dma((2,)),
            dma((2,)),
            dma((2,)),
            dma,
            dma,
            dma,
            dma((3,)),
        ],
        compiler_params=pltpu.CompilerParams(
            collective_id=0, has_side_effects=True, vmem_limit_bytes=36 * 1024 * 1024
        ),
    )(*(pltpu.with_memory_space_constraint(v, pltpu.HBM) for v in (field, index.T, index_offset)))
    maps = pl.pallas_call(
        last_kernel,
        out_shape=jax.ShapeDtypeStruct((KC, CELLS // 128, LAGS), F32),
        in_specs=[vmem] * 5,
        out_specs=pl.BlockSpec(memory_space=pltpu.HBM),
        scratch_shapes=[
            pltpu.VMEM((616, 128), F32),
            pltpu.VMEM((KC, CELLS // 128, LAGS), F32),
            dma((KC,)),
        ],
        compiler_params=pltpu.CompilerParams(vmem_limit_bytes=8 * 1024 * 1024),
    )(fin, sums, stat, lag_list, sea_mask)
    return jnp.transpose(maps, (1, 0, 2))


def solution(mesh):
    finer = Mesh(mesh.devices.reshape(4, 4, 4, 2), TM)
    return jax.shard_map(
        shards,
        mesh=finer,
        in_specs=(P(TM, None), P(TM, None), P(), P(), P(TM)),
        out_specs=P(TM, None, None),
        check_vma=False,
    )
```

```python
import jax
import jax.numpy as jnp
from jax import lax
from jax.experimental import pallas as pl
from jax.experimental.pallas import tpu as pltpu
from jax.sharding import Mesh
from jax.sharding import PartitionSpec as P

MAXLAG = 30
MAXOFF = 14
LAGS = 61
KC = 10
T_DEV = 336
N_CHIP = 64
CELLS = 8192
TDAYS = 43008
TM = ("x", "z", "y", "core")
MESH = pl.DeviceIdType.MESH

K = 2 * T_DEV
KP = 768
R = 208
PR = 204
G = R // 16
HG = 7
LC = 896
QMAX = 32000.0
FAR = 1e9
I32 = jnp.int32
F32 = jnp.float32
BF = jnp.bfloat16


def pieces():
    out = []
    for k in range(KC):
        r = k * LAGS
        end = r + LAGS
        while r < end:
            p = r // PR
            stop = min(end, (p + 1) * PR)
            out.append((k, r - k * LAGS, stop - r, p, r - p * PR))
            r = stop
    return out


def onehot3(t):
    return (2 - t) * (1 - t) // 2, t * (2 - t), t * (t - 1) // 2


def rows(g):
    return pl.ds(16 * g, 16)


def encode(chunk, put, width, raw=None):
    m = jnp.abs(chunk(0))
    for g in range(1, G):
        m = jnp.maximum(m, jnp.abs(chunk(g)))
    m = jnp.max(m, axis=0, keepdims=True)
    e = jnp.ceil(jnp.log2(jnp.maximum(m, 1e-30)))
    scale = QMAX * jnp.exp2(-e)
    last = lax.broadcasted_iota(I32, (16, width), 0) == 15
    for g in range(G):
        q = jnp.round(chunk(g) * scale)
        if g == G - 1:
            q = jnp.where(last, jnp.broadcast_to(e, (16, width)), q)
        if raw is not None:
            raw.append(q)
            continue
        q = q.astype(I32).astype(jnp.int16)
        for i in range(width // 128):
            put(g, i, q[:, 128 * i : 128 * (i + 1)])


def fold(chunks, h, lane):
    out = []
    for g in range(HG):
        lo = chunks[g]
        hi = chunks[g + HG] if g + HG < G else jnp.zeros((16, 128), F32)
        if h:
            out.append(jnp.where(lane < 64, pltpu.roll(lo, 64, axis=1), hi))
        else:
            out.append(jnp.where(lane < 64, lo, pltpu.roll(hi, 64, axis=1)))
    return out


def decode_folded(get):
    lane = lax.broadcasted_iota(I32, (16, 128), 1)
    row = lax.broadcasted_iota(I32, (16, 128), 0)
    out = [get(g).astype(I32).astype(F32) for g in range(HG)]
    e = out[G - 1 - HG][15:16, :]
    e = jnp.where(lane[0:1] < 64, pltpu.roll(jnp.broadcast_to(e, (8, 128)), 64, axis=1)[0:1], e)
    scale = jnp.exp2(e) * (1.0 / QMAX)
    out = [v * scale for v in out]
    out[G - 1 - HG] = jnp.where((row == 15) & (lane >= 64), 0.0, out[G - 1 - HG])
    return out


def decode(get):
    tail = get(G - 1).astype(I32).astype(F32)
    scale = jnp.exp2(tail[15:16, :]) * (1.0 / QMAX)
    last = lax.broadcasted_iota(I32, (16, 128), 0) == 15
    out = [get(g).astype(I32).astype(F32) * scale for g in range(G - 1)]
    out.append(jnp.where(last, 0.0, tail * scale))
    return out


def main_kernel(
    field, idx_in, offs_in, fin, sums_o, stat_o,
    idx, offs, sem_in, F, W, WF, OH, acc, NP, S1,
    s_far, r_far, s_n, r_n, s2f, r2f, s2n, r2n, s3, r3,
    iw, ipad, bs, g1, g2, fsum, sx_s, sx_r, tb1, sy_s, sy_r, tb3,
    sem_loc, sem_fs, sem_fr, sem_is, sem_ir, sem_gs, sem_g1, sem_g2,
    sem_far, sem_n, sem_2f, sem_2n, sem_3,
    sem_sfar, sem_sn, sem_s2f, sem_s2n, sem_s3, sem_ss, sem_sr, sem_os, sem_or, sem_bs, sem_br,
):
    X, Z, Y, C = (lax.axis_index(a) for a in TM)
    Q = (X * 4 + Z) * 4 + Y

    def peer(dx=0, dz=0, dy=0, dc=0):
        return {
            "x": (X + dx) % 4,
            "z": (Z + dz) % 4,
            "y": (Y + dy) % 4,
            "core": (C + dc) % 2,
        }

    def chip_peer(q, core):
        return {"x": q // 16, "z": (q // 4) % 4, "y": q % 4, "core": core}

    def along(t, delta, dc=0):
        f0, f1, f2 = onehot3(t)
        return peer(dx=f0 * delta, dy=f1 * delta, dz=f2 * delta, dc=dc)

    partner = peer(dc=1)
    xpeers = [(dx, dc) for dx in (2, 1, 3, 0) for dc in (1, 0) if dx or dc]
    yzpeers = [(dy, dz) for dy in range(4) for dz in range(4) if dy or dz]
    yzpeers.sort(key=lambda v: -min(v[0], 4 - v[0]) - min(v[1], 4 - v[1]))
    q_next, q_prev = (Q + 1) % N_CHIP, (Q + N_CHIP - 1) % N_CHIP

    copies = [
        pltpu.make_async_copy(idx_in, idx, sem_in.at[0]),
        pltpu.make_async_copy(offs_in, offs, sem_in.at[1]),
    ]
    for c in copies:
        c.start()

    barrier = pltpu.get_barrier_semaphore()

    def greet(device):
        pl.semaphore_signal(barrier, inc=1, device_id=device, device_id_type=MESH)

    for dy, dz in yzpeers:
        greet(peer(dy=dy, dz=dz))
    for dx, dc in xpeers:
        greet(peer(dx=dx, dc=dc))
    for d in range(1, 4):
        greet(peer(dy=d, dc=1))
        greet(peer(dz=d, dc=1))
    for q in (q_next, q_prev):
        for core in range(2):
            greet(chip_peer(q, core))

    def tile_of(slot, core):
        jx, jz, h = slot // 8, (slot // 2) % 4, slot % 2
        jy = 2 * h + (core + jx + jz) % 2
        return (jx * 4 + jz) * 4 + jy

    def columns(slot, core):
        return pl.ds(pl.multiple_of(tile_of(slot, core) * 128, 128), 128)

    own_days = pl.ds(pl.multiple_of(C * T_DEV, 16), T_DEV)

    eye = lax.broadcasted_iota(I32, (16, 128), 0) == lax.broadcasted_iota(I32, (16, 128), 1)

    def as_row(col):
        return jnp.sum(jnp.where(eye[:KC], col, 0.0), axis=0, keepdims=True)

    for c in copies:
        c.wait()
    mine = idx[...]
    final = (C + X + Y + Z) % 2 == 0
    me8, me16 = X * 2 + C, Y * 4 + Z
    g1[me8, 0:1, :] = as_row(jnp.sum(mine, axis=1, keepdims=True))
    g1[me8, 1:2, :] = as_row(jnp.sum(mine * mine, axis=1, keepdims=True))

    pl.semaphore_wait(barrier, 32)

    def remote(src, dst, ssem, rsem, device):
        return pltpu.make_async_remote_copy(
            src_ref=src, dst_ref=dst, send_sem=ssem, recv_sem=rsem,
            device_id=device, device_id_type=MESH,
        )

    def settle(buf, at, sem):
        pltpu.make_async_copy(buf.at[at], buf.at[at], sem).wait()

    g1c = [
        remote(g1.at[me8], g1.at[me8], sem_gs.at[0], sem_g1, peer(dx=dx, dc=dc))
        for dx, dc in xpeers
    ]
    for c in g1c:
        c.start()
    beside = (Q + N_CHIP + 2 * C - 1) % N_CHIP
    iwc = [remote(idx, iw.at[2], sem_is, sem_ir, partner)]
    for core in range(2):
        iwc.append(
            remote(
                idx, iw.at[1 - C], sem_is, sem_ir, chip_peer(beside, core)
            )
        )
    for c in iwc:
        c.start()

    def share(begin, end):
        @pl.loop(begin, end)
        def _(s):
            remote(
                field.at[:, columns(s, 1 - C)], F.at[s, own_days, :], sem_fs, sem_fr, partner
            ).start()

    @pl.loop(0, 32)
    def _(s):
        pltpu.make_async_copy(
            field.at[:, columns(s, C)], F.at[s, own_days, :], sem_loc
        ).start()

    share(0, 20)

    @pl.loop(0, 32)
    def _(s):
        F[s, K:KP, :] = jnp.zeros((KP - K, 128), BF)

    for i in range(4):
        ipad[i] = jnp.zeros((16, 384), F32)
    ipad[3, 0:KC, 0:T_DEV] = mine

    settle(g1, (pl.ds(0, 7),), sem_g1)
    g = ((g1[0] + g1[1]) + (g1[2] + g1[3])) + ((g1[4] + g1[5]) + (g1[6] + g1[7]))
    g2[me16] = g
    g2c = [
        remote(
            g2.at[me16], g2.at[me16], sem_gs.at[1], sem_g2, peer(dy=dy, dz=dz)
        )
        for dy, dz in yzpeers
    ]
    for c in g2c:
        c.start()
    share(20, 32)

    def cell_sums():
        @pl.loop(0, 32)
        def _(s):
            one = two = jnp.zeros((16, 128), F32)
            for g in range(K // 16):
                v = F[s, rows(g), :].astype(F32)
                one, two = one + v, two + v * v
            fsum[s, 0:1, :] = jnp.sum(one, axis=0, keepdims=True)
            fsum[s, 1:2, :] = jnp.sum(two, axis=0, keepdims=True)

    pltpu.make_async_copy(F.at[:, own_days, :], F.at[:, own_days, :], sem_loc).wait()
    pltpu.make_async_copy(iw, iw, sem_ir).wait()
    for i in range(3):
        ipad[i, 0:KC, 0:T_DEV] = iw[i]
    pos = lax.broadcasted_iota(I32, (16, LC), 1)

    def placed(piece, at):
        wide = jnp.concatenate([piece, jnp.zeros((16, LC - 384), F32)], axis=1)
        return pltpu.roll(wide, at % LC, axis=1)

    mine, other = ipad[3], ipad[2]
    fc = C.astype(F32)
    w0 = mine * (1.0 - fc) + other * fc
    w1 = mine * fc + other * (1.0 - fc)
    series = jnp.where(
        pos < 64,
        placed(ipad[0], 64 - T_DEV),
        jnp.where(
            pos < 64 + T_DEV,
            placed(w0, 64),
            jnp.where(pos < 64 + K, placed(w1, 64 + T_DEV), placed(ipad[1], 64 + K)),
        ),
    )
    day = Q * K - 64 + pos
    series = jnp.where((day >= 0) & (day < TDAYS), series, FAR)
    kth = lax.broadcasted_iota(I32, (16, LC), 0)
    off = jnp.zeros((16, LC), I32)
    for k in range(KC):
        off = jnp.where(kth == k, offs[k], off)
    shifted = series
    for o in range(1, MAXOFF + 1):
        shifted = jnp.where(off == o, pltpu.roll(series, o, axis=1), shifted)
    tail = lax.broadcasted_iota(I32, (LAGS, KP), 1) < K
    lane_r = lax.broadcasted_iota(I32, (R, 128), 1)
    for p in range(3):
        lo = PR if p < 2 else KC * LAGS - 2 * PR
        WF[p, lo - lo % 8 : R, :] = jnp.full((R - lo + lo % 8, KP), FAR, F32)
        r = lax.broadcasted_iota(I32, (R, 128), 0) + PR * p
        OH[p] = jnp.where((r >= lane_r * LAGS) & (r < lane_r * LAGS + LAGS), 1.0, 0.0)
    todo = pieces()
    for k in range(KC):
        x = jnp.broadcast_to(shifted[k : k + 1, :], (64, LC))
        x = pltpu.roll(x, LC - 64 - MAXLAG, axis=1, stride=1, stride_axis=0)
        x = jnp.where(tail, x[:LAGS, :KP], FAR)
        for kk, a, n, p, b in todo:
            if kk == k:
                WF[p, b : b + n, :] = x[a : a + n, :]

    settle(g2, (pl.ds(0, 15),), sem_g2)
    g = g2[0]
    for i in range(1, 16):
        g = g + g2[i]
    mean_row = g[0:1, :] / float(TDAYS)
    stat_o[...] = jnp.zeros((8, 128), F32)
    stat_o[0:1, :] = mean_row
    var_row = g[1:2, :] / float(TDAYS) - mean_row * mean_row
    stat_o[1:2, :] = var_row
    size_row = jnp.exp2(-jnp.ceil(0.5 * jnp.log2(jnp.maximum(var_row, 0.0) + 1e-6)))
    stat_o[2:3, :] = size_row

    def center(p):
        col = jnp.sum(OH[p] * mean_row, axis=1, keepdims=True)
        size = jnp.sum(OH[p] * size_row, axis=1, keepdims=True)
        for g in range(G):
            x = WF[p, rows(g), :]
            y = (x - col[16 * g : 16 * g + 16]).astype(BF).astype(F32)
            y = y * size[16 * g : 16 * g + 16]
            W[p, rows(g), :] = jnp.where(x > 0.5 * FAR, 0.0, y).astype(BF)

    pltpu.make_async_copy(F.at[:, own_days, :], F.at[:, own_days, :], sem_fr).wait()

    def part_coords(p):
        e0, e1, e2 = onehot3(p)
        return (
            e0 * X + e1 * Y + e2 * Z,
            e0 * Y + e1 * Z + e2 * X,
            e0 * Z + e1 * X + e2 * Y,
        )

    def slot_of(p, ja, jb, hd):
        e0, e1, e2 = onehot3(p)
        jd = 2 * hd + (C + ja + jb) % 2
        jx = e0 * ja + e1 * jd + e2 * jb
        jy = e0 * jb + e1 * ja + e2 * jd
        jz = e0 * jd + e1 * jb + e2 * ja
        return (jx * 4 + jz) * 2 + jy // 2

    sigma = 1 - 2 * C

    def order(b):
        return [(b + 2) % 4, (b + sigma + 4) % 4, (b - sigma + 4) % 4, b]

    def products(p, ja, b, h):
        wide = [F[slot_of(p, ja, jb, hd)] for hd in (h, 1 - h) for jb in order(b)]
        return jnp.dot(W[p], jnp.concatenate(wide, axis=1), preferred_element_type=F32)

    def send_n(u, hd, m):
        at = (u, hd, m)
        remote(
            s_n.at[at], r_n.at[at], sem_sn, sem_n.at[u // 2, m], along(u // 2, 1 - 2 * (u % 2))
        ).start()

    def send_far(u, m):
        at = (u, m)
        remote(
            s_far.at[at], r_far.at[at], sem_sfar, sem_far.at[u, m],
            along(u // 2, 1 - 2 * (u % 2)),
        ).start()

    def turn(v):
        return v + C * (5 - 2 * v)

    @pl.loop(0, 3)
    def _(v):
        p = (v + C) % 3
        a, b, d = part_coords(p)
        center(p)
        acc[...] = products(p, (a + 2) % 4, b, 0)

        def put(g, i, tile):
            s_far[2 * p + i // 4, i % 4, rows(g), :] = tile

        encode(lambda g: acc[rows(g), :], put, 1024)
        for hd in range(2):
            for i in range(3):
                send_far(2 * p + hd, i)

    @pl.loop(0, 6)
    def _(v):
        u = turn(v)
        p, dr = u // 2, u % 2
        a, b, d = part_coords(p)
        got = products(p, (a + 1 - 2 * dr + 4) % 4, b, 1 - dr)
        acc[:, 0:512] = got[:, 0:512]
        for i in range(4):
            NP[u, i] = got[:, 512 + 128 * i : 640 + 128 * i]

        def put(g, i, tile):
            s_n[u, 1 - dr, i, rows(g), :] = tile

        encode(lambda g: acc[rows(g), 0:512], put, 512)
        send_n(u, 1 - dr, 0)
        send_n(u, 1 - dr, 1)

    def near_sum(i):
        @pl.loop(0, 6)
        def _(v):
            u = turn(v)
            dr = u % 2
            settle(r_far, (u, i), sem_far.at[u, i])
            got = decode(lambda g: r_far[u, i, rows(g), :])
            for g in range(G):
                acc[rows(g), 0:128] = NP[u, i, rows(g), :] + got[g]

            def put(g, t, tile):
                s_n[u, dr, i, rows(g), :] = tile

            encode(lambda g: acc[rows(g), 0:128], put, 128)
            send_n(u, dr, i)
            if i == 0:
                send_far(u, 3)
            if i == 1:
                send_n(u, 1 - dr, 2)
            if i == 3:
                send_n(u, 1 - dr, 3)

    near_sum(0)
    near_sum(1)
    near_sum(2)

    @pl.loop(0, 3)
    def _(p):
        a, b, d = part_coords(p)
        got = products(p, a, b, 0)
        for hd in range(2):
            for i in range(4):
                at = 512 * hd + 128 * i
                S1[2 * p + hd, i] = got[:, at : at + 128]

    def add_tile(w, i, *coded):
        got = [decode(lambda g, c=c: c(g)) for c in coded]
        for g in range(G):
            one = S1[w, i, rows(g), :]
            for c in got:
                one = one + c[g]
            S1[w, i, rows(g), :] = one

    def arrived(p, i):
        settle(r_n, (pl.ds(2 * p, 2), slice(None), i), sem_n.at[p, i])
        for hd in range(2):
            add_tile(
                2 * p + hd, i,
                lambda g: r_n[2 * p, hd, i, rows(g), :],
                lambda g: r_n[2 * p + 1, hd, i, rows(g), :],
            )

    def encode1(w, i, buf, at):
        def put(g, t, tile):
            buf[at + (rows(g), slice(None))] = tile

        encode(lambda g: S1[w, i, rows(g), :], put, 128)

    cell_sums()
    tb1[...] = jnp.zeros((24, 128), F32)
    ones = jnp.ones((8, KP), BF)
    for p in range(3):
        t = lax.dot_general(ones, W[p], (((1,), (1,)), ((), ())), preferred_element_type=F32)
        tb1[16 + 2 * p : 17 + 2 * p, :] = t[0:1, 0:128]
        tb1[17 + 2 * p : 18 + 2 * p, 0:80] = t[0:1, 128:208]

    def gather_sums(dst, ja):
        for jb in range(4):
            for hd in range(2):
                s = slot_of(0, ja, jb, hd)
                i = 2 * jb + hd
                dst[i : i + 1, :] = fsum[s, 0:1, :]
                dst[8 + i : 9 + i, :] = fsum[s, 1:2, :]

    gather_sums(tb1, X)
    for d in range(1, 4):
        to = sx_s.at[d - 1]
        to[16:24, :] = tb1[16:24, :]
        gather_sums(to, (X + d) % 4)
        c = remote(to, sx_r.at[d - 1], sem_ss.at[0], sem_sr.at[0], peer(dx=d))
        c.start()


    @pl.loop(0, 3)
    def _(p):
        arrived(p, 0)
        for hd in range(2):
            u = 2 * p + hd
            encode1(u, 0, s2f, (u,))
            remote(
                s2f.at[u], r2f.at[u], sem_s2f, sem_2f.at[u], along((p + 1) % 3, 1 - 2 * hd)
            ).start()

    def near2(p, i, dr, hd):
        u = 2 * p + dr
        encode1(2 * p + hd, i, s2n, (u, hd))
        remote(
            s2n.at[u, hd], r2n.at[u, hd], sem_s2n, sem_2n.at[p],
            along((p + 1) % 3, 1 - 2 * dr),
        ).start()

    def near2_sum(p, i, dr):
        u = 2 * p + dr
        settle(r2f, (u,), sem_2f.at[u])
        add_tile(u, i, lambda g: r2f[u, rows(g), :])
        near2(p, i, dr, dr)

    near_sum(3)

    @pl.loop(0, 3)
    def _(p):
        arrived(p, 1)
        near2(p, 1, C, 1 - C)

    @pl.loop(0, 3)
    def _(p):
        near2_sum(p, 1, C)

    @pl.loop(0, 3)
    def _(p):
        arrived(p, 2)
        near2(p, 2, 1 - C, C)

    @pl.loop(0, 3)
    def _(p):
        near2_sum(p, 2, 1 - C)

    pltpu.make_async_copy(sx_r, sx_r, sem_sr.at[0]).wait()
    tb1[...] = (tb1[...] + sx_r[0]) + (sx_r[1] + sx_r[2])

    def side_rows(dst, y, z):
        i = 2 * y + z // 2
        dst[0:1, :] = tb1[pl.ds(i, 1), :]
        dst[1:2, :] = tb1[pl.ds(8 + i, 1), :]
        dst[2:8, :] = tb1[16:22, :]

    def side_send(odd):
        some = [(dy, dz) for dy, dz in yzpeers if (dy + dz) % 2 == odd]
        for n, (dy, dz) in enumerate(some):
            side_rows(sy_s.at[n], (Y + dy) % 4, (Z + dz) % 4)
            remote(
                sy_s.at[n], sy_r.at[7 * odd + n], sem_ss.at[1], sem_sr.at[1], peer(dy=dy, dz=dz)
            ).start()

    @pl.when(final)
    def _():
        side_send(0)

    @pl.when(jnp.logical_not(final))
    def _():
        side_send(1)

    @pl.loop(0, 3)
    def _(p):
        arrived(p, 3)

    lane16 = lax.broadcasted_iota(I32, (16, 128), 1)

    @pl.loop(0, 3)
    def _(p):
        a, b, d = part_coords(p)
        settle(r2n, (pl.ds(2 * p, 2),), sem_2n.at[p])
        for hd in range(2):
            w = 2 * p + hd
            add_tile(
                w, 3,
                lambda g: r2n[2 * p, hd, rows(g), :],
                lambda g: r2n[2 * p + 1, hd, rows(g), :],
            )

        def last_send(w, i, delta):
            raw = []
            encode(lambda g: S1[w, 3, rows(g), :], None, 128, raw)
            for h in range(2):
                for g, q in enumerate(fold(raw, h, lane16)):
                    s3[p, i, h, rows(g), :] = q.astype(I32).astype(jnp.int16)
                remote(
                    s3.at[p, i, h], r3.at[p, i], sem_s3.at[h], sem_3.at[p],
                    along((p + 2) % 3, delta, (h + C) % 2),
                ).start()

        @pl.when(final)
        def _():
            last_send(2 * p + 1 - d // 2, 2, 2)
            chunks = [S1[2 * p + d // 2, 3, rows(g), :] for g in range(G)]
            two = [fold(chunks, h, lane16) for h in range(2)]
            for g in range(HG):
                fin[p, rows(g), :] = jnp.where(C == 0, two[0][g], two[1][g])
                bs[p, rows(g), :] = jnp.where(C == 0, two[1][g], two[0][g])
            remote(bs.at[p], fin.at[p], sem_bs, sem_br.at[p], partner).start()

        @pl.when(jnp.logical_not(final))
        def _():
            for i, delta in enumerate((1, 3)):
                last_send(2 * p + ((d + delta) % 4) // 2, i, delta)

    @pl.when(final)
    def _():
        pltpu.make_async_copy(sy_r, sy_r, sem_sr.at[1]).wait()
        side_rows(tb3, Y, Z)
        total = tb3[...]
        for n in range(15):
            total = total + sy_r[n]
        sums_o[...] = total
        remote(sums_o, sums_o, sem_os, sem_or, partner).start()

    @pl.loop(0, 3)
    def _(p):
        @pl.when(jnp.logical_not(final))
        def _():
            settle(fin, (p,), sem_br.at[p])

        settle(r3, (p,), sem_3.at[p])
        got = []
        for i in range(3):
            got.append(decode_folded(lambda g: r3[p, i, rows(g), :]))
        for g in range(HG):
            fin[p, rows(g), :] = (fin[p, rows(g), :] + got[0][g]) + (got[1][g] + got[2][g])

    @pl.when(final)
    def _():
        pltpu.make_async_copy(bs, bs, sem_bs).wait()
        pltpu.make_async_copy(sums_o, sums_o, sem_os).wait()
        settle(sy_s, (pl.ds(0, 7),), sem_ss.at[1])
        for h in range(2):
            pltpu.make_async_copy(s3.at[:, 2, h], s3.at[:, 2, h], sem_s3.at[h]).wait()

    @pl.when(jnp.logical_not(final))
    def _():
        pltpu.make_async_copy(sums_o, sums_o, sem_or).wait()
        settle(sy_s, (pl.ds(0, 8),), sem_ss.at[1])
        for h in range(2):
            pltpu.make_async_copy(s3.at[:, 0:2, h], s3.at[:, 0:2, h], sem_s3.at[h]).wait()

    settle(g1, (pl.ds(0, 7),), sem_gs.at[0])
    settle(g2, (pl.ds(0, 15),), sem_gs.at[1])
    pltpu.make_async_copy(iw, iw, sem_is).wait()
    pltpu.make_async_copy(sx_s, sx_s, sem_ss.at[0]).wait()
    pltpu.make_async_copy(F.at[:, own_days, :], F.at[:, own_days, :], sem_fs).wait()
    for buf, sem in ((s_far, sem_sfar), (s_n, sem_sn), (s2f, sem_s2f), (s2n, sem_s2n)):
        pltpu.make_async_copy(buf, buf, sem).wait()


def last_kernel(fin, sums, stat, lag_list, mask, out_hbm, WS, out, sem):
    core = lax.axis_index("core")
    n = float(TDAYS)
    half = 16 * HG
    both = sums[0:8, :]
    turned = pltpu.roll(both, 64, axis=1)
    low = lax.broadcasted_iota(I32, (8, 128), 1) < 64
    both = jnp.where(low == (core == 0), both, turned)
    mean_x = both[0:1, :] / n
    var_x = both[1:2, :] / n - mean_x * mean_x
    inv = 1.0 / (n * jnp.sqrt(var_x + 1e-6))
    row = lax.broadcasted_iota(I32, (half, 256), 0)
    col = lax.broadcasted_iota(I32, (half, 256), 1)
    left = lax.broadcasted_iota(I32, (half, 128), 1) < 64
    WS[KC * LAGS - LAGS - 5 : KC * LAGS + 6, :] = jnp.zeros((LAGS + 11, 128), F32)
    for p in range(3):
        t = jnp.concatenate([sums[2 * p + 2 : 2 * p + 3, :], sums[2 * p + 3 : 2 * p + 4, :]], axis=1)
        t0 = jnp.sum(jnp.where(row == col, t, 0.0), axis=1, keepdims=True)
        t1 = jnp.sum(jnp.where(row + half == col, t, 0.0), axis=1, keepdims=True)
        x = (fin[p] - mean_x * jnp.where(left, t0, t1)) * inv
        y = pltpu.roll(x, 64, axis=1)
        m = min(PR, KC * LAGS - PR * p) - half
        at = PR * p
        WS[at : at + half, 0:64] = x[:, 0:64]
        WS[at + half : at + half + m, 0:64] = y[:m, 0:64]
        cut = max(0, LAGS - at)
        WS[at - LAGS + cut : at - LAGS + half, 64:128] = y[cut:, 64:128]
        WS[at - LAGS + half : at - LAGS + half + m, 64:128] = x[:m, 64:128]
    inv_i = 1.0 / (jnp.sqrt(stat[1:2, :] + 1e-6) * stat[2:3, :])
    lags = lag_list[...].reshape(1, LAGS)
    place = lax.broadcasted_iota(I32, (64, LAGS), 0) - MAXLAG
    pick = (place == lags).astype(F32).astype(BF)
    pick = jnp.concatenate([pick, pick, pick], axis=0)
    r64 = lax.broadcasted_iota(I32, (64, 64), 0)
    c64 = lax.broadcasted_iota(I32, (64, 64), 1)
    sea = mask[...].reshape(1, 64).astype(F32)
    sea = jnp.sum(jnp.where(r64 == c64, sea, 0.0), axis=1, keepdims=True)
    terms = []
    for k in range(0, KC, 2):
        x = WS[LAGS * k : LAGS * k + 64, :]
        hi = x.astype(BF)
        x = x - hi.astype(F32)
        mid = x.astype(BF)
        lo = (x - mid.astype(F32)).astype(BF)
        terms.append(jnp.concatenate([hi, mid, lo], axis=0))
    y = lax.dot_general(
        jnp.concatenate(terms, axis=1), pick, (((0,), (0,)), ((), ())),
        preferred_element_type=F32,
    )
    for k in range(KC):
        out[k] = y[64 * k : 64 * k + 64] * inv_i[:, k : k + 1] * sea
        pltpu.make_async_copy(out.at[k], out_hbm.at[k], sem.at[k]).start()
    for k in range(KC):
        pltpu.make_async_copy(out.at[k], out_hbm.at[k], sem.at[k]).wait()


def shards(field, index, lag_list, index_offset, sea_mask):
    vmem = pl.BlockSpec(memory_space=pltpu.VMEM)
    i16 = jnp.int16
    dma = pltpu.SemaphoreType.DMA
    fin, sums, stat = pl.pallas_call(
        main_kernel,
        out_shape=(
            jax.ShapeDtypeStruct((3, 16 * HG, 128), F32),
            jax.ShapeDtypeStruct((8, 128), F32),
            jax.ShapeDtypeStruct((8, 128), F32),
        ),
        in_specs=[pl.BlockSpec(memory_space=pltpu.HBM)] * 3,
        out_specs=(vmem, vmem, vmem),
        scratch_shapes=[
            pltpu.VMEM((KC, T_DEV), F32),
            pltpu.SMEM((KC,), I32),
            dma((2,)),
            pltpu.VMEM((32, KP, 128), BF),
            pltpu.VMEM((3, R, KP), BF),
            pltpu.VMEM((3, R, KP), F32),
            pltpu.VMEM((3, R, 128), F32),
            pltpu.VMEM((R, 1024), F32),
            pltpu.VMEM((6, 4, R, 128), F32),
            pltpu.VMEM((6, 4, R, 128), F32),
            pltpu.VMEM((6, 4, R, 128), i16),
            pltpu.VMEM((6, 4, R, 128), i16),
            pltpu.VMEM((6, 2, 4, R, 128), i16),
            pltpu.VMEM((6, 2, 4, R, 128), i16),
            pltpu.VMEM((6, R, 128), i16),
            pltpu.VMEM((6, R, 128), i16),
            pltpu.VMEM((6, 2, R, 128), i16),
            pltpu.VMEM((6, 2, R, 128), i16),
            pltpu.VMEM((3, 3, 2, 16 * HG, 128), i16),
            pltpu.VMEM((3, 3, 16 * HG, 128), i16),
            pltpu.VMEM((3, KC, T_DEV), F32),
            pltpu.VMEM((4, 16, 384), F32),
            pltpu.VMEM((3, 16 * HG, 128), F32),
            pltpu.VMEM((8, 2, 128), F32),
            pltpu.VMEM((16, 2, 128), F32),
            pltpu.VMEM((32, 8, 128), F32),
            pltpu.VMEM((3, 24, 128), F32),
            pltpu.VMEM((3, 24, 128), F32),
            pltpu.VMEM((24, 128), F32),
            pltpu.VMEM((8, 8, 128), F32),
            pltpu.VMEM((15, 8, 128), F32),
            pltpu.VMEM((8, 128), F32),
            dma,
            dma,
            dma,
            dma,
            dma,
            dma((2,)),
            dma,
            dma,
            dma((6, 4)),
            dma((3, 4)),
            dma((6,)),
            dma((3,)),
            dma((3,)),
            dma,
            dma,
            dma,
            dma,
            dma((2,)),
            dma((2,)),
            dma((2,)),
            dma,
            dma,
            dma,
            dma((3,)),
        ],
        compiler_params=pltpu.CompilerParams(
            collective_id=0, has_side_effects=True, vmem_limit_bytes=36 * 1024 * 1024
        ),
    )(*(pltpu.with_memory_space_constraint(v, pltpu.HBM) for v in (field, index.T, index_offset)))
    maps = pl.pallas_call(
        last_kernel,
        out_shape=jax.ShapeDtypeStruct((KC, CELLS // 128, LAGS), F32),
        in_specs=[vmem] * 5,
        out_specs=pl.BlockSpec(memory_space=pltpu.HBM),
        scratch_shapes=[
            pltpu.VMEM((616, 128), F32),
            pltpu.VMEM((KC, CELLS // 128, LAGS), F32),
            dma((KC,)),
        ],
        compiler_params=pltpu.CompilerParams(vmem_limit_bytes=8 * 1024 * 1024),
    )(fin, sums, stat, lag_list, sea_mask)
    return jnp.transpose(maps, (1, 0, 2))


def solution(mesh):
    finer = Mesh(mesh.devices.reshape(4, 4, 4, 2), TM)
    return jax.shard_map(
        shards,
        mesh=finer,
        in_specs=(P(TM, None), P(TM, None), P(), P(), P(TM)),
        out_specs=P(TM, None, None),
        check_vma=False,
    )
```
